256 devices in a mesh: section: 8 (over y, x_hi), fsdp: 32 (over x_lo, z, core).
Axes of the slice: x: 4 (x_hi: 2, x_lo: 2; x = x_hi * 2 + x_lo), y: 4, z: 8, core: 2. Of those that a mesh axis runs over, the one named last changes fastest.
Arguments:
- codes: int32 [8, 8192, 512], P('section', 'fsdp'), may hold values from 0 to 15
- scale_codes: int32 [8, 8192, 8], P('section', 'fsdp'), may hold values from 0 to 255
- second_scales: float32 [8, 256], P('section', 'fsdp'), may hold values from 0.015 to 0.09
- gains: bfloat16 [8, 8192], P('section'), may hold values from 0.5 to 1.5
- down_adapter: bfloat16 [8, 8192, 64], P('section'), may hold values from -0.0625 to 0.0625
- up_projection_weight: bfloat16 [8, 512, 64], P('section'), may hold values from -0.75 to 0.75
- hidden_in: bfloat16 [4096, 8192], P('fsdp'), may hold values from -6 to 6
- cotangent: bfloat16 [4096, 8192], P('fsdp'), may hold values from -6 to 6
Outputs:
- input_grad: bfloat16 [8, 4096, 8192], P('section', 'fsdp')
- grad_down: float32 [8, 8192, 64], P('section', 'fsdp')
- grad_up: float32 [8, 512, 64], P('section', 'fsdp')
The draws below stay inside these ranges and needn't reach their ends.
All inputs are finite; a program needn't handle non-finite values.
Results may differ from the reference program's by a relative error of at most 0.025.
Values may be sent and summed in bfloat16 or wider, within the bound.
A program may use at most 128 MiB of HBM per device.

```python
import math
import jax
import jax.numpy as jnp
from jax import lax

D = 8192
HEAD = 128
GROUP = 8
KV_HEADS = 4
RANK = 64
BLOCK = 64
SROWS = 32
KVW = 512
TOKENS = 4096
LAYERS = 8


def touch_ends(result, stream_key, low, largest):
    longest = result.shape.index(max(result.shape))
    spots = []
    for shift in (0, 1):
        where = [jax.random.randint(jax.random.fold_in(stream_key, axis), (), 0, length) for axis, length in enumerate(result.shape)]
        where[longest] = (where[longest] + shift) % result.shape[longest]
        spots.append(tuple(where))
    return result.at[spots[0]].set(low).at[spots[1]].set(largest)


def with_spikes(drawn, own_key, source, target, parts, factor):
    def block_of(dim):
        return (jnp.arange(drawn.shape[dim]) // (drawn.shape[dim] // parts)).reshape((-1,) + (1,) * (drawn.ndim - 1 - dim))

    one_side = jax.random.permutation(own_key, parts)[block_of(target)]
    far = (block_of(target) + parts // 2) % parts
    return jnp.where((block_of(source) == one_side) | (block_of(source) == far), factor * drawn, drawn)


def block_scale(rng, dims, cuts, least, high):
    loudness, own = 1.0, jax.random.fold_in(rng, 6)
    for axis_at, blocks in cuts:
        draws = jnp.exp(jax.random.uniform(jax.random.fold_in(own, axis_at), (blocks,), jnp.float32, least / len(cuts), high / len(cuts)))
        loudness = loudness * jnp.repeat(draws, dims[axis_at] // blocks).reshape([-1 if axis == axis_at else 1 for axis in range(len(dims))])
    return loudness


def noise(rng, extent, scale, bound, pieces=(), kind=jnp.bfloat16):
    result = jax.random.normal(rng, extent, jnp.float32) * scale
    if len(pieces) > 0:
        result = block_scale(rng, extent, pieces, -0.22, 0.18) * result
    return jnp.clip(result, min=-bound, max=bound).astype(kind)


def bell_draw_with(rng, dims, spread, most, pieces, heavy, kind=jnp.bfloat16):
    drawn = spread * jax.random.normal(rng, dims, jnp.float32)
    if pieces:
        drawn = drawn * block_scale(rng, dims, pieces, -0.22, 0.18)
    return jnp.clip(with_spikes(drawn, jax.random.fold_in(rng, 3), *heavy), -most, most).astype(kind)


def setup_inputs(seed: int = 0) -> dict:
    splits = jax.random.split(jax.random.key(seed), 9)
    return {
        "codes": touch_ends(jax.random.randint(splits[0], (LAYERS, D, KVW), 0, 16), jax.random.fold_in(splits[0], 1), 0, 15).astype(jnp.int32),
        "scale_codes": touch_ends(jax.random.randint(splits[1], (LAYERS, D, KVW // BLOCK), 0, 256), jax.random.fold_in(splits[1], 1), 0, 255).astype(jnp.int32),
        "second_scales": jnp.clip(jnp.exp(math.log(0.09) - 1.7917595 * jax.random.uniform(splits[2], (LAYERS, D // SROWS), jnp.float32) ** block_scale(splits[2], (LAYERS, D // SROWS), ((0, 8), (1, 32)), -0.2, 0.2)), 0.015, 0.09),
        "gains": jnp.clip(1.0 + 0.1 * jax.random.normal(splits[3], (LAYERS, D), jnp.float32), 0.5, 1.5).astype(jnp.bfloat16),
        "down_adapter": noise(splits[4], (LAYERS, D, RANK), D ** -0.5, 0.0625, ((0, 8),)),
        "up_projection_weight": noise(splits[5], (LAYERS, KVW, RANK), RANK ** -0.5, 0.75, ((0, 8),)),
        "hidden_in": bell_draw_with(splits[6], (TOKENS, D), 1.0, 6.0, ((0, 32),), (0, 1, 32, 2.75)),
        "cotangent": noise(splits[7], (TOKENS, D), 1.0, 6.0, ((0, 32),)),
    }


NF4_TABLE = (-1.0, -0.6961928009986877, -0.5250730514526367, -0.39491748809814453, -0.28444138169288635, -0.18477343022823334, -0.09105003625154495, 0.0, 0.07958029955625534, 0.16093020141124725, 0.24611230194568634, 0.33791524171066284, 0.44070982933044434, 0.5626170039176941, 0.7229568362236023, 1.0)
adapter_scale = 0.5
epsilon = 1e-05

def dequantize(codes, scale_codes, second_scales):
    table = jnp.asarray(NF4_TABLE, dtype=jnp.float32)
    value_rows = jnp.take(table, codes, axis=0)
    outer = jnp.repeat(second_scales, SROWS)
    block = outer[:, None] * (scale_codes.astype(jnp.float32) + 1.0) / 256.0
    block = jnp.repeat(block, BLOCK, axis=1)
    return (value_rows * block).astype(jnp.bfloat16)

def spread_heads(value_rows, width):
    count = value_rows.shape[0]
    heads = value_rows.reshape(count, KV_HEADS, 1, HEAD)
    wide = jnp.broadcast_to(heads, (count, KV_HEADS, GROUP, HEAD)).reshape(count, KV_HEADS * GROUP * HEAD)
    filler = jnp.zeros((count, width - KV_HEADS * GROUP * HEAD), value_rows.dtype)
    return jnp.concatenate([wide, filler], axis=1)

def collapse_heads(grads):
    count = grads.shape[0]
    part = grads[:, :KV_HEADS * GROUP * HEAD].reshape(count, KV_HEADS, GROUP, HEAD)
    return lax.optimization_barrier(jnp.sum(part, axis=2)).reshape(count, KV_HEADS * HEAD)

def reference(codes, scale_codes, second_scales, gains, down_adapter, up_projection_weight, hidden_in, cotangent):
    hidden = hidden_in
    kept = []
    for layer_slot in range(LAYERS):
        frozen_base = dequantize(codes[layer_slot], scale_codes[layer_slot], second_scales[layer_slot])
        current = hidden.astype(jnp.float32)
        root_mean = jnp.sqrt(lax.optimization_barrier(jnp.mean(current * current, axis=1, keepdims=True)) + epsilon)
        gain = gains[layer_slot].astype(jnp.float32)
        normalized_input = (current / root_mean * gain).astype(jnp.bfloat16)
        narrow_product = jnp.dot(normalized_input, down_adapter[layer_slot], preferred_element_type=jnp.float32).astype(jnp.bfloat16)
        value_rows = jnp.dot(normalized_input, frozen_base, preferred_element_type=jnp.float32) + adapter_scale * jnp.dot(narrow_product, up_projection_weight[layer_slot].T, preferred_element_type=jnp.float32)
        kept.append((hidden, normalized_input, narrow_product))
        hidden = (current + spread_heads(value_rows, D)).astype(jnp.bfloat16)
    gradient = cotangent
    input_grads = []
    down_grads = []
    up_weight_gradients = []
    for layer_slot in reversed(range(LAYERS)):
        previous, normalized_input, narrow_product = kept[layer_slot]
        frozen_base = dequantize(codes[layer_slot], scale_codes[layer_slot], second_scales[layer_slot])
        current = previous.astype(jnp.float32)
        root_mean = jnp.sqrt(lax.optimization_barrier(jnp.mean(current * current, axis=1, keepdims=True)) + epsilon)
        gain = gains[layer_slot].astype(jnp.float32)
        unit = current / root_mean
        descent_vector = collapse_heads(gradient.astype(jnp.float32)).astype(jnp.bfloat16)
        up_weight_gradients.append(adapter_scale * jnp.dot(descent_vector.T, narrow_product, preferred_element_type=jnp.float32))
        narrow_gradient = (adapter_scale * jnp.dot(descent_vector, up_projection_weight[layer_slot], preferred_element_type=jnp.float32)).astype(jnp.bfloat16)
        down_grads.append(jnp.dot(normalized_input.T, narrow_gradient, preferred_element_type=jnp.float32))
        normed_grad = jnp.dot(descent_vector, frozen_base.T, preferred_element_type=jnp.float32) + jnp.dot(narrow_gradient, down_adapter[layer_slot].T, preferred_element_type=jnp.float32)
        scaled = normed_grad * gain
        hidden_grad = (scaled - unit * lax.optimization_barrier(jnp.mean(scaled * unit, axis=1, keepdims=True))) / root_mean
        gradient = (gradient.astype(jnp.float32) + hidden_grad).astype(jnp.bfloat16)
        input_grads.append(gradient)
    return (jnp.stack(input_grads[::-1]), jnp.stack(down_grads[::-1]), jnp.stack(up_weight_gradients[::-1]))
```

```python
import jax
import jax.numpy as jnp
from jax import lax
from jax.experimental import pallas as pl
from jax.experimental.pallas import tpu as pltpu
from jax.sharding import PartitionSpec as P

HEAD = 128
GROUP = 8
KV_HEADS = 4
KVW = KV_HEADS * HEAD
BLOCK = 64
SROWS = 32

NF4_TABLE = (
    -1.0,
    -0.6961928009986877,
    -0.5250730514526367,
    -0.39491748809814453,
    -0.28444138169288635,
    -0.18477343022823334,
    -0.09105003625154495,
    0.0,
    0.07958029955625534,
    0.16093020141124725,
    0.24611230194568634,
    0.33791524171066284,
    0.44070982933044434,
    0.5626170039176941,
    0.7229568362236023,
    1.0,
)
adapter_scale = 0.5
epsilon = 1e-05
F32 = jnp.float32
BF16 = jnp.bfloat16


def dequantize_shard(codes, scale_codes, second_scales):
    value_rows = jnp.zeros(codes.shape, jnp.float32)
    for entry in range(16):
        value_rows = jnp.where(codes == entry, jnp.float32(NF4_TABLE[entry]), value_rows)
    outer = jnp.repeat(second_scales, SROWS)
    block = outer[:, None] * (scale_codes.astype(jnp.float32) + 1.0) / 256.0
    scaled = value_rows.reshape(codes.shape[0], scale_codes.shape[1], BLOCK) * block[:, :, None]
    return scaled.reshape(codes.shape).astype(jnp.bfloat16)


def collapse(rows):
    count = rows.shape[0]
    part = rows[:, : GROUP * KVW].reshape(count, KV_HEADS, GROUP, HEAD)
    return jnp.sum(part, axis=2).reshape(count, KVW)


def spread(rows, width):
    count = rows.shape[0]
    heads = rows.reshape(count, KV_HEADS, 1, HEAD)
    wide = jnp.broadcast_to(heads, (count, KV_HEADS, GROUP, HEAD)).reshape(count, GROUP * KVW)
    return jnp.concatenate([wide, jnp.zeros((count, width - GROUP * KVW), rows.dtype)], axis=1)


def chain_kernel(width, products, mixes, folded, squares, descent, reply):
    layers = products.shape[0]
    folded_hidden = folded[...]
    square_sum = squares[...]
    total = jnp.zeros_like(folded_hidden)
    totals, inverses, values = [], [], []
    for layer in range(layers):
        moved = 2.0 * folded_hidden + GROUP * total
        square = square_sum + jnp.sum(total * moved, axis=1, keepdims=True)
        inverse = 1.0 / jnp.sqrt(square / width + epsilon)
        mixed = products[layer].astype(F32)
        if layer:
            mixed += jnp.dot(total.astype(BF16), mixes[layer], preferred_element_type=F32)
        value = mixed * inverse
        totals.append(total)
        inverses.append(inverse)
        values.append(value)
        total = total + value
    direction = descent[...]
    for layer in reversed(range(layers)):
        inverse = inverses[layer]
        ratio = jnp.sum(direction * values[layer], axis=1, keepdims=True) / width
        slope = ratio * inverse * inverse
        scaled = (direction * inverse).astype(BF16)
        reply[layer, :, :KVW] = scaled
        reply[layer, :, KVW : 2 * KVW] = totals[layer].astype(BF16)
        reply[layer, :, 2 * KVW :] = jnp.broadcast_to(slope, (slope.shape[0], HEAD)).astype(BF16)
        if layer:
            direction = (
                direction
                + lax.dot_general(
                    scaled, mixes[layer], (((1,), (1,)), ((), ())), preferred_element_type=F32
                )
                - (folded_hidden + GROUP * totals[layer]) * slope
            )


def shards(
    codes,
    scale_codes,
    second_scales,
    gains,
    down_adapter,
    up_projection_weight,
    hidden_in,
    cotangent,
):
    section = lax.axis_index("section")
    sections = lax.axis_size("section")
    place = lax.axis_index("fsdp")
    places = lax.axis_size("fsdp")
    gain = gains[0].astype(F32)
    down = down_adapter[0]
    raised = up_projection_weight[0]
    tokens, width = hidden_in.shape
    rank = down.shape[1]
    own_rows = codes.shape[1]
    own = tokens // sections

    base = dequantize_shard(codes[0], scale_codes[0], second_scales[0])
    down_rows = lax.dynamic_slice_in_dim(down, place * own_rows, own_rows, 0)
    gain_rows = lax.dynamic_slice_in_dim(gain, place * own_rows, own_rows, 0)
    low = jnp.dot(down_rows, raised.T, preferred_element_type=F32)
    shard = ((base.astype(F32) + adapter_scale * low) * gain_rows[:, None]).astype(BF16)
    weight = lax.all_gather(shard, "fsdp", axis=0, tiled=True)

    product = jnp.dot(hidden_in, weight, preferred_element_type=F32).astype(BF16)
    mix = (
        weight[: GROUP * KVW]
        .reshape(KV_HEADS, GROUP, HEAD, KVW)
        .astype(F32)
        .sum(axis=1)
        .reshape(KVW, KVW)
        .astype(BF16)
    )
    mixes = lax.all_gather(mix, "section", axis=0)
    products = lax.all_to_all(
        product.reshape(sections, own, KVW), "section", split_axis=0, concat_axis=0, tiled=True
    )
    own_hidden = lax.dynamic_slice_in_dim(hidden_in, section * own, own, 0).astype(F32)
    own_cotangent = lax.dynamic_slice_in_dim(cotangent, section * own, own, 0).astype(F32)
    squares = jnp.sum(own_hidden * own_hidden, axis=1, keepdims=True)
    reply = pl.pallas_call(
        lambda *refs: chain_kernel(width, *refs),
        out_shape=jax.ShapeDtypeStruct((sections, own, 2 * KVW + HEAD), BF16),
        name="chain",
    )(products, mixes, collapse(own_hidden), squares, collapse(own_cotangent))
    answer = lax.all_to_all(reply, "section", split_axis=0, concat_axis=0, tiled=True)
    answer = answer.reshape(tokens, 2 * KVW + HEAD)
    direction = answer[:, :KVW]
    total = answer[:, KVW : 2 * KVW]
    slope = answer[:, 2 * KVW : 2 * KVW + 1].astype(F32)

    current = hidden_in.astype(F32) + spread(total.astype(F32), width)
    hidden_grad = lax.dot_general(
        direction, weight, (((1,), (1,)), ((), ())), preferred_element_type=F32
    )
    hidden_grad = (hidden_grad - current * slope).astype(BF16)
    pieces = lax.all_to_all(
        hidden_grad.reshape(sections, own, width),
        "section",
        split_axis=0,
        concat_axis=0,
        tiled=True,
    )
    running = own_cotangent
    sums = []
    for layer in reversed(range(sections)):
        running = running + pieces[layer].astype(F32)
        sums.append(running.astype(BF16))
    input_grad = lax.all_to_all(
        jnp.stack(sums[::-1]), "section", split_axis=0, concat_axis=0, tiled=True
    ).reshape(1, tokens, width)

    contract = (((0,), (0,)), ((), ()))
    low_grad = (
        adapter_scale * jnp.dot(direction, raised, preferred_element_type=F32)
    ).astype(BF16)
    current_bf = current.astype(BF16)
    down_grad = lax.dot_general(current_bf, low_grad, contract, preferred_element_type=F32)
    down_grad = (down_grad * gain[:, None]).astype(BF16)
    gained_down = (down.astype(F32) * gain[:, None]).astype(BF16)
    narrow = jnp.dot(current_bf, gained_down, preferred_element_type=F32).astype(BF16)
    up_grad = (
        adapter_scale
        * lax.dot_general(direction, narrow, contract, preferred_element_type=F32)
    ).astype(BF16)
    packed = jnp.concatenate(
        [down_grad.reshape(places, -1, rank), up_grad.reshape(places, -1, rank)], axis=1
    )
    arrived = lax.all_to_all(packed, "fsdp", split_axis=0, concat_axis=0, tiled=True)
    summed = arrived.astype(F32).sum(axis=0)
    return (input_grad, summed[None, :own_rows], summed[None, own_rows:])


def solution(mesh):
    return jax.shard_map(
        shards,
        mesh=mesh,
        in_specs=(
            P("section", "fsdp", None),
            P("section", "fsdp", None),
            P("section", "fsdp"),
            P("section", None),
            P("section", None, None),
            P("section", None, None),
            P("fsdp", None),
            P("fsdp", None),
        ),
        out_specs=(
            P("section", "fsdp", None),
            P("section", "fsdp", None),
            P("section", "fsdp", None),
        ),
        check_vma=False,
    )
```

```python
import functools

import jax
import jax.numpy as jnp
from jax import lax
from jax.experimental import pallas as pl
from jax.experimental.pallas import tpu as pltpu
from jax.sharding import PartitionSpec as P

HEAD = 128
GROUP = 8
KV_HEADS = 4
KVW = KV_HEADS * HEAD
BLOCK = 64
SROWS = 32

NF4_TABLE = (
    -1.0,
    -0.6961928009986877,
    -0.5250730514526367,
    -0.39491748809814453,
    -0.28444138169288635,
    -0.18477343022823334,
    -0.09105003625154495,
    0.0,
    0.07958029955625534,
    0.16093020141124725,
    0.24611230194568634,
    0.33791524171066284,
    0.44070982933044434,
    0.5626170039176941,
    0.7229568362236023,
    1.0,
)
adapter_scale = 0.5
epsilon = 1e-05
F32 = jnp.float32
BF16 = jnp.bfloat16


def dequantize_shard(codes, scale_codes, second_scales):
    value_rows = jnp.zeros(codes.shape, jnp.float32)
    for entry in range(16):
        value_rows = jnp.where(codes == entry, jnp.float32(NF4_TABLE[entry]), value_rows)
    outer = jnp.repeat(second_scales, SROWS)
    block = outer[:, None] * (scale_codes.astype(jnp.float32) + 1.0) / 256.0
    scaled = value_rows.reshape(codes.shape[0], scale_codes.shape[1], BLOCK) * block[:, :, None]
    return scaled.reshape(codes.shape).astype(jnp.bfloat16)


def chip_kernel(
    width,
    shard,
    hidden_hbm,
    cotangent_hbm,
    gained_hbm,
    raised,
    out,
    grad_out,
    weight,
    mixes,
    hidden,
    cotangent,
    gained,
    product,
    product_send,
    product_recv,
    folded,
    descent,
    squares,
    totals,
    values,
    inverses,
    scaled_send,
    total_send,
    slope_send,
    scaled,
    total,
    slopes,
    pair_send,
    odd,
    pair_recv,
    later_send,
    later,
    other_send,
    grad_send,
    grad_recv,
    narrow,
    local_sem,
    send_sem,
    weight_sem,
    mix_sem,
    product_sem,
    reply_sem,
    pair_sem,
    later_sem,
    other_sem,
    grad_send_sem,
    grad_sem,
):
    section = lax.axis_index("section")
    place = lax.axis_index("fsdp")
    y, xh = section // 2, section % 2
    xl, z, core = place // 16, (place // 2) % 8, place % 2
    half_width = width // 2
    column_base = xh * half_width
    layers = 2 * 4

    def device(to_section, to_place):
        return (to_section, to_place)

    mate = device(section, 2 * (place // 2) + 1 - core)
    across = device(section, (place + 16) % 32)
    above = device(section, xl * 16 + ((z + 1) % 8) * 2 + core)
    below = device(section, xl * 16 + ((z + 7) % 8) * 2 + core)
    twin = 2 * y + 1 - xh
    swap = device(twin, (place + 16) % 32)
    used = [0]

    def transfer(source, target, arrival, to, sem=None):
        if sem is None:
            sem = send_sem.at[used[0]]
            used[0] += 1
        copy = pltpu.make_async_remote_copy(
            src_ref=source,
            dst_ref=target,
            send_sem=sem,
            recv_sem=arrival,
            device_id=to,
            device_id_type=pl.DeviceIdType.MESH,
        )
        copy.start()
        return copy

    def arrive(target, arrival):
        pltpu.make_async_remote_copy(
            src_ref=target,
            dst_ref=target,
            send_sem=send_sem.at[0],
            recv_sem=arrival,
            device_id=mate,
            device_id_type=pl.DeviceIdType.MESH,
        ).wait_recv()

    loads = [
        pltpu.make_async_copy(hidden_hbm, hidden, local_sem.at[0]),
        pltpu.make_async_copy(cotangent_hbm, cotangent, local_sem.at[1]),
        pltpu.make_async_copy(gained_hbm, gained, local_sem.at[2]),
    ]
    for load in loads:
        load.start()

    barrier = pltpu.get_barrier_semaphore()

    def greet(to):
        pl.semaphore_signal(
            barrier, inc=1, device_id=to, device_id_type=pl.DeviceIdType.MESH
        )

    def greet_place(step, carry):
        greet(device(section, (place + step) % 32))
        return carry

    lax.fori_loop(1, 32, greet_place, 0)
    for step in range(1, layers):
        greet(device((section + step) % 8, place))
    greet(swap)
    pl.semaphore_wait(barrier, 31 + 7 + 1)

    pending = []

    def slot(x, depth, which):
        return x * 16 + depth * 2 + which

    def half(block, h):
        return weight.at[block, pl.ds(h * 128, 128)]

    def pass_on(block, h, to):
        pending.append(transfer(half(block, h), half(block, h), weight_sem.at[block * 2 + h], to))

    def await_block(block, h):
        arrive(half(block, h), weight_sem.at[block * 2 + h])

    swapped_place = (place + 16) % 32

    @pl.when(xl != xh)
    def _():
        for h in range(2):
            transfer(
                shard.at[pl.ds(h * 128, 128)],
                half(swapped_place, h),
                weight_sem.at[swapped_place * 2 + h],
                swap,
                local_sem.at[3 + h],
            )

    @pl.when(xl == xh)
    def _():
        pltpu.make_async_copy(shard, weight.at[place], local_sem.at[3]).start()

    loads[0].wait()
    loads[1].wait()
    loads[2].wait()
    rows = pl.ds(y * 32, 32)

    def fold(ref):
        for head in range(KV_HEADS):
            part = jnp.zeros((32, HEAD), F32)
            for member in range(GROUP):
                at = (head * GROUP + member) * HEAD
                part += ref[rows, pl.ds(at, HEAD)].astype(F32)
            yield head, part

    @pl.when(xl == xh)
    def _():
        pltpu.make_async_copy(shard, weight.at[place], local_sem.at[3]).wait()

    others = [place, slot(1 - xl, z, core)]
    for h in range(2):

        @pl.when(xl != xh)
        def _():
            await_block(place, h)

        if h == 0:
            pass_on(place, h, across)
        for to in (above, below, mate):
            pass_on(place, h, to)
    for head, part in fold(hidden):
        folded[:, head * HEAD : (head + 1) * HEAD] = part
    for head, part in fold(cotangent):
        descent[:, head * HEAD : (head + 1) * HEAD] = part
    square = jnp.zeros((32, HEAD), F32)
    for at in range(0, width, HEAD):
        piece = hidden[rows, pl.ds(at, HEAD)].astype(F32)
        square += piece * piece
    squares[...] = jnp.broadcast_to(jnp.sum(square, axis=1, keepdims=True), (32, HEAD))
    product[...] = jnp.zeros_like(product)

    await_block(others[1], 0)
    for to in (above, below, mate):
        pass_on(others[1], 0, to)

    def at_distance(distance):
        if distance == 0:
            return [z]
        if distance == 4:
            return [(z + 4) % 8]
        return [(z + 8 - distance) % 8, (z + distance) % 8]

    def multiply(distance, which):
        depths = len(at_distance(distance))

        def step(index, carry):
            x = index // depths
            depth = (z + 8 - distance + (index % depths) * 2 * distance) % 8
            block = slot(x, depth, which)
            columns = pl.ds(pl.multiple_of(column_base + (depth * 2 + which) * 256, 256), 256)
            product[x] += jnp.dot(hidden[:, columns], weight[block], preferred_element_type=F32)
            return carry

        lax.fori_loop(0, 2 * depths, step, 0)

    def relay_across(distance):
        for depth in at_distance(distance):
            block = slot(1 - xl, depth, core)
            await_block(block, 1)
            pass_on(block, 1, mate)

    def await_mate(distance):
        for depth in at_distance(distance):
            for x in range(2):
                for h in range(2):
                    await_block(slot(x, depth, 1 - core), h)

    for distance in range(1, 5):
        low, high = (z + 8 - distance) % 8, (z + distance) % 8
        for x, h, up_reach, down_reach in ((xl, 0, 4, 3), (1 - xl, 0, 3, 4), (xl, 1, 4, 3)):
            for depth, reach, onward in ((low, up_reach, above), (high, down_reach, below)):
                if distance > reach:
                    continue
                block = slot(x, depth, core)
                await_block(block, h)
                if distance < reach:
                    pass_on(block, h, onward)
                pass_on(block, h, mate)
                if h == 1:
                    pass_on(block, h, across)
        if distance == 1:
            pass_on(place, 1, across)
        relay_across(distance - 1)
        multiply(distance - 1, core)
        if distance >= 2:
            await_mate(distance - 2)
            multiply(distance - 2, 1 - core)
    relay_across(4)
    multiply(4, core)
    for distance in (3, 4):
        await_mate(distance)
        multiply(distance, 1 - core)

    @pl.when(xh == 0)
    def _():
        for pair in range(2):
            for head in range(KV_HEADS):

                def add(index, carry):
                    block = pair * 16 + head * 4 + index
                    return (
                        carry
                        + weight[block, :128].astype(F32)
                        + weight[block, 128:].astype(F32)
                    )

                mix = lax.fori_loop(0, 4, add, jnp.zeros((HEAD, KVW), F32))
                mixes[2 * y + pair, head * HEAD : (head + 1) * HEAD] = mix.astype(BF16)

    product_send[...] = product[...].astype(BF16)
    y_up, y_down = (y + 1) % 4, (y + 3) % 4
    y_far = (y + 2) % 4
    mix_base = used[0]
    used[0] += 8

    def mix_block(which_y, which, part=None):
        if part is None:
            return mixes.at[pl.ds(2 * which_y, 2), pl.ds(which * 256, 256)]
        return mixes.at[pl.ds(2 * which_y, 2), pl.ds(which * 256 + part * 128, 128)]

    mix_moves = (
        (mix_block(y, core), 0, (2 * y_up, place)),
        (mix_block(y, core), 1, (2 * y_down, place)),
        (mix_block(y_down, core, 0), 2, (2 * y_up, place)),
        (mix_block(y_up, core, 1), 3, (2 * y_down, place)),
        (mix_block(y_down, core), 4, mate),
        (mix_block(y_up, core), 5, mate),
        (mix_block(y_far, core, 0), 6, mate),
        (mix_block(y_far, core, 1), 7, mate),
    )

    def start_mix(index):
        block, sem, to = mix_moves[index]
        return transfer(block, block, mix_sem.at[sem], to, send_sem.at[mix_base + index])

    @pl.when(xh == 0)
    def _():
        start_mix(0)
        start_mix(1)

    product_base = used[0]
    used[0] += 4

    def send_product(step):
        to_y = (y + step) % 4
        return transfer(
            product_send.at[:, pl.ds(to_y * 32, 32)],
            product_recv.at[section],
            product_sem.at[section],
            (2 * to_y, place),
            send_sem.at[product_base + step],
        )

    for step in range(1, 4):
        pending.append(send_product(step))

    @pl.when(xh == 1)
    def _():
        send_product(0)

    reply_base = used[0]
    used[0] += 24

    def reply_copies(step, to_column):
        to_y = (y + step) % 4
        to = (2 * to_y + to_column, place)
        at = reply_base + (step * 2 + to_column) * 3
        yield (
            scaled_send.at[pl.ds(2 * to_y, 2)],
            scaled.at[:, pl.ds(y * 32, 32)],
            reply_sem.at[y * 3],
            to,
            send_sem.at[at],
        )
        yield (
            slope_send.at[to_y],
            slopes.at[pl.ds(y * 32, 32)],
            reply_sem.at[y * 3 + 1],
            to,
            send_sem.at[at + 1],
        )
        if to_column == 0:
            yield (
                total_send.at[pl.ds(2 * to_y, 2)],
                total.at[:, pl.ds(y * 32, 32)],
                reply_sem.at[y * 3 + 2],
                to,
                send_sem.at[at + 2],
            )
        else:
            yield (
                total_send.at[2 * to_y + 1],
                total.at[1, pl.ds(y * 32, 32)],
                reply_sem.at[y * 3 + 2],
                to,
                send_sem.at[at + 2],
            )

    @pl.when(xh == 0)
    def _():
        product_recv[section] = product_send[:, rows]
        arrive(mix_block(y_down, core), mix_sem.at[0])
        start_mix(2)
        start_mix(4)
        arrive(mix_block(y_up, core), mix_sem.at[1])
        start_mix(3)
        start_mix(5)
        arrive(mix_block(y_far, core, 0), mix_sem.at[2])
        start_mix(6)
        arrive(mix_block(y_far, core, 1), mix_sem.at[3])
        start_mix(7)
        arrive(product_recv.at[section + 1], product_sem.at[section + 1])
        for step in range(1, 4):
            for column in range(2):
                sender = 2 * ((y + step) % 4) + column
                arrive(product_recv.at[sender], product_sem.at[sender])
        arrive(mix_block(y_down, 1 - core), mix_sem.at[4])
        arrive(mix_block(y_up, 1 - core), mix_sem.at[5])
        arrive(mix_block(y_far, 1 - core, 0), mix_sem.at[6])
        arrive(mix_block(y_far, 1 - core, 1), mix_sem.at[7])

        square_sum = squares[:, :1]
        running = jnp.zeros((32, KVW), F32)
        for layer in range(layers):
            moved = 2.0 * folded[...] + GROUP * running
            energy = square_sum + jnp.sum(running * moved, axis=1, keepdims=True)
            inverse = 1.0 / jnp.sqrt(energy / width + epsilon)
            pair_at = layer - layer % 2
            mixed = product_recv[pair_at, layer % 2].astype(F32) + product_recv[
                pair_at + 1, layer % 2
            ].astype(F32)
            if layer:
                mixed += jnp.dot(running.astype(BF16), mixes[layer], preferred_element_type=F32)
            value = mixed * inverse
            totals[layer] = running
            values[layer] = value
            inverses[layer] = jnp.broadcast_to(inverse, (32, HEAD))
            total_send[layer] = running.astype(BF16)
            running = running + value
        direction = descent[...]
        for layer in reversed(range(layers)):
            inverse = inverses[layer][:, :1]
            slope = (
                jnp.sum(direction * values[layer], axis=1, keepdims=True)
                / width
                * inverse
                * inverse
            )
            step_scaled = (direction * inverse).astype(BF16)
            scaled_send[layer] = step_scaled
            at = (layer % 2) * 64
            slope_send[layer // 2, :, at : at + 64] = jnp.broadcast_to(slope, (32, 64))
            if layer:
                direction = (
                    direction
                    + lax.dot_general(
                        step_scaled,
                        mixes[layer],
                        (((1,), (1,)), ((), ())),
                        preferred_element_type=F32,
                    )
                    - (folded[...] + GROUP * totals[layer]) * slope
                )
        for item in range(3):
            for step in (1, 2, 3, 0):
                for column in range(2):
                    if step == 0 and column == 0:
                        continue
                    transfer(*list(reply_copies(step, column))[item])
        scaled[:, rows] = scaled_send[pl.ds(2 * y, 2)]
        total[:, rows] = total_send[pl.ds(2 * y, 2)]
        slopes[rows] = slope_send[y]

    def await_reply(step):
        from_y = (y + step) % 4
        token_rows = pl.ds(from_y * 32, 32)
        arrive(scaled.at[:, token_rows], reply_sem.at[from_y * 3])
        arrive(slopes.at[token_rows], reply_sem.at[from_y * 3 + 1])

        @pl.when(xh == 0)
        def _():
            arrive(total.at[:, token_rows], reply_sem.at[from_y * 3 + 2])

        @pl.when(xh == 1)
        def _():
            arrive(total.at[1, token_rows], reply_sem.at[from_y * 3 + 2])

    for step in range(1, 4):
        await_reply(step)

    @pl.when(xh == 1)
    def _():
        await_reply(0)

    column_flag = (1 - xh).astype(F32)
    pair_base = used[0]
    used[0] += 28
    quarter = half_width // 4

    def pair_copy(q, step):
        to_y = (y + step) % 4
        columns = pl.ds(q * quarter, quarter)
        return (
            pair_send.at[pl.ds(to_y * 32, 32), columns],
            pair_recv.at[y, :, columns],
            pair_sem.at[y * 4 + q],
            (2 * to_y + xh, place),
            send_sem.at[pair_base + q * 3 + step - 1],
        )

    def later_copy(q, step):
        to_y = (y + step) % 4
        columns = pl.ds(q * quarter, quarter)
        return (
            later_send.at[to_y, :, columns],
            later.at[pl.ds(y * 32, 32), columns],
            later_sem.at[y * 4 + q],
            (2 * to_y + xh, place),
            send_sem.at[pair_base + 12 + q * 3 + step - 1],
        )

    def other_copy(q):
        return (
            other_send.at[:, pl.ds(q * quarter, quarter)],
            out.at[:, pl.ds(pl.multiple_of(column_base + q * quarter, quarter), quarter)],
            other_sem.at[q],
            (twin, place),
            send_sem.at[pair_base + 24 + q],
        )

    def hidden_gradients(q):
        def step(index, carry):
            block = q * 4 + index
            at = pl.multiple_of(block * 256, 256)
            columns = pl.ds(pl.multiple_of(column_base + at, 256), 256)
            part = hidden[:, columns].astype(F32)
            grads = []
            for pair in range(2):
                shift = jnp.where(
                    xh == 0, total[pair, :, q * HEAD : (q + 1) * HEAD].astype(F32), 0.0
                )
                current = part + jnp.concatenate([shift, shift], axis=1)
                slope = slopes[:, pair * 64 : pair * 64 + 1]
                grads.append(
                    lax.dot_general(
                        scaled[pair],
                        weight[pair * 16 + block],
                        (((1,), (1,)), ((), ())),
                        preferred_element_type=F32,
                    )
                    - current * slope
                )
            odd[:, pl.ds(at, 256)] = grads[1].astype(BF16)
            pair_send[:, pl.ds(at, 256)] = (grads[0] + grads[1]).astype(BF16)
            return carry

        lax.fori_loop(0, 4, step, 0)

        @pl.when(y >= 1)
        def _():
            for step in range(1, 4):
                transfer(*pair_copy(q, step))

    def suffix(q):
        columns = pl.ds(q * quarter, quarter)
        for step in range(1, 4):
            from_y = (y + step) % 4

            @pl.when(from_y >= 1)
            def _():
                arrive(pair_recv.at[from_y, :, columns], pair_sem.at[from_y * 4 + q])

        @pl.when(y >= 1)
        def _():
            pair_recv[y, :, columns] = pair_send[rows, columns]

        running = pair_recv[3, :, columns].astype(F32)
        later_send[2, :, columns] = running.astype(BF16)
        running += pair_recv[2, :, columns].astype(F32)
        later_send[1, :, columns] = running.astype(BF16)
        running += pair_recv[1, :, columns].astype(F32)
        later_send[0, :, columns] = running.astype(BF16)
        for step in range(1, 4):
            to_y = (y + step) % 4

            @pl.when(to_y < 3)
            def _():
                transfer(*later_copy(q, step))

        @pl.when(y < 3)
        def _():
            later[rows, columns] = later_send[y, :, columns]

        @pl.when(y == 3)
        def _():
            later[:, columns] = jnp.zeros((128, quarter), BF16)

    def finish(q):
        @pl.when(y < 3)
        def _():
            for step in range(1, 4):
                from_y = (y + step) % 4
                target = later.at[pl.ds(from_y * 32, 32), pl.ds(q * quarter, quarter)]
                arrive(target, later_sem.at[from_y * 4 + q])

        def step(index, carry):
            at = pl.multiple_of(q * quarter + index * 256, 256)
            columns = pl.ds(at, 256)
            own_columns = pl.ds(pl.multiple_of(column_base + at, 256), 256)
            start = cotangent[:, own_columns].astype(F32) + later[:, columns].astype(F32)
            even_grad = (start + pair_send[:, columns].astype(F32)).astype(BF16)
            odd_grad = (start + odd[:, columns].astype(F32)).astype(BF16)
            out[:, own_columns] = jnp.where(xh == 0, even_grad, odd_grad)
            other_send[:, columns] = jnp.where(xh == 0, odd_grad, even_grad)
            return carry

        lax.fori_loop(0, 4, step, 0)
        pending.append(transfer(*other_copy(q)))

    def adapter_setup():
        low = lax.dot_general(
            raised[...], scaled[xh], (((0,), (1,)), ((), ())), preferred_element_type=F32
        )
        return (adapter_scale * low).astype(BF16)

    def current_columns(block):
        columns = pl.ds(pl.multiple_of(block * 256, 256), 256)
        part = hidden[:, columns].astype(F32)
        head = jnp.minimum(block // 4, KV_HEADS - 1)
        shift = total[xh, :, pl.ds(pl.multiple_of(head * HEAD, HEAD), HEAD)].astype(F32)
        shift = jnp.where(block < 16, shift, 0.0)
        return (part + jnp.concatenate([shift, shift], axis=1)).astype(BF16)

    low = adapter_setup_holder = None

    def adapter_narrow(block, carry):
        current = current_columns(block)
        rows_at = pl.ds(pl.multiple_of(block * 256, 256), 256)
        return carry + jnp.dot(current, gained[rows_at], preferred_element_type=F32)

    def adapter_up():
        total_narrow = lax.fori_loop(0, 32, adapter_narrow, jnp.zeros((128, 64), F32))
        narrow[...] = total_narrow.astype(BF16)
        up_grad = adapter_scale * lax.dot_general(
            scaled[xh], narrow[...], (((0,), (0,)), ((), ())), preferred_element_type=F32
        )
        padded = jnp.concatenate([up_grad, jnp.zeros((KVW, 192), F32)], axis=1)
        grad_send[:, 64:] = padded.astype(BF16).reshape(32, 16, 256)

    def adapter_down(low):
        def step(block, carry):
            grad = jnp.dot(low, current_columns(block), preferred_element_type=F32)
            grad_send[block, :64] = grad.astype(BF16)
            return carry

        lax.fori_loop(0, 32, step, 0)

    def grad_copy(step):
        to = (place + step) % 32
        return (
            grad_send.at[to],
            grad_recv.at[place],
            grad_sem.at[place],
            device(section, to),
            grad_send_sem.at[step],
        )

    def send_grads(step, carry):
        transfer(*grad_copy(step))
        return carry

    for q in range(4):
        hidden_gradients(q)
    suffix(0)
    suffix(1)
    adapter_up()
    suffix(2)
    finish(0)
    suffix(3)
    finish(1)
    adapter_down(adapter_setup())
    lax.fori_loop(1, 32, send_grads, 0)
    finish(2)
    finish(3)
    grad_recv[place] = grad_send[place]

    def await_grads(step, carry):
        sender = (place + 32 - step) % 32
        arrive(grad_recv.at[sender], grad_sem.at[sender])
        return carry

    lax.fori_loop(1, 32, await_grads, 0)

    def sum_grads(index, carry):
        return carry + grad_recv[index].astype(F32)

    grad_out[...] = lax.fori_loop(0, 32, sum_grads, jnp.zeros((80, 256), F32))
    for q in range(4):
        columns = pl.ds(
            pl.multiple_of((1 - xh) * half_width + q * quarter, quarter), quarter
        )
        arrive(out.at[:, columns], other_sem.at[q])

    def gone(copy):
        source, target, arrival, to, sem = copy
        pltpu.make_async_remote_copy(
            src_ref=source,
            dst_ref=target,
            send_sem=sem,
            recv_sem=arrival,
            device_id=to,
            device_id_type=pl.DeviceIdType.MESH,
        ).wait_send()

    for copy in pending:
        copy.wait_send()

    @pl.when(xl != xh)
    def _():
        for h in range(2):
            gone(
                (
                    shard.at[pl.ds(h * 128, 128)],
                    half(swapped_place, h),
                    weight_sem.at[swapped_place * 2 + h],
                    swap,
                    local_sem.at[3 + h],
                )
            )

    @pl.when(xh == 0)
    def _():
        for index in range(8):
            block, sem, to = mix_moves[index]
            gone((block, block, mix_sem.at[sem], to, send_sem.at[mix_base + index]))
        for step in range(4):
            for column in range(2):
                if step or column:
                    for copy in reply_copies(step, column):
                        gone(copy)

    @pl.when(xh == 1)
    def _():
        gone(
            (
                product_send.at[:, pl.ds(y * 32, 32)],
                product_recv.at[section],
                product_sem.at[section],
                (2 * y, place),
                send_sem.at[product_base],
            )
        )

    @pl.when(y >= 1)
    def _():
        for q in range(4):
            for step in range(1, 4):
                gone(pair_copy(q, step))

    for step in range(1, 4):

        @pl.when((y + step) % 4 < 3)
        def _():
            for q in range(4):
                gone(later_copy(q, step))

    def grads_gone(step, carry):
        gone(grad_copy(step))
        return carry

    lax.fori_loop(1, 32, grads_gone, 0)
    assert used[0] <= SENDS, used


SENDS = 256


def shards(
    codes,
    scale_codes,
    second_scales,
    gains,
    down_adapter,
    up_projection_weight,
    hidden_in,
    cotangent,
):
    place = lax.axis_index("fsdp")
    gain = gains[0].astype(F32)
    down = down_adapter[0]
    raised = up_projection_weight[0]
    tokens, width = hidden_in.shape
    own_rows = codes.shape[1]

    base = dequantize_shard(codes[0], scale_codes[0], second_scales[0])
    down_rows = lax.dynamic_slice_in_dim(down, place * own_rows, own_rows, 0)
    gain_rows = lax.dynamic_slice_in_dim(gain, place * own_rows, own_rows, 0)
    low = jnp.dot(down_rows, raised.T, preferred_element_type=F32)
    shard = ((base.astype(F32) + adapter_scale * low) * gain_rows[:, None]).astype(BF16)
    gained = (down.astype(F32) * gain[:, None]).astype(BF16)
    vmem = pl.BlockSpec(memory_space=pltpu.VMEM)
    hbm = pl.BlockSpec(memory_space=pl.ANY)
    dma = pltpu.SemaphoreType.DMA
    input_grad, grads = pl.pallas_call(
        functools.partial(chip_kernel, width),
        out_shape=(
            jax.ShapeDtypeStruct((tokens, width), BF16),
            jax.ShapeDtypeStruct((80, 256), F32),
        ),
        in_specs=[vmem, hbm, hbm, hbm, vmem],
        out_specs=(vmem, vmem),
        scratch_shapes=[
            pltpu.VMEM((32, 256, KVW), BF16),
            pltpu.VMEM((8, KVW, KVW), BF16),
            pltpu.VMEM((tokens, width), BF16),
            pltpu.VMEM((tokens, width), BF16),
            pltpu.VMEM((width, 64), BF16),
            pltpu.VMEM((2, tokens, KVW), F32),
            pltpu.VMEM((2, tokens, KVW), BF16),
            pltpu.VMEM((8, 2, 32, KVW), BF16),
            pltpu.VMEM((32, KVW), F32),
            pltpu.VMEM((32, KVW), F32),
            pltpu.VMEM((32, HEAD), F32),
            pltpu.VMEM((8, 32, KVW), F32),
            pltpu.VMEM((8, 32, KVW), F32),
            pltpu.VMEM((8, 32, HEAD), F32),
            pltpu.VMEM((8, 32, KVW), BF16),
            pltpu.VMEM((8, 32, KVW), BF16),
            pltpu.VMEM((4, 32, HEAD), F32),
            pltpu.VMEM((2, tokens, KVW), BF16),
            pltpu.VMEM((2, tokens, KVW), BF16),
            pltpu.VMEM((tokens, HEAD), F32),
            pltpu.VMEM((tokens, width // 2), BF16),
            pltpu.VMEM((tokens, width // 2), BF16),
            pltpu.VMEM((4, 32, width // 2), BF16),
            pltpu.VMEM((3, 32, width // 2), BF16),
            pltpu.VMEM((tokens, width // 2), BF16),
            pltpu.VMEM((tokens, width // 2), BF16),
            pltpu.VMEM((32, 80, 256), BF16),
            pltpu.VMEM((32, 80, 256), BF16),
            pltpu.VMEM((tokens, 64), BF16),
            dma((5,)),
            dma((SENDS,)),
            dma((64,)),
            dma((8,)),
            dma((8,)),
            dma((12,)),
            dma((16,)),
            dma((16,)),
            dma((4,)),
            dma((32,)),
            dma((32,)),
        ],
        compiler_params=pltpu.CompilerParams(
            collective_id=0, has_side_effects=True, vmem_limit_bytes=58 * 2**20
        ),
        name="relay",
    )(shard, hidden_in, cotangent, gained, raised)
    down_grad = grads[:64].T * gain_rows[:, None]
    return (input_grad[None], down_grad[None], grads[None, 64:, :64])


def solution(mesh):
    return jax.shard_map(
        shards,
        mesh=mesh,
        in_specs=(
            P("section", "fsdp", None),
            P("section", "fsdp", None),
            P("section", "fsdp"),
            P("section", None),
            P("section", None, None),
            P("section", None, None),
            P("fsdp", None),
            P("fsdp", None),
        ),
        out_specs=(
            P("section", "fsdp", None),
            P("section", "fsdp", None),
            P("section", "fsdp", None),
        ),
        check_vma=False,
    )
```

```python
import functools

import jax
import jax.numpy as jnp
from jax import lax
from jax.experimental import pallas as pl
from jax.experimental.pallas import tpu as pltpu
from jax.sharding import PartitionSpec as P

HEAD = 128
GROUP = 8
KV_HEADS = 4
KVW = KV_HEADS * HEAD
BLOCK = 64
SROWS = 32

NF4_TABLE = (
    -1.0,
    -0.6961928009986877,
    -0.5250730514526367,
    -0.39491748809814453,
    -0.28444138169288635,
    -0.18477343022823334,
    -0.09105003625154495,
    0.0,
    0.07958029955625534,
    0.16093020141124725,
    0.24611230194568634,
    0.33791524171066284,
    0.44070982933044434,
    0.5626170039176941,
    0.7229568362236023,
    1.0,
)
adapter_scale = 0.5
epsilon = 1e-05
F32 = jnp.float32
BF16 = jnp.bfloat16


def chip_kernel(
    width,
    codes_hbm,
    scale_codes,
    second_scales,
    gains,
    down_hbm,
    raised,
    hidden_hbm,
    cotangent_hbm,
    out,
    down_out,
    up_out,
    weight,
    mixes,
    codes,
    shard,
    quad_send,
    quad_recv,
    hidden,
    cotangent,
    down,
    product,
    product_send,
    product_recv,
    folded,
    descent,
    squares,
    totals,
    values,
    inverses,
    scaled_send,
    total_send,
    slope_send,
    scaled,
    total,
    shifts,
    slopes,
    pair_send,
    odd,
    pair_recv,
    later_send,
    later,
    other_send,
    grad_send,
    grad_mate,
    grad_sum,
    grad_recv,
    narrow,
    local_sem,
    send_sem,
    weight_sem,
    quad_sem,
    depth_sem,
    mix_sem,
    product_sem,
    reply_sem,
    pair_sem,
    later_sem,
    other_sem,
    grad_send_sem,
    grad_sem,
):
    section = lax.axis_index("section")
    place = lax.axis_index("fsdp")
    y, xh = section // 2, section % 2
    xl, z, core = place // 16, (place // 2) % 8, place % 2
    half_width = width // 2
    column_base = xh * half_width
    layers = 2 * 4

    def device(to_section, to_place):
        return (to_section, to_place)

    mate = device(section, 2 * (place // 2) + 1 - core)
    across = device(section, (place + 16) % 32)
    above = device(section, xl * 16 + ((z + 1) % 8) * 2 + core)
    below = device(section, xl * 16 + ((z + 7) % 8) * 2 + core)
    twin = 2 * y + 1 - xh
    swap = device(twin, (place + 16) % 32)
    used = [0]

    def transfer(source, target, arrival, to, sem=None):
        if sem is None:
            sem = send_sem.at[used[0]]
            used[0] += 1
        copy = pltpu.make_async_remote_copy(
            src_ref=source,
            dst_ref=target,
            send_sem=sem,
            recv_sem=arrival,
            device_id=to,
            device_id_type=pl.DeviceIdType.MESH,
        )
        copy.start()
        return copy

    def arrive(target, arrival):
        pltpu.make_async_remote_copy(
            src_ref=target,
            dst_ref=target,
            send_sem=send_sem.at[0],
            recv_sem=arrival,
            device_id=mate,
            device_id_type=pl.DeviceIdType.MESH,
        ).wait_recv()

    loads = [
        pltpu.make_async_copy(hidden_hbm, hidden, local_sem.at[0]),
        pltpu.make_async_copy(cotangent_hbm, cotangent, local_sem.at[1]),
        pltpu.make_async_copy(down_hbm, down, local_sem.at[2]),
        pltpu.make_async_copy(codes_hbm, codes, local_sem.at[5]),
    ]
    for load in reversed(loads):
        load.start()

    barrier = pltpu.get_barrier_semaphore()

    def greet(to):
        pl.semaphore_signal(
            barrier, inc=1, device_id=to, device_id_type=pl.DeviceIdType.MESH
        )

    def greet_place(step, carry):
        greet(device(section, (place + step) % 32))
        return carry

    lax.fori_loop(1, 32, greet_place, 0)
    for step in range(1, layers):
        greet(device((section + step) % 8, place))
    greet(swap)

    loads[3].wait()
    loads[2].wait()
    own_features = pl.ds(pl.multiple_of(place * 256, 256), 256)
    lane = lax.broadcasted_iota(jnp.int32, (8, 256), 1)
    outer = jnp.full((8, 256), second_scales[0, 0], F32)
    for group in range(1, 8):
        outer = jnp.where(lane >= group * SROWS, second_scales[0, group], outer)
    block_scale = outer * (scale_codes[...].astype(F32) + 1.0) / 256.0
    gain_lanes = jnp.broadcast_to(gains[:, own_features].astype(F32), (120, 256))
    columns_of = jnp.concatenate([block_scale, gain_lanes], axis=0).T
    side = lax.broadcasted_iota(jnp.int32, (256, HEAD), 1) < BLOCK
    low_rank = lax.dot_general(
        down[:, own_features], raised[...], (((0,), (0,)), ((), ())), preferred_element_type=F32
    )
    for tile in range(KV_HEADS):
        at = slice(tile * HEAD, (tile + 1) * HEAD)
        entries = codes[:, at]
        looked = jnp.full((256, HEAD), NF4_TABLE[0], F32)
        for entry in range(1, 16):
            looked = jnp.where(entries == entry, NF4_TABLE[entry], looked)
        left = columns_of[:, 2 * tile : 2 * tile + 1]
        right = columns_of[:, 2 * tile + 1 : 2 * tile + 2]
        base = (looked * jnp.where(side, left, right)).astype(BF16).astype(F32)
        rows_of = (base + adapter_scale * low_rank[:, at]) * columns_of[:, 8:9]
        shard[:, at] = rows_of.astype(BF16)
    pl.semaphore_wait(barrier, 31 + 7 + 1)

    pending = []

    def slot(x, depth, which):
        return x * 16 + depth * 2 + which

    def half(block, h):
        return weight.at[block, pl.ds(h * 128, 128)]

    def pass_on(block, h, to):
        pending.append(transfer(half(block, h), half(block, h), weight_sem.at[block * 2 + h], to))

    def await_block(block, h):
        arrive(half(block, h), weight_sem.at[block * 2 + h])

    swapped_place = (place + 16) % 32

    @pl.when(xl != xh)
    def _():
        for h in range(2):
            transfer(
                shard.at[pl.ds(h * 128, 128)],
                half(swapped_place, h),
                weight_sem.at[swapped_place * 2 + h],
                swap,
                local_sem.at[3 + h],
            )

    @pl.when(xl == xh)
    def _():
        pltpu.make_async_copy(shard, weight.at[place], local_sem.at[3]).start()

    loads[0].wait()
    loads[1].wait()
    rows = pl.ds(y * 32, 32)

    def fold(ref):
        for head in range(KV_HEADS):
            part = jnp.zeros((32, HEAD), F32)
            for member in range(GROUP):
                at = (head * GROUP + member) * HEAD
                part += ref[rows, pl.ds(at, HEAD)].astype(F32)
            yield head, part

    @pl.when(xl == xh)
    def _():
        pltpu.make_async_copy(shard, weight.at[place], local_sem.at[3]).wait()

    others = [place, slot(1 - xl, z, core)]

    mix_layer = 2 * y + xl
    quarter_at = (z % 2) * 2 + core
    fellows = (
        (quarter_at + 1 - 2 * core, mate),
        ((1 - z % 2) * 2 + core, device(section, xl * 16 + (z + 1 - 2 * (z % 2)) * 2 + core)),
        (
            (1 - z % 2) * 2 + 1 - core,
            device(section, xl * 16 + (z + 1 - 2 * (z % 2)) * 2 + 1 - core),
        ),
    )
    early_base = used[0]
    used[0] += 20
    y_up, y_down = (y + 1) % 4, (y + 3) % 4
    y_far = (y + 2) % 4

    def quad_copy(index):
        which, to = fellows[index]
        return (
            quad_send.at[which],
            quad_recv.at[quarter_at],
            quad_sem.at[quarter_at],
            to,
            send_sem.at[early_base + index],
        )

    def depth_copy(step):
        rows_at = mixes.at[mix_layer, z, core]
        to = device(section, xl * 16 + ((z + step) % 8) * 2 + core)
        return (rows_at, rows_at, depth_sem.at[z], to, send_sem.at[early_base + 2 + step])

    def mix_block(which_y, which, part=None):
        if part is None:
            return mixes.at[pl.ds(2 * which_y, 2), :, which]
        return mixes.at[pl.ds(2 * which_y, 2), pl.ds(part * 4, 4), which]

    mix_moves = (
        (mix_block(y, core), 0, (2 * y_up, place)),
        (mix_block(y, core), 1, (2 * y_down, place)),
        (mix_block(y_down, core, 0), 2, (2 * y_up, place)),
        (mix_block(y_up, core, 1), 3, (2 * y_down, place)),
        (mix_block(y_down, core), 4, mate),
        (mix_block(y_up, core), 5, mate),
        (mix_block(y_far, core, 0), 6, mate),
        (mix_block(y_far, core, 1), 7, mate),
        (mixes.at[mix_layer, :, core], 8, across),
        (mix_block(y, core), 9, mate),
    )

    def mix_copy(index):
        block, sem, to = mix_moves[index]
        return (block, block, mix_sem.at[sem], to, send_sem.at[early_base + 10 + index])

    def quad_start():
        own = weight[place, :128].astype(F32) + weight[place, 128:].astype(F32)
        quad_send[...] = own.astype(BF16).reshape(4, 32, KVW)
        for index in range(3):
            transfer(*quad_copy(index))

    def depth_start():
        summed = quad_send[quarter_at].astype(F32)
        for which, _ in fellows:
            arrive(quad_recv.at[which], quad_sem.at[which])
            summed += quad_recv[which].astype(F32)
        mixes[mix_layer, z, core] = summed.astype(BF16)
        for step in range(1, 8):
            transfer(*depth_copy(step))

    def across_start():
        for step in range(1, 8):
            at_z = (z + step) % 8
            arrive(mixes.at[mix_layer, at_z, core], depth_sem.at[at_z])
        transfer(*mix_copy(8))

    def ring_start():
        arrive(mixes.at[2 * y + 1 - xl, :, core], mix_sem.at[8])
        for index in (0, 1, 9):
            transfer(*mix_copy(index))

    for h in range(2):

        @pl.when(xl != xh)
        def _():
            await_block(place, h)

        if h == 0:
            pass_on(place, h, across)
        else:

            @pl.when(xh == 0)
            def _():
                quad_start()

        for to in (above, below, mate):
            pass_on(place, h, to)
    for head, part in fold(hidden):
        folded[:, head * HEAD : (head + 1) * HEAD] = part
    for head, part in fold(cotangent):
        descent[:, head * HEAD : (head + 1) * HEAD] = part
    square = jnp.zeros((32, HEAD), F32)
    for at in range(0, width, HEAD):
        piece = hidden[rows, pl.ds(at, HEAD)].astype(F32)
        square += piece * piece
    squares[...] = jnp.broadcast_to(jnp.sum(square, axis=1, keepdims=True), (32, HEAD))
    product[...] = jnp.zeros_like(product)

    await_block(others[1], 0)
    for to in (above, below, mate):
        pass_on(others[1], 0, to)

    @pl.when(xh == 0)
    def _():
        depth_start()

    def at_distance(distance):
        if distance == 0:
            return [z]
        if distance == 4:
            return [(z + 4) % 8]
        return [(z + 8 - distance) % 8, (z + distance) % 8]

    def multiply(distance, which):
        depths = len(at_distance(distance))

        def step(index, carry):
            x = index // depths
            depth = (z + 8 - distance + (index % depths) * 2 * distance) % 8
            block = slot(x, depth, which)
            columns = pl.ds(pl.multiple_of(column_base + (depth * 2 + which) * 256, 256), 256)
            product[x] += jnp.dot(hidden[:, columns], weight[block], preferred_element_type=F32)
            return carry

        lax.fori_loop(0, 2 * depths, step, 0)

    def relay_across(distance):
        for depth in at_distance(distance):
            block = slot(1 - xl, depth, core)
            await_block(block, 1)
            pass_on(block, 1, mate)

    def await_mate(distance):
        for depth in at_distance(distance):
            for x in range(2):
                for h in range(2):
                    await_block(slot(x, depth, 1 - core), h)

    for distance in range(1, 5):
        low, high = (z + 8 - distance) % 8, (z + distance) % 8
        for x, h, up_reach, down_reach in ((xl, 0, 4, 3), (1 - xl, 0, 3, 4), (xl, 1, 4, 3)):
            for depth, reach, onward in ((low, up_reach, above), (high, down_reach, below)):
                if distance > reach:
                    continue
                block = slot(x, depth, core)
                await_block(block, h)
                if distance < reach:
                    pass_on(block, h, onward)
                pass_on(block, h, mate)
                if h == 1:
                    pass_on(block, h, across)
        if distance == 1:
            pass_on(place, 1, across)
        if distance == 2:

            @pl.when(xh == 0)
            def _():
                across_start()

        if distance == 3:

            @pl.when(xh == 0)
            def _():
                ring_start()

        relay_across(distance - 1)
        multiply(distance - 1, core)
        if distance >= 2:
            await_mate(distance - 2)
            multiply(distance - 2, 1 - core)
    relay_across(4)
    multiply(4, core)
    for distance in (3, 4):
        await_mate(distance)
        multiply(distance, 1 - core)

    product_send[...] = product[...].astype(BF16)
    product_base = used[0]
    used[0] += 4

    def send_product(step):
        to_y = (y + step) % 4
        return transfer(
            product_send.at[:, pl.ds(to_y * 32, 32)],
            product_recv.at[section],
            product_sem.at[section],
            (2 * to_y, place),
            send_sem.at[product_base + step],
        )

    for step in range(1, 4):
        pending.append(send_product(step))

    @pl.when(xh == 1)
    def _():
        send_product(0)

    reply_base = used[0]
    used[0] += 24

    def reply_copies(step, to_column):
        to_y = (y + step) % 4
        to = (2 * to_y + to_column, place)
        at = reply_base + (step * 2 + to_column) * 3
        yield (
            scaled_send.at[pl.ds(2 * to_y, 2)],
            scaled.at[:, pl.ds(y * 32, 32)],
            reply_sem.at[y * 3],
            to,
            send_sem.at[at],
        )
        yield (
            slope_send.at[to_y],
            slopes.at[pl.ds(y * 32, 32)],
            reply_sem.at[y * 3 + 1],
            to,
            send_sem.at[at + 1],
        )
        if to_column == 0:
            yield (
                total_send.at[pl.ds(2 * to_y, 2)],
                total.at[:, pl.ds(y * 32, 32)],
                reply_sem.at[y * 3 + 2],
                to,
                send_sem.at[at + 2],
            )
        else:
            yield (
                total_send.at[2 * to_y + 1],
                total.at[1, pl.ds(y * 32, 32)],
                reply_sem.at[y * 3 + 2],
                to,
                send_sem.at[at + 2],
            )

    @pl.when(xh == 0)
    def _():
        product_recv[section] = product_send[:, rows]
        arrive(mix_block(y_down, core), mix_sem.at[0])
        transfer(*mix_copy(2))
        transfer(*mix_copy(4))
        arrive(mix_block(y_up, core), mix_sem.at[1])
        transfer(*mix_copy(3))
        transfer(*mix_copy(5))
        arrive(mix_block(y_far, core, 0), mix_sem.at[2])
        transfer(*mix_copy(6))
        arrive(mix_block(y_far, core, 1), mix_sem.at[3])
        transfer(*mix_copy(7))
        arrive(product_recv.at[section + 1], product_sem.at[section + 1])
        for step in range(1, 4):
            for column in range(2):
                sender = 2 * ((y + step) % 4) + column
                arrive(product_recv.at[sender], product_sem.at[sender])
        arrive(mix_block(y, 1 - core), mix_sem.at[9])
        arrive(mix_block(y_down, 1 - core), mix_sem.at[4])
        arrive(mix_block(y_up, 1 - core), mix_sem.at[5])
        arrive(mix_block(y_far, 1 - core, 0), mix_sem.at[6])
        arrive(mix_block(y_far, 1 - core, 1), mix_sem.at[7])

        square_sum = squares[:, :1]
        running = jnp.zeros((32, KVW), F32)
        for layer in range(layers):
            moved = 2.0 * folded[...] + GROUP * running
            energy = square_sum + jnp.sum(running * moved, axis=1, keepdims=True)
            inverse = 1.0 / jnp.sqrt(energy / width + epsilon)
            pair_at = layer - layer % 2
            mixed = product_recv[pair_at, layer % 2].astype(F32) + product_recv[
                pair_at + 1, layer % 2
            ].astype(F32)
            if layer:
                mixed += jnp.dot(
                    running.astype(BF16), mixes[layer].reshape(KVW, KVW), preferred_element_type=F32
                )
            value = mixed * inverse
            totals[layer] = running
            values[layer] = value
            inverses[layer] = jnp.broadcast_to(inverse, (32, HEAD))
            total_send[layer] = running.astype(BF16)
            running = running + value
        direction = descent[...]
        for layer in reversed(range(layers)):
            inverse = inverses[layer][:, :1]
            slope = (
                jnp.sum(direction * values[layer], axis=1, keepdims=True)
                / width
                * inverse
                * inverse
            )
            step_scaled = (direction * inverse).astype(BF16)
            scaled_send[layer] = step_scaled
            at = (layer % 2) * 64
            slope_send[layer // 2, :, at : at + 64] = jnp.broadcast_to(slope, (32, 64)).astype(
                BF16
            )
            if layer:
                direction = (
                    direction
                    + lax.dot_general(
                        step_scaled,
                        mixes[layer].reshape(KVW, KVW),
                        (((1,), (1,)), ((), ())),
                        preferred_element_type=F32,
                    )
                    - (folded[...] + GROUP * totals[layer]) * slope
                )
        for item in range(3):
            for step in (1, 2, 3, 0):
                for column in range(2):
                    if step == 0 and column == 0:
                        continue
                    transfer(*list(reply_copies(step, column))[item])
        scaled[:, rows] = scaled_send[pl.ds(2 * y, 2)]
        total[:, rows] = total_send[pl.ds(2 * y, 2)]
        slopes[rows] = slope_send[y]

    def await_reply(step):
        from_y = (y + step) % 4
        token_rows = pl.ds(from_y * 32, 32)
        arrive(scaled.at[:, token_rows], reply_sem.at[from_y * 3])
        arrive(slopes.at[token_rows], reply_sem.at[from_y * 3 + 1])

        @pl.when(xh == 0)
        def _():
            arrive(total.at[:, token_rows], reply_sem.at[from_y * 3 + 2])

    for step in range(1, 4):
        await_reply(step)

    @pl.when(xh == 1)
    def _():
        await_reply(0)
        shifts[...] = jnp.zeros_like(shifts)

    @pl.when(xh == 0)
    def _():
        shifts[...] = total[...]

    pair_base = used[0]
    used[0] += 28
    quarter = half_width // 4

    def pair_copy(q, step):
        to_y = (y + step) % 4
        columns = pl.ds(q * quarter, quarter)
        return (
            pair_send.at[pl.ds(to_y * 32, 32), columns],
            pair_recv.at[y, :, columns],
            pair_sem.at[y * 4 + q],
            (2 * to_y + xh, place),
            send_sem.at[pair_base + q * 3 + step - 1],
        )

    def later_copy(q, step):
        to_y = (y + step) % 4
        columns = pl.ds(q * quarter, quarter)
        return (
            later_send.at[to_y, :, columns],
            later.at[pl.ds(y * 32, 32), columns],
            later_sem.at[y * 4 + q],
            (2 * to_y + xh, place),
            send_sem.at[pair_base + 12 + q * 3 + step - 1],
        )

    def other_copy(q):
        return (
            other_send.at[:, pl.ds(q * quarter, quarter)],
            out.at[:, pl.ds(pl.multiple_of(column_base + q * quarter, quarter), quarter)],
            other_sem.at[q],
            (twin, place),
            send_sem.at[pair_base + 24 + q],
        )

    def hidden_gradients(q):
        def step(index, carry):
            block = q * 4 + index
            at = pl.multiple_of(block * 256, 256)
            columns = pl.ds(pl.multiple_of(column_base + at, 256), 256)
            part = hidden[:, columns].astype(F32)
            grads = []
            for pair in range(2):
                shift = shifts[pair, :, q * HEAD : (q + 1) * HEAD].astype(F32)
                current = part + jnp.concatenate([shift, shift], axis=1)
                slope = slopes[:, pair * 64 : pair * 64 + 1].astype(F32)
                grads.append(
                    lax.dot_general(
                        scaled[pair],
                        weight[pair * 16 + block],
                        (((1,), (1,)), ((), ())),
                        preferred_element_type=F32,
                    )
                    - current * slope
                )
            odd[:, pl.ds(at, 256)] = grads[1].astype(BF16)
            pair_send[:, pl.ds(at, 256)] = (grads[0] + grads[1]).astype(BF16)
            return carry

        lax.fori_loop(0, 4, step, 0)

        @pl.when(y >= 1)
        def _():
            for step in range(1, 4):
                transfer(*pair_copy(q, step))

    def suffix(q):
        columns = pl.ds(q * quarter, quarter)
        for step in range(1, 4):
            from_y = (y + step) % 4

            @pl.when(from_y >= 1)
            def _():
                arrive(pair_recv.at[from_y, :, columns], pair_sem.at[from_y * 4 + q])

        @pl.when(y >= 1)
        def _():
            pair_recv[y, :, columns] = pair_send[rows, columns]

        running = pair_recv[3, :, columns].astype(F32)
        later_send[2, :, columns] = running.astype(BF16)
        running += pair_recv[2, :, columns].astype(F32)
        later_send[1, :, columns] = running.astype(BF16)
        running += pair_recv[1, :, columns].astype(F32)
        later_send[0, :, columns] = running.astype(BF16)
        for step in range(1, 4):
            to_y = (y + step) % 4

            @pl.when(to_y < 3)
            def _():
                transfer(*later_copy(q, step))

        @pl.when(y < 3)
        def _():
            later[rows, columns] = later_send[y, :, columns]

        @pl.when(y == 3)
        def _():
            later[:, columns] = jnp.zeros((128, quarter), BF16)

    def finish(q):
        @pl.when(y < 3)
        def _():
            for step in range(1, 4):
                from_y = (y + step) % 4
                target = later.at[pl.ds(from_y * 32, 32), pl.ds(q * quarter, quarter)]
                arrive(target, later_sem.at[from_y * 4 + q])

        def step(index, carry):
            at = pl.multiple_of(q * quarter + index * 256, 256)
            columns = pl.ds(at, 256)
            own_columns = pl.ds(pl.multiple_of(column_base + at, 256), 256)
            start = cotangent[:, own_columns].astype(F32) + later[:, columns].astype(F32)
            even_grad = (start + pair_send[:, columns].astype(F32)).astype(BF16)
            odd_grad = (start + odd[:, columns].astype(F32)).astype(BF16)
            out[:, own_columns] = jnp.where(xh == 0, even_grad, odd_grad)
            other_send[:, columns] = jnp.where(xh == 0, odd_grad, even_grad)
            return carry

        lax.fori_loop(0, 4, step, 0)
        pending.append(transfer(*other_copy(q)))

    def await_totals():
        for from_y in range(4):
            arrive(total.at[1, pl.ds(from_y * 32, 32)], reply_sem.at[from_y * 3 + 2])

    def adapter_low():
        low = lax.dot_general(
            raised[...], scaled[xh], (((1,), (1,)), ((), ())), preferred_element_type=F32
        )
        return (adapter_scale * low).astype(BF16)

    def adapter_part(low, first, carry):
        def step(block, carry):
            columns = pl.ds(pl.multiple_of(block * 512, 512), 512)
            part = hidden[:, columns].astype(F32)
            if first < 8:
                at = pl.ds(pl.multiple_of((block // 2) * HEAD, HEAD), HEAD)
                shift = total[xh, :, at].astype(F32)
                part += jnp.concatenate([shift, shift, shift, shift], axis=1)
            grad = jnp.dot(low, part.astype(BF16), preferred_element_type=F32).astype(BF16)
            grad_send[block, 0, :64] = grad[:, :256]
            grad_send[block, 1, :64] = grad[:, 256:]
            gained = (part * gains[:, columns].astype(F32)).astype(BF16)
            return carry + lax.dot_general(
                gained, down[:, columns], (((1,), (1,)), ((), ())), preferred_element_type=F32
            )

        return lax.fori_loop(first, first + 8, step, carry)

    def adapter_up(carry):
        narrow[...] = carry.astype(BF16)
        up_grad = adapter_scale * lax.dot_general(
            scaled[xh], narrow[...], (((0,), (0,)), ((), ())), preferred_element_type=F32
        )
        padded = jnp.concatenate([up_grad, jnp.zeros((KVW, 192), F32)], axis=1)
        grad_send[:, :, 64:] = padded.astype(BF16).reshape(16, 2, 16, 256)

    def mate_copy():
        return (
            grad_send.at[:, 1 - core],
            grad_mate,
            grad_sem.at[16],
            mate,
            grad_send_sem.at[16],
        )

    seat = place // 2

    def grad_copy(step):
        to = (seat + step) % 16
        return (
            grad_sum.at[to],
            grad_recv.at[seat],
            grad_sem.at[seat],
            device(section, 2 * to + core),
            grad_send_sem.at[step],
        )

    def send_grads(step, carry):
        transfer(*grad_copy(step))
        return carry

    for q in range(4):
        hidden_gradients(q)
    suffix(0)
    suffix(1)

    @pl.when(xh == 1)
    def _():
        await_totals()

    low = adapter_low()
    carry = adapter_part(low, 0, jnp.zeros((128, 64), F32))
    suffix(2)
    suffix(3)
    finish(0)
    finish(1)
    adapter_up(adapter_part(low, 8, carry))
    transfer(*mate_copy())
    finish(2)
    finish(3)
    arrive(grad_mate, grad_sem.at[16])

    def sum_mate(index, carry):
        both = grad_send[index, core].astype(F32) + grad_mate[index].astype(F32)
        grad_sum[index] = both.astype(BF16)
        return carry

    lax.fori_loop(0, 16, sum_mate, 0)
    lax.fori_loop(1, 16, send_grads, 0)
    grad_recv[seat] = grad_sum[seat]

    def await_grads(step, carry):
        sender = (seat + 16 - step) % 16
        arrive(grad_recv.at[sender], grad_sem.at[sender])
        return carry

    lax.fori_loop(1, 16, await_grads, 0)

    def sum_grads(index, carry):
        return carry + grad_recv[index].astype(F32)

    summed = lax.fori_loop(0, 16, sum_grads, jnp.zeros((80, 256), F32))
    down_out[...] = summed[:64] * gains[:, own_features].astype(F32)
    up_out[...] = summed[64:, :64]
    for q in range(4):
        columns = pl.ds(
            pl.multiple_of((1 - xh) * half_width + q * quarter, quarter), quarter
        )
        arrive(out.at[:, columns], other_sem.at[q])

    def gone(copy):
        source, target, arrival, to, sem = copy
        pltpu.make_async_remote_copy(
            src_ref=source,
            dst_ref=target,
            send_sem=sem,
            recv_sem=arrival,
            device_id=to,
            device_id_type=pl.DeviceIdType.MESH,
        ).wait_send()

    for copy in pending:
        copy.wait_send()

    @pl.when(xl != xh)
    def _():
        for h in range(2):
            gone(
                (
                    shard.at[pl.ds(h * 128, 128)],
                    half(swapped_place, h),
                    weight_sem.at[swapped_place * 2 + h],
                    swap,
                    local_sem.at[3 + h],
                )
            )

    @pl.when(xh == 0)
    def _():
        for index in range(3):
            gone(quad_copy(index))
        for step in range(1, 8):
            gone(depth_copy(step))
        for index in range(10):
            gone(mix_copy(index))
        for step in range(4):
            for column in range(2):
                if step or column:
                    for copy in reply_copies(step, column):
                        gone(copy)

    @pl.when(xh == 1)
    def _():
        gone(
            (
                product_send.at[:, pl.ds(y * 32, 32)],
                product_recv.at[section],
                product_sem.at[section],
                (2 * y, place),
                send_sem.at[product_base],
            )
        )

    @pl.when(y >= 1)
    def _():
        for q in range(4):
            for step in range(1, 4):
                gone(pair_copy(q, step))

    for step in range(1, 4):

        @pl.when((y + step) % 4 < 3)
        def _():
            for q in range(4):
                gone(later_copy(q, step))

    def grads_gone(step, carry):
        gone(grad_copy(step))
        return carry

    lax.fori_loop(1, 16, grads_gone, 0)
    gone(mate_copy())
    assert used[0] <= SENDS, used


SENDS = 256


def shards(
    codes,
    scale_codes,
    second_scales,
    gains,
    down_adapter,
    up_projection_weight,
    hidden_in,
    cotangent,
):
    tokens, width = hidden_in.shape
    vmem = pl.BlockSpec(memory_space=pltpu.VMEM)
    smem = pl.BlockSpec(memory_space=pltpu.SMEM)
    hbm = pl.BlockSpec(memory_space=pl.ANY)
    dma = pltpu.SemaphoreType.DMA
    input_grad, down_grad, up_grad = pl.pallas_call(
        functools.partial(chip_kernel, width),
        out_shape=(
            jax.ShapeDtypeStruct((tokens, width), BF16),
            jax.ShapeDtypeStruct((64, 256), F32),
            jax.ShapeDtypeStruct((16, 64), F32),
        ),
        in_specs=[hbm, vmem, smem, vmem, hbm, vmem, hbm, hbm],
        out_specs=(vmem, vmem, vmem),
        scratch_shapes=[
            pltpu.VMEM((32, 256, KVW), BF16),
            pltpu.VMEM((8, 8, 2, 32, KVW), BF16),
            pltpu.VMEM((256, KVW), jnp.int32),
            pltpu.VMEM((256, KVW), BF16),
            pltpu.VMEM((4, 32, KVW), BF16),
            pltpu.VMEM((4, 32, KVW), BF16),
            pltpu.VMEM((tokens, width), BF16),
            pltpu.VMEM((tokens, width), BF16),
            pltpu.VMEM((64, width), BF16),
            pltpu.VMEM((2, tokens, KVW), F32),
            pltpu.VMEM((2, tokens, KVW), BF16),
            pltpu.VMEM((8, 2, 32, KVW), BF16),
            pltpu.VMEM((32, KVW), F32),
            pltpu.VMEM((32, KVW), F32),
            pltpu.VMEM((32, HEAD), F32),
            pltpu.VMEM((8, 32, KVW), F32),
            pltpu.VMEM((8, 32, KVW), F32),
            pltpu.VMEM((8, 32, HEAD), F32),
            pltpu.VMEM((8, 32, KVW), BF16),
            pltpu.VMEM((8, 32, KVW), BF16),
            pltpu.VMEM((4, 32, HEAD), BF16),
            pltpu.VMEM((2, tokens, KVW), BF16),
            pltpu.VMEM((2, tokens, KVW), BF16),
            pltpu.VMEM((2, tokens, KVW), BF16),
            pltpu.VMEM((tokens, HEAD), BF16),
            pltpu.VMEM((tokens, width // 2), BF16),
            pltpu.VMEM((tokens, width // 2), BF16),
            pltpu.VMEM((4, 32, width // 2), BF16),
            pltpu.VMEM((3, 32, width // 2), BF16),
            pltpu.VMEM((tokens, width // 2), BF16),
            pltpu.VMEM((tokens, width // 2), BF16),
            pltpu.VMEM((16, 2, 80, 256), BF16),
            pltpu.VMEM((16, 80, 256), BF16),
            pltpu.VMEM((16, 80, 256), BF16),
            pltpu.VMEM((16, 80, 256), BF16),
            pltpu.VMEM((tokens, 64), BF16),
            dma((6,)),
            dma((SENDS,)),
            dma((64,)),
            dma((4,)),
            dma((8,)),
            dma((10,)),
            dma((8,)),
            dma((12,)),
            dma((16,)),
            dma((16,)),
            dma((4,)),
            dma((17,)),
            dma((17,)),
        ],
        compiler_params=pltpu.CompilerParams(
            collective_id=0, has_side_effects=True, vmem_limit_bytes=48 * 2**20
        ),
        name="relay",
    )(
        codes[0],
        scale_codes[0].T,
        second_scales,
        gains,
        down_adapter[0].T,
        up_projection_weight[0].T,
        hidden_in,
        cotangent,
    )
    return (input_grad[None], down_grad.T[None], up_grad[None])


def solution(mesh):
    return jax.shard_map(
        shards,
        mesh=mesh,
        in_specs=(
            P("section", "fsdp", None),
            P("section", "fsdp", None),
            P("section", "fsdp"),
            P("section", None),
            P("section", None, None),
            P("section", None, None),
            P("fsdp", None),
            P("fsdp", None),
        ),
        out_specs=(
            P("section", "fsdp", None),
            P("section", "fsdp", None),
            P("section", "fsdp", None),
        ),
        check_vma=False,
    )
```

```python
import functools

import jax
import jax.numpy as jnp
from jax import lax
from jax.experimental import pallas as pl
from jax.experimental.pallas import tpu as pltpu
from jax.sharding import PartitionSpec as P

HEAD = 128
GROUP = 8
KV_HEADS = 4
KVW = KV_HEADS * HEAD
BLOCK = 64
SROWS = 32

NF4_TABLE = (
    -1.0,
    -0.6961928009986877,
    -0.5250730514526367,
    -0.39491748809814453,
    -0.28444138169288635,
    -0.18477343022823334,
    -0.09105003625154495,
    0.0,
    0.07958029955625534,
    0.16093020141124725,
    0.24611230194568634,
    0.33791524171066284,
    0.44070982933044434,
    0.5626170039176941,
    0.7229568362236023,
    1.0,
)
adapter_scale = 0.5
epsilon = 1e-05
F32 = jnp.float32
BF16 = jnp.bfloat16


def chip_kernel(
    width,
    codes_hbm,
    scale_hbm,
    second_scales,
    gains_hbm,
    down_hbm,
    raised_hbm,
    hidden_hbm,
    cotangent_hbm,
    out,
    down_out,
    up_out,
    weight,
    mixes,
    codes,
    scale_codes,
    gains,
    raised,
    shard,
    quad_send,
    quad_recv,
    hidden,
    cotangent,
    down,
    product,
    product_send,
    product_recv,
    folded,
    descent,
    squares,
    totals,
    values,
    inverses,
    scaled_send,
    total_send,
    slope_send,
    scaled,
    total,
    shifts,
    slopes,
    pair_send,
    odd,
    pair_recv,
    later_send,
    later,
    other_send,
    grad_send,
    grad_mate,
    grad_sum,
    grad_recv,
    narrow,
    local_sem,
    send_sem,
    weight_sem,
    quad_sem,
    depth_sem,
    mix_sem,
    product_sem,
    reply_sem,
    pair_sem,
    later_sem,
    other_sem,
    grad_send_sem,
    grad_sem,
):
    section = lax.axis_index("section")
    place = lax.axis_index("fsdp")
    y, xh = section // 2, section % 2
    xl, z, core = place // 16, (place // 2) % 8, place % 2
    half_width = width // 2
    column_base = xh * half_width
    layers = 2 * 4

    def device(to_section, to_place):
        return (to_section, to_place)

    mate = device(section, 2 * (place // 2) + 1 - core)
    across = device(section, (place + 16) % 32)
    above = device(section, xl * 16 + ((z + 1) % 8) * 2 + core)
    below = device(section, xl * 16 + ((z + 7) % 8) * 2 + core)
    twin = 2 * y + 1 - xh
    swap = device(twin, (place + 16) % 32)
    used = [0]

    def transfer(source, target, arrival, to, sem=None):
        if sem is None:
            sem = send_sem.at[used[0]]
            used[0] += 1
        copy = pltpu.make_async_remote_copy(
            src_ref=source,
            dst_ref=target,
            send_sem=sem,
            recv_sem=arrival,
            device_id=to,
            device_id_type=pl.DeviceIdType.MESH,
        )
        copy.start()
        return copy

    def arrive(target, arrival):
        pltpu.make_async_remote_copy(
            src_ref=target,
            dst_ref=target,
            send_sem=send_sem.at[0],
            recv_sem=arrival,
            device_id=mate,
            device_id_type=pl.DeviceIdType.MESH,
        ).wait_recv()

    loads = [
        pltpu.make_async_copy(hidden_hbm, hidden, local_sem.at[0]),
        pltpu.make_async_copy(cotangent_hbm, cotangent, local_sem.at[1]),
        pltpu.make_async_copy(down_hbm, down, local_sem.at[2]),
        pltpu.make_async_copy(codes_hbm, codes, local_sem.at[5]),
        pltpu.make_async_copy(scale_hbm, scale_codes, local_sem.at[6]),
        pltpu.make_async_copy(gains_hbm, gains, local_sem.at[7]),
        pltpu.make_async_copy(raised_hbm, raised, local_sem.at[8]),
    ]
    for load in reversed(loads):
        load.start()

    barrier = pltpu.get_barrier_semaphore()

    def greet(to):
        pl.semaphore_signal(
            barrier, inc=1, device_id=to, device_id_type=pl.DeviceIdType.MESH
        )

    def greet_place(step, carry):
        greet(device(section, (place + step) % 32))
        return carry

    lax.fori_loop(1, 32, greet_place, 0)
    for step in range(1, layers):
        greet(device((section + step) % 8, place))
    greet(swap)

    for load in loads[2:]:
        load.wait()
    own_features = pl.ds(pl.multiple_of(place * 256, 256), 256)
    lane = lax.broadcasted_iota(jnp.int32, (8, 256), 1)
    outer = jnp.full((8, 256), second_scales[0, 0], F32)
    for group in range(1, 8):
        outer = jnp.where(lane >= group * SROWS, second_scales[0, group], outer)
    block_scale = outer * (scale_codes[...].astype(F32) + 1.0) / 256.0
    gain_lanes = jnp.broadcast_to(gains[:, own_features].astype(F32), (120, 256))
    columns_of = jnp.concatenate([block_scale, gain_lanes], axis=0).T
    side = lax.broadcasted_iota(jnp.int32, (256, HEAD), 1) < BLOCK
    low_rank = lax.dot_general(
        down[:, own_features], raised[...], (((0,), (0,)), ((), ())), preferred_element_type=F32
    )
    for tile in range(KV_HEADS):
        at = slice(tile * HEAD, (tile + 1) * HEAD)
        entries = codes[:, at]
        looked = jnp.full((256, HEAD), NF4_TABLE[0], F32)
        for entry in range(1, 16):
            looked = jnp.where(entries == entry, NF4_TABLE[entry], looked)
        left = columns_of[:, 2 * tile : 2 * tile + 1]
        right = columns_of[:, 2 * tile + 1 : 2 * tile + 2]
        base = (looked * jnp.where(side, left, right)).astype(BF16).astype(F32)
        rows_of = (base + adapter_scale * low_rank[:, at]) * columns_of[:, 8:9]
        shard[:, at] = rows_of.astype(BF16)
    pl.semaphore_wait(barrier, 31 + 7 + 1)

    quarter_at = (z % 2) * 2 + core
    fellows = (
        (quarter_at + 1 - 2 * core, mate),
        ((1 - z % 2) * 2 + core, device(section, xl * 16 + (z + 1 - 2 * (z % 2)) * 2 + core)),
        (
            (1 - z % 2) * 2 + 1 - core,
            device(section, xl * 16 + (z + 1 - 2 * (z % 2)) * 2 + 1 - core),
        ),
    )
    early_base = used[0]
    used[0] += 24
    y_up, y_down = (y + 1) % 4, (y + 3) % 4
    y_far = (y + 2) % 4

    def quad_copy(index):
        which, to = fellows[index]
        return (
            quad_send.at[which],
            quad_recv.at[quarter_at],
            quad_sem.at[quarter_at],
            to,
            send_sem.at[early_base + index],
        )

    def depth_copy(step):
        rows_at = mixes.at[section, z, core]
        to = device(section, xl * 16 + ((z + step) % 8) * 2 + core)
        return (rows_at, rows_at, depth_sem.at[z], to, send_sem.at[early_base + 2 + step])

    def mix_block(which_y, which, part=None):
        if part is None:
            return mixes.at[pl.ds(2 * which_y, 2), :, which]
        return mixes.at[pl.ds(2 * which_y, 2), pl.ds(part * 4, 4), which]

    mix_moves = (
        (mix_block(y, core), 0, (2 * y_up + xh, place)),
        (mix_block(y, core), 1, (2 * y_down + xh, place)),
        (mix_block(y_down, core, 0), 2, (2 * y_up + xh, place)),
        (mix_block(y_up, core, 1), 3, (2 * y_down + xh, place)),
        (mix_block(y_down, core), 4, mate),
        (mix_block(y_up, core), 5, mate),
        (mix_block(y_far, core, 0), 6, mate),
        (mix_block(y_far, core, 1), 7, mate),
        (mixes.at[section, :, core], 8, across),
        (mix_block(y, core), 9, mate),
        (mixes.at[section, :, core], 10, swap),
        (mixes.at[twin, :, core], 11, across),
    )

    def mix_copy(index):
        block, sem, to = mix_moves[index]
        return (block, block, mix_sem.at[sem], to, send_sem.at[early_base + 10 + index])

    def quad_start():
        own = shard[:128].astype(F32) + shard[128:].astype(F32)
        quad_send[...] = own.astype(BF16).reshape(4, 32, KVW)
        for index in range(3):
            transfer(*quad_copy(index))

    def depth_start():
        summed = quad_send[quarter_at].astype(F32)
        for which, _ in fellows:
            arrive(quad_recv.at[which], quad_sem.at[which])
            summed += quad_recv[which].astype(F32)
        mixes[section, z, core] = summed.astype(BF16)
        for step in range(1, 8):
            transfer(*depth_copy(step))

    def across_start():
        @pl.when(xl == 0)
        def _():
            for step in range(1, 8):
                at_z = (z + step) % 8
                arrive(mixes.at[section, at_z, core], depth_sem.at[at_z])
            transfer(*mix_copy(8))
            transfer(*mix_copy(10))

    def across_more():
        @pl.when(xl == 1)
        def _():
            arrive(mixes.at[twin, :, core], mix_sem.at[10])
            transfer(*mix_copy(11))
            arrive(mixes.at[section, :, core], mix_sem.at[8])

    def ring_start():
        @pl.when(xl == 0)
        def _():
            arrive(mixes.at[twin, :, core], mix_sem.at[11])

        for index in (0, 1, 9):
            transfer(*mix_copy(index))

    @pl.when(xl == 0)
    def _():
        quad_start()

    pending = []

    def slot(x, depth, which):
        return x * 16 + depth * 2 + which

    def half(block, h):
        return weight.at[block, pl.ds(h * 128, 128)]

    def pass_on(block, h, to):
        pending.append(transfer(half(block, h), half(block, h), weight_sem.at[block * 2 + h], to))

    def await_block(block, h):
        arrive(half(block, h), weight_sem.at[block * 2 + h])

    swapped_place = (place + 16) % 32

    @pl.when(xl != xh)
    def _():
        for h in range(2):
            transfer(
                shard.at[pl.ds(h * 128, 128)],
                half(swapped_place, h),
                weight_sem.at[swapped_place * 2 + h],
                swap,
                local_sem.at[3 + h],
            )

    @pl.when(xl == xh)
    def _():
        pltpu.make_async_copy(shard, weight.at[place], local_sem.at[3]).start()

    rows = pl.ds(y * 32, 32)
    chain_rows = pl.ds(section * 16, 16)

    def fold(ref):
        for head in range(KV_HEADS):
            part = jnp.zeros((16, HEAD), F32)
            for member in range(GROUP):
                at = (head * GROUP + member) * HEAD
                part += ref[chain_rows, pl.ds(at, HEAD)].astype(F32)
            yield head, part

    @pl.when(xl == xh)
    def _():
        pltpu.make_async_copy(shard, weight.at[place], local_sem.at[3]).wait()

    others = [place, slot(1 - xl, z, core)]

    for h in range(2):

        @pl.when(xl != xh)
        def _():
            await_block(place, h)

        if h == 0:
            pass_on(place, h, across)
        for to in (above, below, mate):
            pass_on(place, h, to)

    @pl.when(xl == 0)
    def _():
        depth_start()

    loads[0].wait()
    loads[1].wait()
    for head, part in fold(hidden):
        folded[:, head * HEAD : (head + 1) * HEAD] = part
    for head, part in fold(cotangent):
        descent[:, head * HEAD : (head + 1) * HEAD] = part
    square = jnp.zeros((16, HEAD), F32)
    for at in range(0, width, HEAD):
        piece = hidden[chain_rows, pl.ds(at, HEAD)].astype(F32)
        square += piece * piece
    squares[...] = jnp.broadcast_to(jnp.sum(square, axis=1, keepdims=True), (16, HEAD))
    product[...] = jnp.zeros_like(product)

    await_block(others[1], 0)
    for to in (above, below, mate):
        pass_on(others[1], 0, to)


    def at_distance(distance):
        if distance == 0:
            return [z]
        if distance == 4:
            return [(z + 4) % 8]
        return [(z + 8 - distance) % 8, (z + distance) % 8]

    def multiply(distance, which):
        depths = len(at_distance(distance))

        def step(index, carry):
            x = index // depths
            depth = (z + 8 - distance + (index % depths) * 2 * distance) % 8
            block = slot(x, depth, which)
            columns = pl.ds(pl.multiple_of(column_base + (depth * 2 + which) * 256, 256), 256)
            product[x] += jnp.dot(hidden[:, columns], weight[block], preferred_element_type=F32)
            return carry

        lax.fori_loop(0, 2 * depths, step, 0)

    def relay_across(distance):
        for depth in at_distance(distance):
            block = slot(1 - xl, depth, core)
            await_block(block, 1)
            pass_on(block, 1, mate)

    def await_mate(distance):
        for depth in at_distance(distance):
            for x in range(2):
                for h in range(2):
                    await_block(slot(x, depth, 1 - core), h)

    for distance in range(1, 5):
        low, high = (z + 8 - distance) % 8, (z + distance) % 8
        for x, h, up_reach, down_reach in ((xl, 1, 3, 3), (xl, 0, 4, 3), (1 - xl, 0, 3, 4)):
            for depth, reach, onward in ((low, up_reach, above), (high, down_reach, below)):
                if distance > reach:
                    continue
                block = slot(x, depth, core)
                await_block(block, h)
                if distance < reach:
                    pass_on(block, h, onward)
                pass_on(block, h, mate)
                if h == 1:
                    pass_on(block, h, across)
            if distance == 3 and h == 1:
                ends = slot(xl, low + (high - low) * core, core)
                pass_on(ends, 1, device(section, xl * 16 + ((z + 1 + 6 * core) % 8) * 2 + core))
            if distance == 4 and h == 1:
                await_block(slot(x, low, core), 1)
                pass_on(slot(x, low, core), 1, across)
                pass_on(slot(x, low, core), 1, mate)
        if distance == 1:
            pass_on(place, 1, across)
        if distance == 1:
            across_start()
        if distance == 2:
            across_more()
        if distance == 3:
            ring_start()
        relay_across(distance - 1)
        multiply(distance - 1, core)
        if distance >= 2:
            await_mate(distance - 2)
            multiply(distance - 2, 1 - core)
    relay_across(4)
    multiply(4, core)
    for distance in (3, 4):
        await_mate(distance)
        multiply(distance, 1 - core)

    product_send[...] = product[...].astype(BF16)
    for step in range(1, 8):
        to_section = (section + step) % 8
        pending.append(
            transfer(
                product_send.at[:, pl.ds(to_section * 16, 16)],
                product_recv.at[section],
                product_sem.at[section],
                (to_section, place),
            )
        )

    reply_base = used[0]
    used[0] += 24

    def reply_copies(step):
        to_section = (section + step) % 8
        to = (to_section, place)
        at = reply_base + step * 3
        pair = pl.ds(to_section - to_section % 2, 2)
        return (
            (
                scaled_send.at[pair],
                scaled.at[:, chain_rows],
                reply_sem.at[section * 3],
                to,
                send_sem.at[at],
            ),
            (
                slope_send.at[to_section // 2],
                slopes.at[chain_rows],
                reply_sem.at[section * 3 + 1],
                to,
                send_sem.at[at + 1],
            ),
            (
                total_send.at[pair],
                total.at[:, chain_rows],
                reply_sem.at[section * 3 + 2],
                to,
                send_sem.at[at + 2],
            ),
        )

    product_recv[section] = product_send[:, chain_rows]
    arrive(mix_block(y_down, core), mix_sem.at[0])
    transfer(*mix_copy(2))
    transfer(*mix_copy(4))
    arrive(mix_block(y_up, core), mix_sem.at[1])
    transfer(*mix_copy(3))
    transfer(*mix_copy(5))
    arrive(mix_block(y_far, core, 0), mix_sem.at[2])
    transfer(*mix_copy(6))
    arrive(mix_block(y_far, core, 1), mix_sem.at[3])
    transfer(*mix_copy(7))
    for step in range(1, 8):
        sender = (section + step) % 8
        arrive(product_recv.at[sender], product_sem.at[sender])
    arrive(mix_block(y, 1 - core), mix_sem.at[9])
    arrive(mix_block(y_down, 1 - core), mix_sem.at[4])
    arrive(mix_block(y_up, 1 - core), mix_sem.at[5])
    arrive(mix_block(y_far, 1 - core, 0), mix_sem.at[6])
    arrive(mix_block(y_far, 1 - core, 1), mix_sem.at[7])

    square_sum = squares[:, :1]
    running = jnp.zeros((16, KVW), F32)
    for layer in range(layers):
        moved = 2.0 * folded[...] + GROUP * running
        energy = square_sum + jnp.sum(running * moved, axis=1, keepdims=True)
        inverse = 1.0 / jnp.sqrt(energy / width + epsilon)
        pair_at = layer - layer % 2
        mixed = product_recv[pair_at, layer % 2].astype(F32) + product_recv[
            pair_at + 1, layer % 2
        ].astype(F32)
        if layer:
            mixed += jnp.dot(
                running.astype(BF16), mixes[layer].reshape(KVW, KVW), preferred_element_type=F32
            )
        value = mixed * inverse
        totals[layer] = running
        values[layer] = value
        inverses[layer] = jnp.broadcast_to(inverse, (16, HEAD))
        total_send[layer] = running.astype(BF16)
        running = running + value
    direction = descent[...]
    for layer in reversed(range(layers)):
        inverse = inverses[layer][:, :1]
        slope = (
            jnp.sum(direction * values[layer], axis=1, keepdims=True)
            / width
            * inverse
            * inverse
        )
        step_scaled = (direction * inverse).astype(BF16)
        scaled_send[layer] = step_scaled
        at = (layer % 2) * 64
        slope_send[layer // 2, :, at : at + 64] = jnp.broadcast_to(slope, (16, 64)).astype(
            BF16
        )
        if layer:
            direction = (
                direction
                + lax.dot_general(
                    step_scaled,
                    mixes[layer].reshape(KVW, KVW),
                    (((1,), (1,)), ((), ())),
                    preferred_element_type=F32,
                )
                - (folded[...] + GROUP * totals[layer]) * slope
            )
    for item in range(3):
        for step in range(1, 8):
            transfer(*reply_copies(step)[item])
    own_pair = pl.ds(2 * y, 2)
    scaled[:, chain_rows] = scaled_send[own_pair]
    total[:, chain_rows] = total_send[own_pair]
    slopes[chain_rows] = slope_send[y]

    def await_totals():
        for step in range(1, 8):
            sender = (section + step) % 8
            arrive(total.at[:, pl.ds(sender * 16, 16)], reply_sem.at[sender * 3 + 2])

    for step in range(1, 8):
        sender = (section + step) % 8
        token_rows = pl.ds(sender * 16, 16)
        arrive(scaled.at[:, token_rows], reply_sem.at[sender * 3])
        arrive(slopes.at[token_rows], reply_sem.at[sender * 3 + 1])

    @pl.when(xh == 1)
    def _():
        shifts[...] = jnp.zeros_like(shifts)

    @pl.when(xh == 0)
    def _():
        await_totals()
        shifts[...] = total[...]

    pair_base = used[0]
    used[0] += 28
    quarter = half_width // 4

    def pair_copy(q, step):
        to_y = (y + step) % 4
        columns = pl.ds(q * quarter, quarter)
        return (
            pair_send.at[pl.ds(to_y * 32, 32), columns],
            pair_recv.at[y, :, columns],
            pair_sem.at[y * 4 + q],
            (2 * to_y + xh, place),
            send_sem.at[pair_base + q * 3 + step - 1],
        )

    def later_copy(q, step):
        to_y = (y + step) % 4
        columns = pl.ds(q * quarter, quarter)
        return (
            later_send.at[to_y, :, columns],
            later.at[pl.ds(y * 32, 32), columns],
            later_sem.at[y * 4 + q],
            (2 * to_y + xh, place),
            send_sem.at[pair_base + 12 + q * 3 + step - 1],
        )

    def other_copy(q):
        return (
            other_send.at[:, pl.ds(q * quarter, quarter)],
            out.at[:, pl.ds(pl.multiple_of(column_base + q * quarter, quarter), quarter)],
            other_sem.at[q],
            (twin, place),
            send_sem.at[pair_base + 24 + q],
        )

    def hidden_gradients(q):
        def step(index, carry):
            block = q * 4 + index
            at = pl.multiple_of(block * 256, 256)
            columns = pl.ds(pl.multiple_of(column_base + at, 256), 256)
            part = hidden[:, columns].astype(F32)
            grads = []
            for pair in range(2):
                shift = shifts[pair, :, q * HEAD : (q + 1) * HEAD].astype(F32)
                current = part + jnp.concatenate([shift, shift], axis=1)
                slope = slopes[:, pair * 64 : pair * 64 + 1].astype(F32)
                grads.append(
                    lax.dot_general(
                        scaled[pair],
                        weight[pair * 16 + block],
                        (((1,), (1,)), ((), ())),
                        preferred_element_type=F32,
                    )
                    - current * slope
                )
            odd[:, pl.ds(at, 256)] = grads[1].astype(BF16)
            pair_send[:, pl.ds(at, 256)] = (grads[0] + grads[1]).astype(BF16)
            return carry

        lax.fori_loop(0, 4, step, 0)

        @pl.when(y >= 1)
        def _():
            for step in range(1, 4):
                transfer(*pair_copy(q, step))

    def suffix(q):
        columns = pl.ds(q * quarter, quarter)
        for step in range(1, 4):
            from_y = (y + step) % 4

            @pl.when(from_y >= 1)
            def _():
                arrive(pair_recv.at[from_y, :, columns], pair_sem.at[from_y * 4 + q])

        @pl.when(y >= 1)
        def _():
            pair_recv[y, :, columns] = pair_send[rows, columns]

        running = pair_recv[3, :, columns].astype(F32)
        later_send[2, :, columns] = running.astype(BF16)
        running += pair_recv[2, :, columns].astype(F32)
        later_send[1, :, columns] = running.astype(BF16)
        running += pair_recv[1, :, columns].astype(F32)
        later_send[0, :, columns] = running.astype(BF16)
        for step in range(1, 4):
            to_y = (y + step) % 4

            @pl.when(to_y < 3)
            def _():
                transfer(*later_copy(q, step))

        @pl.when(y < 3)
        def _():
            later[rows, columns] = later_send[y, :, columns]

        @pl.when(y == 3)
        def _():
            later[:, columns] = jnp.zeros((128, quarter), BF16)

    def finish(q):
        @pl.when(y < 3)
        def _():
            for step in range(1, 4):
                from_y = (y + step) % 4
                target = later.at[pl.ds(from_y * 32, 32), pl.ds(q * quarter, quarter)]
                arrive(target, later_sem.at[from_y * 4 + q])

        def step(index, carry):
            at = pl.multiple_of(q * quarter + index * 256, 256)
            columns = pl.ds(at, 256)
            own_columns = pl.ds(pl.multiple_of(column_base + at, 256), 256)
            start = cotangent[:, own_columns].astype(F32) + later[:, columns].astype(F32)
            even_grad = (start + pair_send[:, columns].astype(F32)).astype(BF16)
            odd_grad = (start + odd[:, columns].astype(F32)).astype(BF16)
            out[:, own_columns] = jnp.where(xh == 0, even_grad, odd_grad)
            other_send[:, columns] = jnp.where(xh == 0, odd_grad, even_grad)
            return carry

        lax.fori_loop(0, 4, step, 0)
        pending.append(transfer(*other_copy(q)))

    def adapter_low():
        low = lax.dot_general(
            raised[...], scaled[xh], (((1,), (1,)), ((), ())), preferred_element_type=F32
        )
        return (adapter_scale * low).astype(BF16)

    def adapter_part(low, first, carry):
        def step(block, carry):
            columns = pl.ds(pl.multiple_of(block * 512, 512), 512)
            part = hidden[:, columns].astype(F32)
            if first < 8:
                at = pl.ds(pl.multiple_of((block // 2) * HEAD, HEAD), HEAD)
                shift = total[xh, :, at].astype(F32)
                part += jnp.concatenate([shift, shift, shift, shift], axis=1)
            grad = jnp.dot(low, part.astype(BF16), preferred_element_type=F32).astype(BF16)
            grad_send[block, 0, :64] = grad[:, :256]
            grad_send[block, 1, :64] = grad[:, 256:]
            gained = (part * gains[:, columns].astype(F32)).astype(BF16)
            return carry + lax.dot_general(
                gained, down[:, columns], (((1,), (1,)), ((), ())), preferred_element_type=F32
            )

        return lax.fori_loop(first, first + 8, step, carry)

    def adapter_up(carry):
        narrow[...] = carry.astype(BF16)
        up_grad = adapter_scale * lax.dot_general(
            scaled[xh], narrow[...], (((0,), (0,)), ((), ())), preferred_element_type=F32
        )
        padded = jnp.concatenate([up_grad, jnp.zeros((KVW, 192), F32)], axis=1)
        grad_send[:, :, 64:] = padded.astype(BF16).reshape(16, 2, 16, 256)

    def mate_copy():
        return (
            grad_send.at[:, 1 - core],
            grad_mate,
            grad_sem.at[16],
            mate,
            grad_send_sem.at[16],
        )

    seat = place // 2

    def grad_copy(step):
        to = (seat + step) % 16
        return (
            grad_sum.at[to],
            grad_recv.at[seat],
            grad_sem.at[seat],
            device(section, 2 * to + core),
            grad_send_sem.at[step],
        )

    def send_grads(step, carry):
        transfer(*grad_copy(step))
        return carry

    for q in range(4):
        hidden_gradients(q)
    suffix(0)

    @pl.when(xh == 1)
    def _():
        await_totals()

    low = adapter_low()
    carry = adapter_part(low, 0, jnp.zeros((128, 64), F32))
    suffix(1)
    adapter_up(adapter_part(low, 8, carry))
    transfer(*mate_copy())
    suffix(2)
    suffix(3)
    arrive(grad_mate, grad_sem.at[16])

    def sum_mate(index, carry):
        both = grad_send[index, core].astype(F32) + grad_mate[index].astype(F32)
        grad_sum[index] = both.astype(BF16)
        return carry

    lax.fori_loop(0, 16, sum_mate, 0)
    lax.fori_loop(1, 16, send_grads, 0)
    grad_recv[seat] = grad_sum[seat]
    for q in range(4):
        finish(q)

    def await_grads(step, carry):
        sender = (seat + 16 - step) % 16
        arrive(grad_recv.at[sender], grad_sem.at[sender])
        return carry

    lax.fori_loop(1, 16, await_grads, 0)

    def sum_grads(index, carry):
        return carry + grad_recv[index].astype(F32)

    summed = lax.fori_loop(0, 16, sum_grads, jnp.zeros((80, 256), F32))
    down_out[...] = summed[:64] * gains[:, own_features].astype(F32)
    up_out[...] = summed[64:, :64]
    for q in range(4):
        columns = pl.ds(
            pl.multiple_of((1 - xh) * half_width + q * quarter, quarter), quarter
        )
        arrive(out.at[:, columns], other_sem.at[q])

    def gone(copy):
        source, target, arrival, to, sem = copy
        pltpu.make_async_remote_copy(
            src_ref=source,
            dst_ref=target,
            send_sem=sem,
            recv_sem=arrival,
            device_id=to,
            device_id_type=pl.DeviceIdType.MESH,
        ).wait_send()

    for copy in pending:
        copy.wait_send()

    @pl.when(xl != xh)
    def _():
        for h in range(2):
            gone(
                (
                    shard.at[pl.ds(h * 128, 128)],
                    half(swapped_place, h),
                    weight_sem.at[swapped_place * 2 + h],
                    swap,
                    local_sem.at[3 + h],
                )
            )

    @pl.when(xl == 0)
    def _():
        for index in range(3):
            gone(quad_copy(index))
        for step in range(1, 8):
            gone(depth_copy(step))
        gone(mix_copy(8))
        gone(mix_copy(10))

    @pl.when(xl == 1)
    def _():
        gone(mix_copy(11))

    for index in (0, 1, 2, 3, 4, 5, 6, 7, 9):
        gone(mix_copy(index))
    for step in range(1, 8):
        for copy in reply_copies(step):
            gone(copy)

    @pl.when(y >= 1)
    def _():
        for q in range(4):
            for step in range(1, 4):
                gone(pair_copy(q, step))

    for step in range(1, 4):

        @pl.when((y + step) % 4 < 3)
        def _():
            for q in range(4):
                gone(later_copy(q, step))

    def grads_gone(step, carry):
        gone(grad_copy(step))
        return carry

    lax.fori_loop(1, 16, grads_gone, 0)
    gone(mate_copy())
    assert used[0] <= SENDS, used


SENDS = 256


def shards(
    codes,
    scale_codes,
    second_scales,
    gains,
    down_adapter,
    up_projection_weight,
    hidden_in,
    cotangent,
):
    tokens, width = hidden_in.shape
    vmem = pl.BlockSpec(memory_space=pltpu.VMEM)
    smem = pl.BlockSpec(memory_space=pltpu.SMEM)
    hbm = pl.BlockSpec(memory_space=pltpu.HBM)
    dma = pltpu.SemaphoreType.DMA
    input_grad, down_grad, up_grad = pl.pallas_call(
        functools.partial(chip_kernel, width),
        out_shape=(
            pltpu.VMEM((tokens, width), BF16),
            pltpu.VMEM((64, 256), F32),
            pltpu.VMEM((16, 64), F32),
        ),
        in_specs=[hbm, hbm, smem, hbm, hbm, hbm, hbm, hbm],
        out_specs=(vmem, vmem, vmem),
        scratch_shapes=[
            pltpu.VMEM((32, 256, KVW), BF16),
            pltpu.VMEM((8, 8, 2, 32, KVW), BF16),
            pltpu.VMEM((256, KVW), jnp.int32),
            pltpu.VMEM((8, 256), jnp.int32),
            pltpu.VMEM((1, width), BF16),
            pltpu.VMEM((64, KVW), BF16),
            pltpu.VMEM((256, KVW), BF16),
            pltpu.VMEM((4, 32, KVW), BF16),
            pltpu.VMEM((4, 32, KVW), BF16),
            pltpu.VMEM((tokens, width), BF16),
            pltpu.VMEM((tokens, width), BF16),
            pltpu.VMEM((64, width), BF16),
            pltpu.VMEM((2, tokens, KVW), F32),
            pltpu.VMEM((2, tokens, KVW), BF16),
            pltpu.VMEM((8, 2, 16, KVW), BF16),
            pltpu.VMEM((16, KVW), F32),
            pltpu.VMEM((16, KVW), F32),
            pltpu.VMEM((16, HEAD), F32),
            pltpu.VMEM((8, 16, KVW), F32),
            pltpu.VMEM((8, 16, KVW), F32),
            pltpu.VMEM((8, 16, HEAD), F32),
            pltpu.VMEM((8, 16, KVW), BF16),
            pltpu.VMEM((8, 16, KVW), BF16),
            pltpu.VMEM((4, 16, HEAD), BF16),
            pltpu.VMEM((2, tokens, KVW), BF16),
            pltpu.VMEM((2, tokens, KVW), BF16),
            pltpu.VMEM((2, tokens, KVW), BF16),
            pltpu.VMEM((tokens, HEAD), BF16),
            pltpu.VMEM((tokens, width // 2), BF16),
            pltpu.VMEM((tokens, width // 2), BF16),
            pltpu.VMEM((4, 32, width // 2), BF16),
            pltpu.VMEM((3, 32, width // 2), BF16),
            pltpu.VMEM((tokens, width // 2), BF16),
            pltpu.VMEM((tokens, width // 2), BF16),
            pltpu.VMEM((16, 2, 80, 256), BF16),
            pltpu.VMEM((16, 80, 256), BF16),
            pltpu.VMEM((16, 80, 256), BF16),
            pltpu.VMEM((16, 80, 256), BF16),
            pltpu.VMEM((tokens, 64), BF16),
            dma((9,)),
            dma((SENDS,)),
            dma((64,)),
            dma((4,)),
            dma((8,)),
            dma((12,)),
            dma((8,)),
            dma((24,)),
            dma((16,)),
            dma((16,)),
            dma((4,)),
            dma((17,)),
            dma((17,)),
        ],
        compiler_params=pltpu.CompilerParams(
            collective_id=0, has_side_effects=True, vmem_limit_bytes=56 * 2**20
        ),
        name="relay",
    )(
        codes[0],
        scale_codes[0].T,
        second_scales,
        gains,
        down_adapter[0].T,
        up_projection_weight[0].T,
        hidden_in,
        cotangent,
    )
    return (input_grad[None], down_grad.T[None], up_grad[None])


def solution(mesh):
    return jax.shard_map(
        shards,
        mesh=mesh,
        in_specs=(
            P("section", "fsdp", None),
            P("section", "fsdp", None),
            P("section", "fsdp"),
            P("section", None),
            P("section", None, None),
            P("section", None, None),
            P("fsdp", None),
            P("fsdp", None),
        ),
        out_specs=(
            P("section", "fsdp", None),
            P("section", "fsdp", None),
            P("section", "fsdp", None),
        ),
        check_vma=False,
    )
```

```python
import functools

import jax
import jax.numpy as jnp
from jax import lax
from jax.experimental import pallas as pl
from jax.experimental.pallas import tpu as pltpu
from jax.sharding import PartitionSpec as P

HEAD = 128
GROUP = 8
KV_HEADS = 4
KVW = KV_HEADS * HEAD
BLOCK = 64
SROWS = 32

NF4_TABLE = (
    -1.0,
    -0.6961928009986877,
    -0.5250730514526367,
    -0.39491748809814453,
    -0.28444138169288635,
    -0.18477343022823334,
    -0.09105003625154495,
    0.0,
    0.07958029955625534,
    0.16093020141124725,
    0.24611230194568634,
    0.33791524171066284,
    0.44070982933044434,
    0.5626170039176941,
    0.7229568362236023,
    1.0,
)
adapter_scale = 0.5
epsilon = 1e-05
F32 = jnp.float32
BF16 = jnp.bfloat16


def chip_kernel(
    width,
    codes_hbm,
    scale_hbm,
    second_scales,
    gains_hbm,
    down_hbm,
    raised_hbm,
    hidden_hbm,
    cotangent_hbm,
    out,
    down_out,
    up_out,
    weight,
    mixes,
    codes,
    scale_codes,
    gains,
    raised,
    shard,
    quad_send,
    quad_recv,
    hidden,
    cotangent,
    down,
    product,
    product_send,
    product_recv,
    folded,
    descent,
    squares,
    totals,
    values,
    inverses,
    scaled_send,
    total_send,
    slope_send,
    scaled,
    total,
    shifts,
    slopes,
    pair_send,
    odd,
    pair_recv,
    later_send,
    later,
    other_send,
    grad_send,
    grad_mate,
    grad_sum,
    grad_recv,
    narrow,
    local_sem,
    send_sem,
    weight_sem,
    quad_sem,
    depth_sem,
    mix_sem,
    product_sem,
    reply_sem,
    pair_sem,
    later_sem,
    other_sem,
    grad_send_sem,
    grad_sem,
):
    section = lax.axis_index("section")
    place = lax.axis_index("fsdp")
    y, xh = section // 2, section % 2
    xl, z, core = place // 16, (place // 2) % 8, place % 2
    half_width = width // 2
    column_base = xh * half_width
    layers = 2 * 4

    def device(to_section, to_place):
        return (to_section, to_place)

    mate = device(section, 2 * (place // 2) + 1 - core)
    across = device(section, (place + 16) % 32)
    above = device(section, xl * 16 + ((z + 1) % 8) * 2 + core)
    below = device(section, xl * 16 + ((z + 7) % 8) * 2 + core)
    twin = 2 * y + 1 - xh
    swap = device(twin, (place + 16) % 32)
    used = [0]

    def transfer(source, target, arrival, to, sem=None):
        if sem is None:
            sem = send_sem.at[used[0]]
            used[0] += 1
        copy = pltpu.make_async_remote_copy(
            src_ref=source,
            dst_ref=target,
            send_sem=sem,
            recv_sem=arrival,
            device_id=to,
            device_id_type=pl.DeviceIdType.MESH,
        )
        copy.start()
        return copy

    def arrive(target, arrival):
        pltpu.make_async_remote_copy(
            src_ref=target,
            dst_ref=target,
            send_sem=send_sem.at[0],
            recv_sem=arrival,
            device_id=mate,
            device_id_type=pl.DeviceIdType.MESH,
        ).wait_recv()

    loads = [
        pltpu.make_async_copy(hidden_hbm, hidden, local_sem.at[0]),
        pltpu.make_async_copy(cotangent_hbm, cotangent, local_sem.at[1]),
        pltpu.make_async_copy(down_hbm, down, local_sem.at[2]),
        pltpu.make_async_copy(codes_hbm, codes, local_sem.at[5]),
        pltpu.make_async_copy(scale_hbm, scale_codes, local_sem.at[6]),
        pltpu.make_async_copy(gains_hbm, gains, local_sem.at[7]),
        pltpu.make_async_copy(raised_hbm, raised, local_sem.at[8]),
    ]
    for load in reversed(loads):
        load.start()

    barrier = pltpu.get_barrier_semaphore()

    def greet(to):
        pl.semaphore_signal(
            barrier, inc=1, device_id=to, device_id_type=pl.DeviceIdType.MESH
        )

    def greet_place(step, carry):
        greet(device(section, (place + step) % 32))
        return carry

    lax.fori_loop(1, 32, greet_place, 0)
    for step in range(1, layers):
        greet(device((section + step) % 8, place))
    greet(swap)

    for load in loads[2:]:
        load.wait()
    own_features = pl.ds(pl.multiple_of(place * 256, 256), 256)
    lane = lax.broadcasted_iota(jnp.int32, (8, 256), 1)
    outer = jnp.full((8, 256), second_scales[0, 0], F32)
    for group in range(1, 8):
        outer = jnp.where(lane >= group * SROWS, second_scales[0, group], outer)
    block_scale = outer * (scale_codes[...].astype(F32) + 1.0) / 256.0
    gain_lanes = jnp.broadcast_to(gains[:, own_features].astype(F32), (120, 256))
    columns_of = jnp.concatenate([block_scale, gain_lanes], axis=0).T
    side = lax.broadcasted_iota(jnp.int32, (256, HEAD), 1) < BLOCK
    low_rank = lax.dot_general(
        down[:, own_features], raised[...], (((0,), (0,)), ((), ())), preferred_element_type=F32
    )
    for tile in range(KV_HEADS):
        at = slice(tile * HEAD, (tile + 1) * HEAD)
        entries = codes[:, at]
        looked = jnp.full((256, HEAD), NF4_TABLE[0], F32)
        for entry in range(1, 16):
            looked = jnp.where(entries == entry, NF4_TABLE[entry], looked)
        left = columns_of[:, 2 * tile : 2 * tile + 1]
        right = columns_of[:, 2 * tile + 1 : 2 * tile + 2]
        base = (looked * jnp.where(side, left, right)).astype(BF16).astype(F32)
        rows_of = (base + adapter_scale * low_rank[:, at]) * columns_of[:, 8:9]
        shard[:, at] = rows_of.astype(BF16)
    pl.semaphore_wait(barrier, 31 + 7 + 1)

    quarter_at = (z % 2) * 2 + core
    fellows = (
        (quarter_at + 1 - 2 * core, mate),
        ((1 - z % 2) * 2 + core, device(section, xl * 16 + (z + 1 - 2 * (z % 2)) * 2 + core)),
        (
            (1 - z % 2) * 2 + 1 - core,
            device(section, xl * 16 + (z + 1 - 2 * (z % 2)) * 2 + 1 - core),
        ),
    )
    early_base = used[0]
    used[0] += 24
    y_up, y_down = (y + 1) % 4, (y + 3) % 4
    y_far = (y + 2) % 4

    def quad_copy(index):
        which, to = fellows[index]
        return (
            quad_send.at[which],
            quad_recv.at[quarter_at],
            quad_sem.at[quarter_at],
            to,
            send_sem.at[early_base + index],
        )

    def depth_copy(step):
        rows_at = mixes.at[section, z, core]
        to = device(section, xl * 16 + ((z + step) % 8) * 2 + core)
        return (rows_at, rows_at, depth_sem.at[z], to, send_sem.at[early_base + 2 + step])

    def mix_block(which_y, which, part=None):
        if part is None:
            return mixes.at[pl.ds(2 * which_y, 2), :, which]
        return mixes.at[pl.ds(2 * which_y, 2), pl.ds(part * 4, 4), which]

    mix_moves = (
        (mix_block(y, core), 0, (2 * y_up + xh, place)),
        (mix_block(y, core), 1, (2 * y_down + xh, place)),
        (mix_block(y_down, core, 0), 2, (2 * y_up + xh, place)),
        (mix_block(y_up, core, 1), 3, (2 * y_down + xh, place)),
        (mix_block(y_down, core), 4, mate),
        (mix_block(y_up, core), 5, mate),
        (mix_block(y_far, core, 0), 6, mate),
        (mix_block(y_far, core, 1), 7, mate),
        (mixes.at[section, :, core], 8, across),
        (mix_block(y, core), 9, mate),
        (mixes.at[section, :, core], 10, swap),
        (mixes.at[twin, :, core], 11, across),
    )

    def mix_copy(index):
        block, sem, to = mix_moves[index]
        return (block, block, mix_sem.at[sem], to, send_sem.at[early_base + 10 + index])

    def quad_start():
        own = shard[:128].astype(F32) + shard[128:].astype(F32)
        quad_send[...] = own.astype(BF16).reshape(4, 32, KVW)
        for index in range(3):
            transfer(*quad_copy(index))

    def depth_start():
        summed = quad_send[quarter_at].astype(F32)
        for which, _ in fellows:
            arrive(quad_recv.at[which], quad_sem.at[which])
            summed += quad_recv[which].astype(F32)
        mixes[section, z, core] = summed.astype(BF16)
        for step in range(1, 8):
            transfer(*depth_copy(step))

    def across_start():
        @pl.when(xl == 0)
        def _():
            for step in range(1, 8):
                at_z = (z + step) % 8
                arrive(mixes.at[section, at_z, core], depth_sem.at[at_z])
            transfer(*mix_copy(8))
            transfer(*mix_copy(10))

    def across_more():
        @pl.when(xl == 1)
        def _():
            arrive(mixes.at[twin, :, core], mix_sem.at[10])
            transfer(*mix_copy(11))
            arrive(mixes.at[section, :, core], mix_sem.at[8])

    def ring_start():
        @pl.when(xl == 0)
        def _():
            arrive(mixes.at[twin, :, core], mix_sem.at[11])

        for index in (0, 1, 9):
            transfer(*mix_copy(index))

    def ring_more():
        arrive(mix_block(y_down, core), mix_sem.at[0])
        transfer(*mix_copy(2))
        transfer(*mix_copy(4))
        arrive(mix_block(y_up, core), mix_sem.at[1])
        transfer(*mix_copy(3))
        transfer(*mix_copy(5))

    def ring_last():
        arrive(mix_block(y_far, core, 0), mix_sem.at[2])
        transfer(*mix_copy(6))
        arrive(mix_block(y_far, core, 1), mix_sem.at[3])
        transfer(*mix_copy(7))

    @pl.when(xl == 0)
    def _():
        quad_start()

    pending = []

    def slot(x, depth, which):
        return x * 16 + depth * 2 + which

    def half(block, h):
        return weight.at[block, pl.ds(h * 128, 128)]

    def pass_on(block, h, to):
        pending.append(transfer(half(block, h), half(block, h), weight_sem.at[block * 2 + h], to))

    def await_block(block, h):
        arrive(half(block, h), weight_sem.at[block * 2 + h])

    swapped_place = (place + 16) % 32

    @pl.when(xl != xh)
    def _():
        for h in range(2):
            transfer(
                shard.at[pl.ds(h * 128, 128)],
                half(swapped_place, h),
                weight_sem.at[swapped_place * 2 + h],
                swap,
                local_sem.at[3 + h],
            )

    @pl.when(xl == xh)
    def _():
        pltpu.make_async_copy(shard, weight.at[place], local_sem.at[3]).start()

    rows = pl.ds(y * 32, 32)
    chain_rows = pl.ds(section * 16, 16)

    def fold(ref):
        for head in range(KV_HEADS):
            part = jnp.zeros((16, HEAD), F32)
            for member in range(GROUP):
                at = (head * GROUP + member) * HEAD
                part += ref[chain_rows, pl.ds(at, HEAD)].astype(F32)
            yield head, part

    @pl.when(xl == xh)
    def _():
        pltpu.make_async_copy(shard, weight.at[place], local_sem.at[3]).wait()

    others = [place, slot(1 - xl, z, core)]

    for h in range(2):

        @pl.when(xl != xh)
        def _():
            await_block(place, h)

        if h == 0:
            pass_on(place, h, across)
        for to in (above, below, mate):
            pass_on(place, h, to)

    @pl.when(xl == 0)
    def _():
        depth_start()

    loads[0].wait()
    loads[1].wait()
    for head, part in fold(hidden):
        folded[:, head * HEAD : (head + 1) * HEAD] = part
    for head, part in fold(cotangent):
        descent[:, head * HEAD : (head + 1) * HEAD] = part
    square = jnp.zeros((16, HEAD), F32)
    for at in range(0, width, HEAD):
        piece = hidden[chain_rows, pl.ds(at, HEAD)].astype(F32)
        square += piece * piece
    squares[...] = jnp.broadcast_to(jnp.sum(square, axis=1, keepdims=True), (16, HEAD))
    product[...] = jnp.zeros_like(product)

    await_block(others[1], 0)
    for to in (above, below, mate):
        pass_on(others[1], 0, to)


    def at_distance(distance):
        if distance == 0:
            return [z]
        if distance == 4:
            return [(z + 4) % 8]
        return [(z + 8 - distance) % 8, (z + distance) % 8]

    def multiply(distance, which):
        depths = len(at_distance(distance))

        def step(index, carry):
            x = index // depths
            depth = (z + 8 - distance + (index % depths) * 2 * distance) % 8
            block = slot(x, depth, which)
            columns = pl.ds(pl.multiple_of(column_base + (depth * 2 + which) * 256, 256), 256)
            product[x] += jnp.dot(hidden[:, columns], weight[block], preferred_element_type=F32)
            return carry

        lax.fori_loop(0, 2 * depths, step, 0)

    def relay_across(distance):
        for depth in at_distance(distance):
            block = slot(1 - xl, depth, core)
            await_block(block, 1)
            pass_on(block, 1, mate)

    def await_mate(distance):
        for depth in at_distance(distance):
            for x in range(2):
                for h in range(2):
                    await_block(slot(x, depth, 1 - core), h)

    hooks = {
        (1, 1): across_start,
        (1, 2): across_more,
        (2, 1): ring_start,
        (4, 0): ring_more,
    }
    for distance in range(1, 5):
        low, high = (z + 8 - distance) % 8, (z + distance) % 8
        for turn, (x, h, up_reach, down_reach) in enumerate(
            ((xl, 1, 3, 3), (xl, 0, 4, 3), (1 - xl, 0, 3, 4))
        ):
            for depth, reach, onward in ((low, up_reach, above), (high, down_reach, below)):
                if distance > reach:
                    continue
                block = slot(x, depth, core)
                await_block(block, h)
                if distance < reach:
                    pass_on(block, h, onward)
                pass_on(block, h, mate)
                if h == 1:
                    pass_on(block, h, across)
            if distance == 3 and h == 1:
                ends = slot(xl, low + (high - low) * core, core)
                pass_on(ends, 1, device(section, xl * 16 + ((z + 1 + 6 * core) % 8) * 2 + core))
            if distance == 4 and h == 1:
                await_block(slot(x, low, core), 1)
                pass_on(slot(x, low, core), 1, across)
                pass_on(slot(x, low, core), 1, mate)
            if (distance, turn) in hooks:
                hooks[distance, turn]()
        if distance == 1:
            pass_on(place, 1, across)
        relay_across(distance - 1)
        multiply(distance - 1, core)
        if distance >= 2:
            await_mate(distance - 2)
            multiply(distance - 2, 1 - core)
    relay_across(4)
    ring_last()
    multiply(4, core)
    for distance in (3, 4):
        await_mate(distance)
        multiply(distance, 1 - core)

    product_send[...] = product[...].astype(BF16)
    for step in range(1, 8):
        to_section = (section + step) % 8
        pending.append(
            transfer(
                product_send.at[:, pl.ds(to_section * 16, 16)],
                product_recv.at[section],
                product_sem.at[section],
                (to_section, place),
            )
        )

    reply_base = used[0]
    used[0] += 24

    total_base = used[0]
    used[0] += 8

    def reply_copies(step):
        to_section = (section + step) % 8
        to = (to_section, place)
        at = reply_base + step * 3
        pair = pl.ds(to_section - to_section % 2, 2)
        return (
            (
                scaled_send.at[pair],
                scaled.at[:, chain_rows],
                reply_sem.at[section * 3],
                to,
                send_sem.at[at],
            ),
            (
                slope_send.at[to_section // 2],
                slopes.at[chain_rows],
                reply_sem.at[section * 3 + 1],
                to,
                send_sem.at[at + 1],
            ),
        )

    def total_copy(step, column):
        to_y = (y + step) % 4
        if column == 0:
            source, target = total_send.at[pl.ds(2 * to_y, 2)], total.at[:, chain_rows]
        else:
            source, target = total_send.at[2 * to_y + 1], total.at[1, chain_rows]
        return (
            source,
            target,
            reply_sem.at[section * 3 + 2],
            (2 * to_y + column, place),
            send_sem.at[total_base + step * 2 + column],
        )

    def each_total(column, act):
        for step in range(1, 4):
            act(total_copy(step, column))

        @pl.when(xh == 1 - column)
        def _():
            act(total_copy(0, column))

    product_recv[section] = product_send[:, chain_rows]
    for step in range(1, 8):
        sender = (section + step) % 8
        arrive(product_recv.at[sender], product_sem.at[sender])
    arrive(mix_block(y, 1 - core), mix_sem.at[9])
    arrive(mix_block(y_down, 1 - core), mix_sem.at[4])
    arrive(mix_block(y_up, 1 - core), mix_sem.at[5])
    arrive(mix_block(y_far, 1 - core, 0), mix_sem.at[6])
    arrive(mix_block(y_far, 1 - core, 1), mix_sem.at[7])

    square_sum = squares[:, :1]
    running = jnp.zeros((16, KVW), F32)
    for layer in range(layers):
        moved = 2.0 * folded[...] + GROUP * running
        energy = square_sum + jnp.sum(running * moved, axis=1, keepdims=True)
        inverse = 1.0 / jnp.sqrt(energy / width + epsilon)
        pair_at = layer - layer % 2
        mixed = product_recv[pair_at, layer % 2].astype(F32) + product_recv[
            pair_at + 1, layer % 2
        ].astype(F32)
        if layer:
            mixed += jnp.dot(
                running.astype(BF16), mixes[layer].reshape(KVW, KVW), preferred_element_type=F32
            )
        value = mixed * inverse
        totals[layer] = running
        values[layer] = value
        inverses[layer] = jnp.broadcast_to(inverse, (16, HEAD))
        total_send[layer] = running.astype(BF16)
        running = running + value
    each_total(0, lambda copy: transfer(*copy))
    direction = descent[...]
    for layer in reversed(range(layers)):
        inverse = inverses[layer][:, :1]
        slope = (
            jnp.sum(direction * values[layer], axis=1, keepdims=True)
            / width
            * inverse
            * inverse
        )
        step_scaled = (direction * inverse).astype(BF16)
        scaled_send[layer] = step_scaled
        at = (layer % 2) * 64
        slope_send[layer // 2, :, at : at + 64] = jnp.broadcast_to(slope, (16, 64)).astype(
            BF16
        )
        if layer:
            direction = (
                direction
                + lax.dot_general(
                    step_scaled,
                    mixes[layer].reshape(KVW, KVW),
                    (((1,), (1,)), ((), ())),
                    preferred_element_type=F32,
                )
                - (folded[...] + GROUP * totals[layer]) * slope
            )
    for item in range(2):
        for step in range(1, 8):
            transfer(*reply_copies(step)[item])
    each_total(1, lambda copy: transfer(*copy))
    own_pair = pl.ds(2 * y, 2)
    scaled[:, chain_rows] = scaled_send[own_pair]
    total[:, chain_rows] = total_send[own_pair]
    slopes[chain_rows] = slope_send[y]

    def await_totals(layers_at):
        for step in range(1, 8):
            sender = (section + step) % 8
            arrive(total.at[layers_at, pl.ds(sender * 16, 16)], reply_sem.at[sender * 3 + 2])

    for step in range(1, 8):
        sender = (section + step) % 8
        token_rows = pl.ds(sender * 16, 16)
        arrive(scaled.at[:, token_rows], reply_sem.at[sender * 3])
        arrive(slopes.at[token_rows], reply_sem.at[sender * 3 + 1])

    @pl.when(xh == 1)
    def _():
        shifts[...] = jnp.zeros_like(shifts)

    @pl.when(xh == 0)
    def _():
        await_totals(slice(None))
        shifts[...] = total[...]

    pair_base = used[0]
    used[0] += 28
    quarter = half_width // 4

    def pair_copy(q, step):
        to_y = (y + step) % 4
        columns = pl.ds(q * quarter, quarter)
        return (
            pair_send.at[pl.ds(to_y * 32, 32), columns],
            pair_recv.at[y, :, columns],
            pair_sem.at[y * 4 + q],
            (2 * to_y + xh, place),
            send_sem.at[pair_base + q * 3 + step - 1],
        )

    def later_copy(q, step):
        to_y = (y + step) % 4
        columns = pl.ds(q * quarter, quarter)
        return (
            later_send.at[to_y, :, columns],
            later.at[pl.ds(y * 32, 32), columns],
            later_sem.at[y * 4 + q],
            (2 * to_y + xh, place),
            send_sem.at[pair_base + 12 + q * 3 + step - 1],
        )

    def other_copy(q):
        return (
            other_send.at[:, pl.ds(q * quarter, quarter)],
            out.at[:, pl.ds(pl.multiple_of(column_base + q * quarter, quarter), quarter)],
            other_sem.at[q],
            (twin, place),
            send_sem.at[pair_base + 24 + q],
        )

    def hidden_gradients(q):
        def step(index, carry):
            block = q * 4 + index
            at = pl.multiple_of(block * 256, 256)
            columns = pl.ds(pl.multiple_of(column_base + at, 256), 256)
            part = hidden[:, columns].astype(F32)
            grads = []
            for pair in range(2):
                shift = shifts[pair, :, q * HEAD : (q + 1) * HEAD].astype(F32)
                current = part + jnp.concatenate([shift, shift], axis=1)
                slope = slopes[:, pair * 64 : pair * 64 + 1].astype(F32)
                grads.append(
                    lax.dot_general(
                        scaled[pair],
                        weight[pair * 16 + block],
                        (((1,), (1,)), ((), ())),
                        preferred_element_type=F32,
                    )
                    - current * slope
                )
            odd[:, pl.ds(at, 256)] = grads[1].astype(BF16)
            pair_send[:, pl.ds(at, 256)] = (grads[0] + grads[1]).astype(BF16)
            return carry

        lax.fori_loop(0, 4, step, 0)

    def send_pairs(q):
        @pl.when(y >= 1)
        def _():
            for step in range(1, 4):
                transfer(*pair_copy(q, step))

    def suffix(q):
        columns = pl.ds(q * quarter, quarter)
        for step in range(1, 4):
            from_y = (y + step) % 4

            @pl.when(from_y >= 1)
            def _():
                arrive(pair_recv.at[from_y, :, columns], pair_sem.at[from_y * 4 + q])

        @pl.when(y >= 1)
        def _():
            pair_recv[y, :, columns] = pair_send[rows, columns]

        running = pair_recv[3, :, columns].astype(F32)
        later_send[2, :, columns] = running.astype(BF16)
        running += pair_recv[2, :, columns].astype(F32)
        later_send[1, :, columns] = running.astype(BF16)
        running += pair_recv[1, :, columns].astype(F32)
        later_send[0, :, columns] = running.astype(BF16)
        for step in range(1, 4):
            to_y = (y + step) % 4

            @pl.when(to_y < 3)
            def _():
                transfer(*later_copy(q, step))

        @pl.when(y < 3)
        def _():
            later[rows, columns] = later_send[y, :, columns]

        @pl.when(y == 3)
        def _():
            later[:, columns] = jnp.zeros((128, quarter), BF16)

    def finish(q):
        @pl.when(y < 3)
        def _():
            for step in range(1, 4):
                from_y = (y + step) % 4
                target = later.at[pl.ds(from_y * 32, 32), pl.ds(q * quarter, quarter)]
                arrive(target, later_sem.at[from_y * 4 + q])

        def step(index, carry):
            at = pl.multiple_of(q * quarter + index * 256, 256)
            columns = pl.ds(at, 256)
            own_columns = pl.ds(pl.multiple_of(column_base + at, 256), 256)
            start = cotangent[:, own_columns].astype(F32) + later[:, columns].astype(F32)
            even_grad = (start + pair_send[:, columns].astype(F32)).astype(BF16)
            odd_grad = (start + odd[:, columns].astype(F32)).astype(BF16)
            out[:, own_columns] = jnp.where(xh == 0, even_grad, odd_grad)
            other_send[:, columns] = jnp.where(xh == 0, odd_grad, even_grad)
            return carry

        lax.fori_loop(0, 4, step, 0)
        pending.append(transfer(*other_copy(q)))

    def adapter_low():
        low = lax.dot_general(
            raised[...], scaled[xh], (((1,), (1,)), ((), ())), preferred_element_type=F32
        )
        return (adapter_scale * low).astype(BF16)

    def adapter_part(low, first, carry):
        def step(block, carry):
            columns = pl.ds(pl.multiple_of(block * 512, 512), 512)
            part = hidden[:, columns].astype(F32)
            if first < 8:
                at = pl.ds(pl.multiple_of((block // 2) * HEAD, HEAD), HEAD)
                shift = total[xh, :, at].astype(F32)
                part += jnp.concatenate([shift, shift, shift, shift], axis=1)
            grad = jnp.dot(low, part.astype(BF16), preferred_element_type=F32).astype(BF16)
            grad_send[block, 0, :64] = grad[:, :256]
            grad_send[block, 1, :64] = grad[:, 256:]
            gained = (part * gains[:, columns].astype(F32)).astype(BF16)
            return carry + lax.dot_general(
                gained, down[:, columns], (((1,), (1,)), ((), ())), preferred_element_type=F32
            )

        return lax.fori_loop(first, first + 8, step, carry)

    def adapter_up(carry):
        narrow[...] = carry.astype(BF16)
        up_grad = adapter_scale * lax.dot_general(
            scaled[xh], narrow[...], (((0,), (0,)), ((), ())), preferred_element_type=F32
        )
        padded = jnp.concatenate([up_grad, jnp.zeros((KVW, 192), F32)], axis=1)
        grad_send[:, :, 64:] = padded.astype(BF16).reshape(16, 2, 16, 256)

    def mate_copy():
        return (
            grad_send.at[:, 1 - core],
            grad_mate,
            grad_sem.at[16],
            mate,
            grad_send_sem.at[16],
        )

    seat = place // 2

    def grad_copy(step):
        to = (seat + step) % 16
        return (
            grad_sum.at[to],
            grad_recv.at[seat],
            grad_sem.at[seat],
            device(section, 2 * to + core),
            grad_send_sem.at[step],
        )

    def send_grads(step, carry):
        transfer(*grad_copy(step))
        return carry

    def sum_mate(index, carry):
        both = grad_send[index, core].astype(F32) + grad_mate[index].astype(F32)
        grad_sum[index] = both.astype(BF16)
        return carry

    hidden_gradients(0)
    send_pairs(0)
    hidden_gradients(1)
    send_pairs(1)

    @pl.when(xh == 1)
    def _():
        await_totals(1)

    low = adapter_low()
    carry = adapter_part(low, 0, jnp.zeros((128, 64), F32))
    adapter_up(adapter_part(low, 8, carry))
    transfer(*mate_copy())
    suffix(0)
    hidden_gradients(2)
    send_pairs(2)
    suffix(1)
    hidden_gradients(3)
    send_pairs(3)
    arrive(grad_mate, grad_sem.at[16])
    lax.fori_loop(0, 16, sum_mate, 0)
    lax.fori_loop(1, 16, send_grads, 0)
    grad_recv[seat] = grad_sum[seat]
    finish(0)
    suffix(2)
    finish(1)
    suffix(3)
    finish(2)
    finish(3)

    def await_grads(step, carry):
        sender = (seat + 16 - step) % 16
        arrive(grad_recv.at[sender], grad_sem.at[sender])
        return carry

    lax.fori_loop(1, 16, await_grads, 0)

    def sum_grads(index, carry):
        return carry + grad_recv[index].astype(F32)

    summed = lax.fori_loop(0, 16, sum_grads, jnp.zeros((80, 256), F32))
    down_out[...] = summed[:64] * gains[:, own_features].astype(F32)
    up_out[...] = summed[64:, :64]
    for q in range(4):
        columns = pl.ds(
            pl.multiple_of((1 - xh) * half_width + q * quarter, quarter), quarter
        )
        arrive(out.at[:, columns], other_sem.at[q])

    def gone(copy):
        source, target, arrival, to, sem = copy
        pltpu.make_async_remote_copy(
            src_ref=source,
            dst_ref=target,
            send_sem=sem,
            recv_sem=arrival,
            device_id=to,
            device_id_type=pl.DeviceIdType.MESH,
        ).wait_send()

    for copy in pending:
        copy.wait_send()

    @pl.when(xl != xh)
    def _():
        for h in range(2):
            gone(
                (
                    shard.at[pl.ds(h * 128, 128)],
                    half(swapped_place, h),
                    weight_sem.at[swapped_place * 2 + h],
                    swap,
                    local_sem.at[3 + h],
                )
            )

    @pl.when(xl == 0)
    def _():
        for index in range(3):
            gone(quad_copy(index))
        for step in range(1, 8):
            gone(depth_copy(step))
        gone(mix_copy(8))
        gone(mix_copy(10))

    @pl.when(xl == 1)
    def _():
        gone(mix_copy(11))

    for index in (0, 1, 2, 3, 4, 5, 6, 7, 9):
        gone(mix_copy(index))
    for step in range(1, 8):
        for copy in reply_copies(step):
            gone(copy)
    each_total(0, gone)
    each_total(1, gone)

    @pl.when(y >= 1)
    def _():
        for q in range(4):
            for step in range(1, 4):
                gone(pair_copy(q, step))

    for step in range(1, 4):

        @pl.when((y + step) % 4 < 3)
        def _():
            for q in range(4):
                gone(later_copy(q, step))

    def grads_gone(step, carry):
        gone(grad_copy(step))
        return carry

    lax.fori_loop(1, 16, grads_gone, 0)
    gone(mate_copy())
    assert used[0] <= SENDS, used


SENDS = 256


def shards(
    codes,
    scale_codes,
    second_scales,
    gains,
    down_adapter,
    up_projection_weight,
    hidden_in,
    cotangent,
):
    tokens, width = hidden_in.shape
    vmem = pl.BlockSpec(memory_space=pltpu.VMEM)
    smem = pl.BlockSpec(memory_space=pltpu.SMEM)
    hbm = pl.BlockSpec(memory_space=pltpu.HBM)
    dma = pltpu.SemaphoreType.DMA
    input_grad, down_grad, up_grad = pl.pallas_call(
        functools.partial(chip_kernel, width),
        out_shape=(
            pltpu.VMEM((tokens, width), BF16),
            pltpu.VMEM((64, 256), F32),
            pltpu.VMEM((16, 64), F32),
        ),
        in_specs=[hbm, hbm, smem, hbm, hbm, hbm, hbm, hbm],
        out_specs=(vmem, vmem, vmem),
        scratch_shapes=[
            pltpu.VMEM((32, 256, KVW), BF16),
            pltpu.VMEM((8, 8, 2, 32, KVW), BF16),
            pltpu.VMEM((256, KVW), jnp.int32),
            pltpu.VMEM((8, 256), jnp.int32),
            pltpu.VMEM((1, width), BF16),
            pltpu.VMEM((64, KVW), BF16),
            pltpu.VMEM((256, KVW), BF16),
            pltpu.VMEM((4, 32, KVW), BF16),
            pltpu.VMEM((4, 32, KVW), BF16),
            pltpu.VMEM((tokens, width), BF16),
            pltpu.VMEM((tokens, width), BF16),
            pltpu.VMEM((64, width), BF16),
            pltpu.VMEM((2, tokens, KVW), F32),
            pltpu.VMEM((2, tokens, KVW), BF16),
            pltpu.VMEM((8, 2, 16, KVW), BF16),
            pltpu.VMEM((16, KVW), F32),
            pltpu.VMEM((16, KVW), F32),
            pltpu.VMEM((16, HEAD), F32),
            pltpu.VMEM((8, 16, KVW), F32),
            pltpu.VMEM((8, 16, KVW), F32),
            pltpu.VMEM((8, 16, HEAD), F32),
            pltpu.VMEM((8, 16, KVW), BF16),
            pltpu.VMEM((8, 16, KVW), BF16),
            pltpu.VMEM((4, 16, HEAD), BF16),
            pltpu.VMEM((2, tokens, KVW), BF16),
            pltpu.VMEM((2, tokens, KVW), BF16),
            pltpu.VMEM((2, tokens, KVW), BF16),
            pltpu.VMEM((tokens, HEAD), BF16),
            pltpu.VMEM((tokens, width // 2), BF16),
            pltpu.VMEM((tokens, width // 2), BF16),
            pltpu.VMEM((4, 32, width // 2), BF16),
            pltpu.VMEM((3, 32, width // 2), BF16),
            pltpu.VMEM((tokens, width // 2), BF16),
            pltpu.VMEM((tokens, width // 2), BF16),
            pltpu.VMEM((16, 2, 80, 256), BF16),
            pltpu.VMEM((16, 80, 256), BF16),
            pltpu.VMEM((16, 80, 256), BF16),
            pltpu.VMEM((16, 80, 256), BF16),
            pltpu.VMEM((tokens, 64), BF16),
            dma((9,)),
            dma((SENDS,)),
            dma((64,)),
            dma((4,)),
            dma((8,)),
            dma((12,)),
            dma((8,)),
            dma((24,)),
            dma((16,)),
            dma((16,)),
            dma((4,)),
            dma((17,)),
            dma((17,)),
        ],
        compiler_params=pltpu.CompilerParams(
            collective_id=0, has_side_effects=True, vmem_limit_bytes=56 * 2**20
        ),
        name="relay",
    )(
        codes[0],
        scale_codes[0].T,
        second_scales,
        gains,
        down_adapter[0].T,
        up_projection_weight[0].T,
        hidden_in,
        cotangent,
    )
    return (input_grad[None], down_grad.T[None], up_grad[None])


def solution(mesh):
    return jax.shard_map(
        shards,
        mesh=mesh,
        in_specs=(
            P("section", "fsdp", None),
            P("section", "fsdp", None),
            P("section", "fsdp"),
            P("section", None),
            P("section", None, None),
            P("section", None, None),
            P("fsdp", None),
            P("fsdp", None),
        ),
        out_specs=(
            P("section", "fsdp", None),
            P("section", "fsdp", None),
            P("section", "fsdp", None),
        ),
        check_vma=False,
    )
```

```python
import functools

import jax
import jax.numpy as jnp
from jax import lax
from jax.experimental import pallas as pl
from jax.experimental.pallas import tpu as pltpu
from jax.sharding import PartitionSpec as P

HEAD = 128
GROUP = 8
KV_HEADS = 4
KVW = KV_HEADS * HEAD
BLOCK = 64
SROWS = 32

NF4_TABLE = (
    -1.0,
    -0.6961928009986877,
    -0.5250730514526367,
    -0.39491748809814453,
    -0.28444138169288635,
    -0.18477343022823334,
    -0.09105003625154495,
    0.0,
    0.07958029955625534,
    0.16093020141124725,
    0.24611230194568634,
    0.33791524171066284,
    0.44070982933044434,
    0.5626170039176941,
    0.7229568362236023,
    1.0,
)
adapter_scale = 0.5
epsilon = 1e-05
F32 = jnp.float32
BF16 = jnp.bfloat16


def chip_kernel(
    width,
    codes_hbm,
    scale_hbm,
    second_scales,
    gains_hbm,
    down_hbm,
    raised_hbm,
    hidden_hbm,
    cotangent_hbm,
    out,
    down_out,
    up_out,
    weight,
    mixes,
    codes,
    scale_codes,
    gains,
    raised,
    shard,
    quad_send,
    quad_recv,
    hidden,
    cotangent,
    down,
    product,
    product_send,
    product_recv,
    folded,
    descent,
    squares,
    totals,
    values,
    inverses,
    scaled_send,
    total_send,
    slope_send,
    scaled,
    total,
    shifts,
    slopes,
    pair_send,
    odd,
    pair_recv,
    later_send,
    later,
    other_send,
    grad_send,
    grad_mate,
    grad_sum,
    grad_recv,
    grad_cross,
    narrow,
    local_sem,
    send_sem,
    weight_sem,
    quad_sem,
    depth_sem,
    mix_sem,
    product_sem,
    reply_sem,
    pair_sem,
    later_sem,
    other_sem,
    grad_send_sem,
    grad_sem,
):
    section = lax.axis_index("section")
    place = lax.axis_index("fsdp")
    y, xh = section // 2, section % 2
    xl, z, core = place // 16, (place // 2) % 8, place % 2
    half_width = width // 2
    column_base = xh * half_width
    layers = 2 * 4

    def device(to_section, to_place):
        return (to_section, to_place)

    mate = device(section, 2 * (place // 2) + 1 - core)
    across = device(section, (place + 16) % 32)
    above = device(section, xl * 16 + ((z + 1) % 8) * 2 + core)
    below = device(section, xl * 16 + ((z + 7) % 8) * 2 + core)
    twin = 2 * y + 1 - xh
    swap = device(twin, (place + 16) % 32)
    used = [0]

    def transfer(source, target, arrival, to, sem=None):
        if sem is None:
            sem = send_sem.at[used[0]]
            used[0] += 1
        copy = pltpu.make_async_remote_copy(
            src_ref=source,
            dst_ref=target,
            send_sem=sem,
            recv_sem=arrival,
            device_id=to,
            device_id_type=pl.DeviceIdType.MESH,
        )
        copy.start()
        return copy

    def arrive(target, arrival):
        pltpu.make_async_remote_copy(
            src_ref=target,
            dst_ref=target,
            send_sem=send_sem.at[0],
            recv_sem=arrival,
            device_id=mate,
            device_id_type=pl.DeviceIdType.MESH,
        ).wait_recv()

    loads = [
        pltpu.make_async_copy(hidden_hbm, hidden, local_sem.at[0]),
        pltpu.make_async_copy(cotangent_hbm, cotangent, local_sem.at[1]),
        pltpu.make_async_copy(down_hbm, down, local_sem.at[2]),
        pltpu.make_async_copy(codes_hbm, codes, local_sem.at[5]),
        pltpu.make_async_copy(scale_hbm, scale_codes, local_sem.at[6]),
        pltpu.make_async_copy(gains_hbm, gains, local_sem.at[7]),
        pltpu.make_async_copy(raised_hbm, raised, local_sem.at[8]),
    ]
    for load in reversed(loads):
        load.start()

    barrier = pltpu.get_barrier_semaphore()

    def greet(to):
        pl.semaphore_signal(
            barrier, inc=1, device_id=to, device_id_type=pl.DeviceIdType.MESH
        )

    def greet_place(step, carry):
        greet(device(section, (place + step) % 32))
        return carry

    lax.fori_loop(1, 32, greet_place, 0)
    for step in range(1, layers):
        greet(device((section + step) % 8, place))
    greet(swap)

    for load in loads[2:]:
        load.wait()
    own_features = pl.ds(pl.multiple_of(place * 256, 256), 256)
    lane = lax.broadcasted_iota(jnp.int32, (8, 256), 1)
    outer = jnp.full((8, 256), second_scales[0, 0], F32)
    for group in range(1, 8):
        outer = jnp.where(lane >= group * SROWS, second_scales[0, group], outer)
    block_scale = outer * (scale_codes[...].astype(F32) + 1.0) / 256.0
    gain_lanes = jnp.broadcast_to(gains[:, own_features].astype(F32), (120, 256))
    columns_of = jnp.concatenate([block_scale, gain_lanes], axis=0).T
    side = lax.broadcasted_iota(jnp.int32, (256, HEAD), 1) < BLOCK
    low_rank = lax.dot_general(
        down[:, own_features], raised[...], (((0,), (0,)), ((), ())), preferred_element_type=F32
    )
    for tile in range(KV_HEADS):
        at = slice(tile * HEAD, (tile + 1) * HEAD)
        entries = codes[:, at]
        looked = jnp.full((256, HEAD), NF4_TABLE[0], F32)
        for entry in range(1, 16):
            looked = jnp.where(entries == entry, NF4_TABLE[entry], looked)
        left = columns_of[:, 2 * tile : 2 * tile + 1]
        right = columns_of[:, 2 * tile + 1 : 2 * tile + 2]
        base = (looked * jnp.where(side, left, right)).astype(BF16).astype(F32)
        rows_of = (base + adapter_scale * low_rank[:, at]) * columns_of[:, 8:9]
        shard[:, at] = rows_of.astype(BF16)
    pl.semaphore_wait(barrier, 31 + 7 + 1)

    quarter_at = (z % 2) * 2 + core
    fellows = (
        (quarter_at + 1 - 2 * core, mate),
        ((1 - z % 2) * 2 + core, device(section, xl * 16 + (z + 1 - 2 * (z % 2)) * 2 + core)),
        (
            (1 - z % 2) * 2 + 1 - core,
            device(section, xl * 16 + (z + 1 - 2 * (z % 2)) * 2 + 1 - core),
        ),
    )
    early_base = used[0]
    used[0] += 24
    y_up, y_down = (y + 1) % 4, (y + 3) % 4
    y_far = (y + 2) % 4

    def quad_copy(index):
        which, to = fellows[index]
        return (
            quad_send.at[which],
            quad_recv.at[quarter_at],
            quad_sem.at[quarter_at],
            to,
            send_sem.at[early_base + index],
        )

    def depth_copy(step):
        rows_at = mixes.at[section, z, core]
        to = device(section, xl * 16 + ((z + step) % 8) * 2 + core)
        return (rows_at, rows_at, depth_sem.at[z], to, send_sem.at[early_base + 2 + step])

    def mix_block(which_y, which, part=None):
        if part is None:
            return mixes.at[pl.ds(2 * which_y, 2), :, which]
        return mixes.at[pl.ds(2 * which_y, 2), pl.ds(part * 4, 4), which]

    mix_moves = (
        (mix_block(y, core), 0, (2 * y_up + xh, place)),
        (mix_block(y, core), 1, (2 * y_down + xh, place)),
        (mix_block(y_down, core, 0), 2, (2 * y_up + xh, place)),
        (mix_block(y_up, core, 1), 3, (2 * y_down + xh, place)),
        (mix_block(y_down, core), 4, mate),
        (mix_block(y_up, core), 5, mate),
        (mix_block(y_far, core, 0), 6, mate),
        (mix_block(y_far, core, 1), 7, mate),
        (mixes.at[section, :, core], 8, across),
        (mix_block(y, core), 9, mate),
        (mixes.at[section, :, core], 10, swap),
        (mixes.at[twin, :, core], 11, across),
    )

    def mix_copy(index):
        block, sem, to = mix_moves[index]
        return (block, block, mix_sem.at[sem], to, send_sem.at[early_base + 10 + index])

    def quad_start():
        own = shard[:128].astype(F32) + shard[128:].astype(F32)
        quad_send[...] = own.astype(BF16).reshape(4, 32, KVW)
        for index in range(3):
            transfer(*quad_copy(index))

    def depth_start():
        summed = quad_send[quarter_at].astype(F32)
        for which, _ in fellows:
            arrive(quad_recv.at[which], quad_sem.at[which])
            summed += quad_recv[which].astype(F32)
        mixes[section, z, core] = summed.astype(BF16)
        for step in range(1, 8):
            transfer(*depth_copy(step))

    def across_start():
        @pl.when(xl == 0)
        def _():
            for step in range(1, 8):
                at_z = (z + step) % 8
                arrive(mixes.at[section, at_z, core], depth_sem.at[at_z])
            transfer(*mix_copy(8))
            transfer(*mix_copy(10))

    def across_more():
        @pl.when(xl == 1)
        def _():
            arrive(mixes.at[twin, :, core], mix_sem.at[10])
            transfer(*mix_copy(11))
            arrive(mixes.at[section, :, core], mix_sem.at[8])

    def ring_start():
        @pl.when(xl == 0)
        def _():
            arrive(mixes.at[twin, :, core], mix_sem.at[11])

        for index in (0, 1, 9):
            transfer(*mix_copy(index))

    def ring_more():
        arrive(mix_block(y_down, core), mix_sem.at[0])
        transfer(*mix_copy(2))
        transfer(*mix_copy(4))
        arrive(mix_block(y_up, core), mix_sem.at[1])
        transfer(*mix_copy(3))
        transfer(*mix_copy(5))

    def ring_last():
        arrive(mix_block(y_far, core, 0), mix_sem.at[2])
        transfer(*mix_copy(6))
        arrive(mix_block(y_far, core, 1), mix_sem.at[3])
        transfer(*mix_copy(7))

    @pl.when(xl == 0)
    def _():
        quad_start()

    pending = []

    def slot(x, depth, which):
        return x * 16 + depth * 2 + which

    def half(block, h):
        return weight.at[block, pl.ds(h * 128, 128)]

    def pass_on(block, h, to):
        pending.append(transfer(half(block, h), half(block, h), weight_sem.at[block * 2 + h], to))

    def await_block(block, h):
        arrive(half(block, h), weight_sem.at[block * 2 + h])

    swapped_place = (place + 16) % 32

    @pl.when(xl != xh)
    def _():
        for h in range(2):
            transfer(
                shard.at[pl.ds(h * 128, 128)],
                half(swapped_place, h),
                weight_sem.at[swapped_place * 2 + h],
                swap,
                local_sem.at[3 + h],
            )

    @pl.when(xl == xh)
    def _():
        pltpu.make_async_copy(shard, weight.at[place], local_sem.at[3]).start()

    rows = pl.ds(y * 32, 32)
    chain_rows = pl.ds(section * 16, 16)

    def fold(ref):
        for head in range(KV_HEADS):
            part = jnp.zeros((16, HEAD), F32)
            for member in range(GROUP):
                at = (head * GROUP + member) * HEAD
                part += ref[chain_rows, pl.ds(at, HEAD)].astype(F32)
            yield head, part

    @pl.when(xl == xh)
    def _():
        pltpu.make_async_copy(shard, weight.at[place], local_sem.at[3]).wait()

    others = [place, slot(1 - xl, z, core)]

    for h in range(2):

        @pl.when(xl != xh)
        def _():
            await_block(place, h)

        if h == 0:
            pass_on(place, h, across)
        for to in (above, below, mate):
            pass_on(place, h, to)

    @pl.when(xl == 0)
    def _():
        depth_start()

    loads[0].wait()
    loads[1].wait()
    for head, part in fold(hidden):
        folded[:, head * HEAD : (head + 1) * HEAD] = part
    for head, part in fold(cotangent):
        descent[:, head * HEAD : (head + 1) * HEAD] = part
    square = jnp.zeros((16, HEAD), F32)
    for at in range(0, width, HEAD):
        piece = hidden[chain_rows, pl.ds(at, HEAD)].astype(F32)
        square += piece * piece
    squares[...] = jnp.broadcast_to(jnp.sum(square, axis=1, keepdims=True), (16, HEAD))
    product[...] = jnp.zeros_like(product)

    await_block(others[1], 0)
    for to in (above, below, mate):
        pass_on(others[1], 0, to)


    def at_distance(distance):
        if distance == 0:
            return [z]
        if distance == 4:
            return [(z + 4) % 8]
        return [(z + 8 - distance) % 8, (z + distance) % 8]

    def multiply(distance, which):
        depths = len(at_distance(distance))

        def step(index, carry):
            x = index // depths
            depth = (z + 8 - distance + (index % depths) * 2 * distance) % 8
            block = slot(x, depth, which)
            columns = pl.ds(pl.multiple_of(column_base + (depth * 2 + which) * 256, 256), 256)
            product[x] += jnp.dot(hidden[:, columns], weight[block], preferred_element_type=F32)
            return carry

        lax.fori_loop(0, 2 * depths, step, 0)

    def relay_across(distance):
        for depth in at_distance(distance):
            block = slot(1 - xl, depth, core)
            await_block(block, 1)
            pass_on(block, 1, mate)

    def await_mate(distance):
        for depth in at_distance(distance):
            for x in range(2):
                for h in range(2):
                    await_block(slot(x, depth, 1 - core), h)

    hooks = {
        (1, 1): across_start,
        (1, 2): across_more,
        (2, 1): ring_start,
        (4, 0): ring_more,
    }
    for distance in range(1, 5):
        low, high = (z + 8 - distance) % 8, (z + distance) % 8
        for turn, (x, h, up_reach, down_reach) in enumerate(
            ((xl, 1, 3, 3), (xl, 0, 4, 3), (1 - xl, 0, 3, 4))
        ):
            for depth, reach, onward in ((low, up_reach, above), (high, down_reach, below)):
                if distance > reach:
                    continue
                block = slot(x, depth, core)
                await_block(block, h)
                if distance < reach:
                    pass_on(block, h, onward)
                pass_on(block, h, mate)
                if h == 1:
                    pass_on(block, h, across)
            if distance == 3 and h == 1:
                ends = slot(xl, low + (high - low) * core, core)
                pass_on(ends, 1, device(section, xl * 16 + ((z + 1 + 6 * core) % 8) * 2 + core))
            if distance == 4 and h == 1:
                await_block(slot(x, low, core), 1)
                pass_on(slot(x, low, core), 1, across)
                pass_on(slot(x, low, core), 1, mate)
            if (distance, turn) in hooks:
                hooks[distance, turn]()
        if distance == 1:
            pass_on(place, 1, across)
        relay_across(distance - 1)
        multiply(distance - 1, core)
        if distance >= 2:
            await_mate(distance - 2)
            multiply(distance - 2, 1 - core)
    relay_across(4)
    ring_last()
    multiply(4, core)
    for distance in (3, 4):
        await_mate(distance)
        multiply(distance, 1 - core)

    product_send[...] = product[...].astype(BF16)
    for step in range(1, 8):
        to_section = (section + step) % 8
        pending.append(
            transfer(
                product_send.at[:, pl.ds(to_section * 16, 16)],
                product_recv.at[section],
                product_sem.at[section],
                (to_section, place),
            )
        )

    reply_base = used[0]
    used[0] += 24

    total_base = used[0]
    used[0] += 8

    def reply_copies(step):
        to_section = (section + step) % 8
        to = (to_section, place)
        at = reply_base + step * 3
        pair = pl.ds(to_section - to_section % 2, 2)
        return (
            (
                scaled_send.at[pair],
                scaled.at[:, chain_rows],
                reply_sem.at[section * 3],
                to,
                send_sem.at[at],
            ),
            (
                slope_send.at[to_section // 2],
                slopes.at[chain_rows],
                reply_sem.at[section * 3 + 1],
                to,
                send_sem.at[at + 1],
            ),
        )

    def total_copy(step, column):
        to_y = (y + step) % 4
        if column == 0:
            source, target = total_send.at[pl.ds(2 * to_y, 2)], total.at[:, chain_rows]
        else:
            source, target = total_send.at[2 * to_y + 1], total.at[1, chain_rows]
        return (
            source,
            target,
            reply_sem.at[section * 3 + 2],
            (2 * to_y + column, place),
            send_sem.at[total_base + step * 2 + column],
        )

    def each_total(column, act):
        for step in range(1, 4):
            act(total_copy(step, column))

        @pl.when(xh == 1 - column)
        def _():
            act(total_copy(0, column))

    product_recv[section] = product_send[:, chain_rows]
    for step in range(1, 8):
        sender = (section + step) % 8
        arrive(product_recv.at[sender], product_sem.at[sender])
    arrive(mix_block(y, 1 - core), mix_sem.at[9])
    arrive(mix_block(y_down, 1 - core), mix_sem.at[4])
    arrive(mix_block(y_up, 1 - core), mix_sem.at[5])
    arrive(mix_block(y_far, 1 - core, 0), mix_sem.at[6])
    arrive(mix_block(y_far, 1 - core, 1), mix_sem.at[7])

    square_sum = squares[:, :1]
    running = jnp.zeros((16, KVW), F32)
    for layer in range(layers):
        moved = 2.0 * folded[...] + GROUP * running
        energy = square_sum + jnp.sum(running * moved, axis=1, keepdims=True)
        inverse = 1.0 / jnp.sqrt(energy / width + epsilon)
        pair_at = layer - layer % 2
        mixed = product_recv[pair_at, layer % 2].astype(F32) + product_recv[
            pair_at + 1, layer % 2
        ].astype(F32)
        if layer:
            mixed += jnp.dot(
                running.astype(BF16), mixes[layer].reshape(KVW, KVW), preferred_element_type=F32
            )
        value = mixed * inverse
        totals[layer] = running
        values[layer] = value
        inverses[layer] = jnp.broadcast_to(inverse, (16, HEAD))
        total_send[layer] = running.astype(BF16)
        running = running + value
    each_total(0, lambda copy: transfer(*copy))
    direction = descent[...]
    for layer in reversed(range(layers)):
        inverse = inverses[layer][:, :1]
        slope = (
            jnp.sum(direction * values[layer], axis=1, keepdims=True)
            / width
            * inverse
            * inverse
        )
        step_scaled = (direction * inverse).astype(BF16)
        scaled_send[layer] = step_scaled
        at = (layer % 2) * 64
        slope_send[layer // 2, :, at : at + 64] = jnp.broadcast_to(slope, (16, 64)).astype(
            BF16
        )
        if layer:
            direction = (
                direction
                + lax.dot_general(
                    step_scaled,
                    mixes[layer].reshape(KVW, KVW),
                    (((1,), (1,)), ((), ())),
                    preferred_element_type=F32,
                )
                - (folded[...] + GROUP * totals[layer]) * slope
            )
    for item in range(2):
        for step in range(1, 8):
            transfer(*reply_copies(step)[item])
    each_total(1, lambda copy: transfer(*copy))
    own_pair = pl.ds(2 * y, 2)
    scaled[:, chain_rows] = scaled_send[own_pair]
    total[:, chain_rows] = total_send[own_pair]
    slopes[chain_rows] = slope_send[y]

    def await_totals(layers_at):
        for step in range(1, 8):
            sender = (section + step) % 8
            arrive(total.at[layers_at, pl.ds(sender * 16, 16)], reply_sem.at[sender * 3 + 2])

    for step in range(1, 8):
        sender = (section + step) % 8
        token_rows = pl.ds(sender * 16, 16)
        arrive(scaled.at[:, token_rows], reply_sem.at[sender * 3])
        arrive(slopes.at[token_rows], reply_sem.at[sender * 3 + 1])

    @pl.when(xh == 1)
    def _():
        shifts[...] = jnp.zeros_like(shifts)

    @pl.when(xh == 0)
    def _():
        await_totals(slice(None))
        shifts[...] = total[...]

    pair_base = used[0]
    used[0] += 28
    quarter = half_width // 4

    def pair_copy(q, step):
        to_y = (y + step) % 4
        columns = pl.ds(q * quarter, quarter)
        return (
            pair_send.at[pl.ds(to_y * 32, 32), columns],
            pair_recv.at[y, :, columns],
            pair_sem.at[y * 4 + q],
            (2 * to_y + xh, place),
            send_sem.at[pair_base + q * 3 + step - 1],
        )

    def later_copy(q, step):
        to_y = (y + step) % 4
        columns = pl.ds(q * quarter, quarter)
        return (
            later_send.at[to_y, :, columns],
            later.at[pl.ds(y * 32, 32), columns],
            later_sem.at[y * 4 + q],
            (2 * to_y + xh, place),
            send_sem.at[pair_base + 12 + q * 3 + step - 1],
        )

    def other_copy(q):
        return (
            other_send.at[:, pl.ds(q * quarter, quarter)],
            out.at[:, pl.ds(pl.multiple_of(column_base + q * quarter, quarter), quarter)],
            other_sem.at[q],
            (twin, place),
            send_sem.at[pair_base + 24 + q],
        )

    def hidden_gradients(q):
        def step(index, carry):
            block = q * 4 + index
            at = pl.multiple_of(block * 256, 256)
            columns = pl.ds(pl.multiple_of(column_base + at, 256), 256)
            part = hidden[:, columns].astype(F32)
            grads = []
            for pair in range(2):
                shift = shifts[pair, :, q * HEAD : (q + 1) * HEAD].astype(F32)
                current = part + jnp.concatenate([shift, shift], axis=1)
                slope = slopes[:, pair * 64 : pair * 64 + 1].astype(F32)
                grads.append(
                    lax.dot_general(
                        scaled[pair],
                        weight[pair * 16 + block],
                        (((1,), (1,)), ((), ())),
                        preferred_element_type=F32,
                    )
                    - current * slope
                )
            odd[:, pl.ds(at, 256)] = grads[1].astype(BF16)
            pair_send[:, pl.ds(at, 256)] = (grads[0] + grads[1]).astype(BF16)
            return carry

        lax.fori_loop(0, 4, step, 0)

    def send_pairs(q):
        @pl.when(y >= 1)
        def _():
            for step in range(1, 4):
                transfer(*pair_copy(q, step))

    def suffix(q):
        columns = pl.ds(q * quarter, quarter)
        for step in range(1, 4):
            from_y = (y + step) % 4

            @pl.when(from_y >= 1)
            def _():
                arrive(pair_recv.at[from_y, :, columns], pair_sem.at[from_y * 4 + q])

        @pl.when(y >= 1)
        def _():
            pair_recv[y, :, columns] = pair_send[rows, columns]

        running = pair_recv[3, :, columns].astype(F32)
        later_send[2, :, columns] = running.astype(BF16)
        running += pair_recv[2, :, columns].astype(F32)
        later_send[1, :, columns] = running.astype(BF16)
        running += pair_recv[1, :, columns].astype(F32)
        later_send[0, :, columns] = running.astype(BF16)
        for step in range(1, 4):
            to_y = (y + step) % 4

            @pl.when(to_y < 3)
            def _():
                transfer(*later_copy(q, step))

        @pl.when(y < 3)
        def _():
            later[rows, columns] = later_send[y, :, columns]

        @pl.when(y == 3)
        def _():
            later[:, columns] = jnp.zeros((128, quarter), BF16)

    def finish(q):
        @pl.when(y < 3)
        def _():
            for step in range(1, 4):
                from_y = (y + step) % 4
                target = later.at[pl.ds(from_y * 32, 32), pl.ds(q * quarter, quarter)]
                arrive(target, later_sem.at[from_y * 4 + q])

        def step(index, carry):
            at = pl.multiple_of(q * quarter + index * 256, 256)
            columns = pl.ds(at, 256)
            own_columns = pl.ds(pl.multiple_of(column_base + at, 256), 256)
            start = cotangent[:, own_columns].astype(F32) + later[:, columns].astype(F32)
            even_grad = (start + pair_send[:, columns].astype(F32)).astype(BF16)
            odd_grad = (start + odd[:, columns].astype(F32)).astype(BF16)
            out[:, own_columns] = jnp.where(xh == 0, even_grad, odd_grad)
            other_send[:, columns] = jnp.where(xh == 0, odd_grad, even_grad)
            return carry

        lax.fori_loop(0, 4, step, 0)
        pending.append(transfer(*other_copy(q)))

    def adapter_low():
        low = lax.dot_general(
            raised[...], scaled[xh], (((1,), (1,)), ((), ())), preferred_element_type=F32
        )
        return (adapter_scale * low).astype(BF16)

    def adapter_part(low, first, carry):
        def step(block, carry):
            columns = pl.ds(pl.multiple_of(block * 512, 512), 512)
            part = hidden[:, columns].astype(F32)
            if first < 8:
                at = pl.ds(pl.multiple_of((block // 2) * HEAD, HEAD), HEAD)
                shift = total[xh, :, at].astype(F32)
                part += jnp.concatenate([shift, shift, shift, shift], axis=1)
            grad = jnp.dot(low, part.astype(BF16), preferred_element_type=F32).astype(BF16)
            grad_send[block, 0, :64] = grad[:, :256]
            grad_send[block, 1, :64] = grad[:, 256:]
            gained = (part * gains[:, columns].astype(F32)).astype(BF16)
            return carry + lax.dot_general(
                gained, down[:, columns], (((1,), (1,)), ((), ())), preferred_element_type=F32
            )

        return lax.fori_loop(first, first + 8, step, carry)

    def adapter_up(carry):
        narrow[...] = carry.astype(BF16)
        up_grad = adapter_scale * lax.dot_general(
            scaled[xh], narrow[...], (((0,), (0,)), ((), ())), preferred_element_type=F32
        )
        padded = jnp.concatenate([up_grad, jnp.zeros((KVW, 192), F32)], axis=1)
        grad_send[:, :, 64:] = padded.astype(BF16).reshape(16, 2, 16, 256)

    def mate_copy():
        return (
            grad_send.at[:, 1 - core],
            grad_mate,
            grad_sem.at[16],
            mate,
            grad_send_sem.at[16],
        )

    def grad_copy(step):
        to = (z + step) % 8
        return (
            grad_sum.at[:, to],
            grad_recv.at[z],
            grad_sem.at[z],
            device(section, xl * 16 + to * 2 + core),
            grad_send_sem.at[step],
        )

    def send_grads(step, carry):
        transfer(*grad_copy(step))
        return carry

    def cross_copy():
        return (
            grad_cross.at[0],
            grad_cross.at[1],
            grad_sem.at[17],
            across,
            grad_send_sem.at[17],
        )

    def sum_mate(index, carry):
        both = grad_send[index, core].astype(F32) + grad_mate[index].astype(F32)
        grad_sum[index // 8, index % 8] = both.astype(BF16)
        return carry

    hidden_gradients(0)
    send_pairs(0)
    hidden_gradients(1)
    send_pairs(1)

    @pl.when(xh == 1)
    def _():
        await_totals(1)

    low = adapter_low()
    carry = adapter_part(low, 0, jnp.zeros((128, 64), F32))
    adapter_up(adapter_part(low, 8, carry))
    transfer(*mate_copy())
    suffix(0)
    hidden_gradients(2)
    send_pairs(2)
    suffix(1)
    hidden_gradients(3)
    send_pairs(3)
    arrive(grad_mate, grad_sem.at[16])
    lax.fori_loop(0, 16, sum_mate, 0)
    lax.fori_loop(1, 8, send_grads, 0)
    grad_recv[z] = grad_sum[:, z]
    finish(0)
    suffix(2)
    finish(1)
    suffix(3)
    finish(2)
    finish(3)

    def await_grads(step, carry):
        sender = (z + 8 - step) % 8
        arrive(grad_recv.at[sender], grad_sem.at[sender])
        return carry

    lax.fori_loop(1, 8, await_grads, 0)

    def sum_grads(index, carry):
        own, cross = carry
        return (
            own + grad_recv[index, xl].astype(F32),
            cross + grad_recv[index, 1 - xl].astype(F32),
        )

    nothing = jnp.zeros((80, 256), F32)
    summed, cross = lax.fori_loop(0, 8, sum_grads, (nothing, nothing))
    grad_cross[0] = cross.astype(BF16)
    transfer(*cross_copy())
    arrive(grad_cross.at[1], grad_sem.at[17])
    summed += grad_cross[1].astype(F32)
    down_out[...] = summed[:64] * gains[:, own_features].astype(F32)
    up_out[...] = summed[64:, :64]
    for q in range(4):
        columns = pl.ds(
            pl.multiple_of((1 - xh) * half_width + q * quarter, quarter), quarter
        )
        arrive(out.at[:, columns], other_sem.at[q])

    def gone(copy):
        source, target, arrival, to, sem = copy
        pltpu.make_async_remote_copy(
            src_ref=source,
            dst_ref=target,
            send_sem=sem,
            recv_sem=arrival,
            device_id=to,
            device_id_type=pl.DeviceIdType.MESH,
        ).wait_send()

    for copy in pending:
        copy.wait_send()

    @pl.when(xl != xh)
    def _():
        for h in range(2):
            gone(
                (
                    shard.at[pl.ds(h * 128, 128)],
                    half(swapped_place, h),
                    weight_sem.at[swapped_place * 2 + h],
                    swap,
                    local_sem.at[3 + h],
                )
            )

    @pl.when(xl == 0)
    def _():
        for index in range(3):
            gone(quad_copy(index))
        for step in range(1, 8):
            gone(depth_copy(step))
        gone(mix_copy(8))
        gone(mix_copy(10))

    @pl.when(xl == 1)
    def _():
        gone(mix_copy(11))

    for index in (0, 1, 2, 3, 4, 5, 6, 7, 9):
        gone(mix_copy(index))
    for step in range(1, 8):
        for copy in reply_copies(step):
            gone(copy)
    each_total(0, gone)
    each_total(1, gone)

    @pl.when(y >= 1)
    def _():
        for q in range(4):
            for step in range(1, 4):
                gone(pair_copy(q, step))

    for step in range(1, 4):

        @pl.when((y + step) % 4 < 3)
        def _():
            for q in range(4):
                gone(later_copy(q, step))

    def grads_gone(step, carry):
        gone(grad_copy(step))
        return carry

    lax.fori_loop(1, 8, grads_gone, 0)
    gone(mate_copy())
    gone(cross_copy())
    assert used[0] <= SENDS, used


SENDS = 256


def shards(
    codes,
    scale_codes,
    second_scales,
    gains,
    down_adapter,
    up_projection_weight,
    hidden_in,
    cotangent,
):
    tokens, width = hidden_in.shape
    vmem = pl.BlockSpec(memory_space=pltpu.VMEM)
    smem = pl.BlockSpec(memory_space=pltpu.SMEM)
    hbm = pl.BlockSpec(memory_space=pltpu.HBM)
    dma = pltpu.SemaphoreType.DMA
    input_grad, down_grad, up_grad = pl.pallas_call(
        functools.partial(chip_kernel, width),
        out_shape=(
            pltpu.VMEM((tokens, width), BF16),
            pltpu.VMEM((64, 256), F32),
            pltpu.VMEM((16, 64), F32),
        ),
        in_specs=[hbm, hbm, smem, hbm, hbm, hbm, hbm, hbm],
        out_specs=(vmem, vmem, vmem),
        scratch_shapes=[
            pltpu.VMEM((32, 256, KVW), BF16),
            pltpu.VMEM((8, 8, 2, 32, KVW), BF16),
            pltpu.VMEM((256, KVW), jnp.int32),
            pltpu.VMEM((8, 256), jnp.int32),
            pltpu.VMEM((1, width), BF16),
            pltpu.VMEM((64, KVW), BF16),
            pltpu.VMEM((256, KVW), BF16),
            pltpu.VMEM((4, 32, KVW), BF16),
            pltpu.VMEM((4, 32, KVW), BF16),
            pltpu.VMEM((tokens, width), BF16),
            pltpu.VMEM((tokens, width), BF16),
            pltpu.VMEM((64, width), BF16),
            pltpu.VMEM((2, tokens, KVW), F32),
            pltpu.VMEM((2, tokens, KVW), BF16),
            pltpu.VMEM((8, 2, 16, KVW), BF16),
            pltpu.VMEM((16, KVW), F32),
            pltpu.VMEM((16, KVW), F32),
            pltpu.VMEM((16, HEAD), F32),
            pltpu.VMEM((8, 16, KVW), F32),
            pltpu.VMEM((8, 16, KVW), F32),
            pltpu.VMEM((8, 16, HEAD), F32),
            pltpu.VMEM((8, 16, KVW), BF16),
            pltpu.VMEM((8, 16, KVW), BF16),
            pltpu.VMEM((4, 16, HEAD), BF16),
            pltpu.VMEM((2, tokens, KVW), BF16),
            pltpu.VMEM((2, tokens, KVW), BF16),
            pltpu.VMEM((2, tokens, KVW), BF16),
            pltpu.VMEM((tokens, HEAD), BF16),
            pltpu.VMEM((tokens, width // 2), BF16),
            pltpu.VMEM((tokens, width // 2), BF16),
            pltpu.VMEM((4, 32, width // 2), BF16),
            pltpu.VMEM((3, 32, width // 2), BF16),
            pltpu.VMEM((tokens, width // 2), BF16),
            pltpu.VMEM((tokens, width // 2), BF16),
            pltpu.VMEM((16, 2, 80, 256), BF16),
            pltpu.VMEM((16, 80, 256), BF16),
            pltpu.VMEM((2, 8, 80, 256), BF16),
            pltpu.VMEM((8, 2, 80, 256), BF16),
            pltpu.VMEM((2, 80, 256), BF16),
            pltpu.VMEM((tokens, 64), BF16),
            dma((9,)),
            dma((SENDS,)),
            dma((64,)),
            dma((4,)),
            dma((8,)),
            dma((12,)),
            dma((8,)),
            dma((24,)),
            dma((16,)),
            dma((16,)),
            dma((4,)),
            dma((18,)),
            dma((18,)),
        ],
        compiler_params=pltpu.CompilerParams(
            collective_id=0, has_side_effects=True, vmem_limit_bytes=56 * 2**20
        ),
        name="relay",
    )(
        codes[0],
        scale_codes[0].T,
        second_scales,
        gains,
        down_adapter[0].T,
        up_projection_weight[0].T,
        hidden_in,
        cotangent,
    )
    return (input_grad[None], down_grad.T[None], up_grad[None])


def solution(mesh):
    return jax.shard_map(
        shards,
        mesh=mesh,
        in_specs=(
            P("section", "fsdp", None),
            P("section", "fsdp", None),
            P("section", "fsdp"),
            P("section", None),
            P("section", None, None),
            P("section", None, None),
            P("fsdp", None),
            P("fsdp", None),
        ),
        out_specs=(
            P("section", "fsdp", None),
            P("section", "fsdp", None),
            P("section", "fsdp", None),
        ),
        check_vma=False,
    )
```

```python
import functools

import jax
import jax.numpy as jnp
from jax import lax
from jax.experimental import pallas as pl
from jax.experimental.pallas import tpu as pltpu
from jax.sharding import PartitionSpec as P

HEAD = 128
GROUP = 8
KV_HEADS = 4
KVW = KV_HEADS * HEAD
BLOCK = 64
SROWS = 32

NF4_TABLE = (
    -1.0,
    -0.6961928009986877,
    -0.5250730514526367,
    -0.39491748809814453,
    -0.28444138169288635,
    -0.18477343022823334,
    -0.09105003625154495,
    0.0,
    0.07958029955625534,
    0.16093020141124725,
    0.24611230194568634,
    0.33791524171066284,
    0.44070982933044434,
    0.5626170039176941,
    0.7229568362236023,
    1.0,
)
adapter_scale = 0.5
epsilon = 1e-05
F32 = jnp.float32
BF16 = jnp.bfloat16


def chip_kernel(
    width,
    codes_hbm,
    scale_hbm,
    second_scales,
    gains_hbm,
    down_hbm,
    raised_hbm,
    hidden_hbm,
    cotangent_hbm,
    out,
    down_out,
    up_out,
    weight,
    mixes,
    codes,
    scale_codes,
    gains,
    raised,
    shard,
    quad_send,
    quad_recv,
    hidden,
    cotangent,
    down,
    product,
    product_send,
    product_recv,
    folded,
    descent,
    squares,
    totals,
    values,
    inverses,
    scaled_send,
    total_send,
    slope_send,
    scaled,
    total,
    shifts,
    slopes,
    pair_send,
    odd,
    pair_recv,
    later_send,
    later,
    other_send,
    grad_send,
    grad_mate,
    grad_sum,
    grad_recv,
    grad_cross,
    narrow,
    local_sem,
    send_sem,
    weight_sem,
    quad_sem,
    depth_sem,
    mix_sem,
    product_sem,
    reply_sem,
    pair_sem,
    later_sem,
    other_sem,
    grad_send_sem,
    grad_sem,
):
    section = lax.axis_index("section")
    place = lax.axis_index("fsdp")
    y, xh = section // 2, section % 2
    xl, z, core = place // 16, (place // 2) % 8, place % 2
    half_width = width // 2
    column_base = xh * half_width
    layers = 2 * 4

    def device(to_section, to_place):
        return (to_section, to_place)

    mate = device(section, 2 * (place // 2) + 1 - core)
    across = device(section, (place + 16) % 32)
    above = device(section, xl * 16 + ((z + 1) % 8) * 2 + core)
    below = device(section, xl * 16 + ((z + 7) % 8) * 2 + core)
    twin = 2 * y + 1 - xh
    swap = device(twin, (place + 16) % 32)
    used = [0]

    def transfer(source, target, arrival, to, sem=None):
        if sem is None:
            sem = send_sem.at[used[0]]
            used[0] += 1
        copy = pltpu.make_async_remote_copy(
            src_ref=source,
            dst_ref=target,
            send_sem=sem,
            recv_sem=arrival,
            device_id=to,
            device_id_type=pl.DeviceIdType.MESH,
        )
        copy.start()
        return copy

    def arrive(target, arrival):
        pltpu.make_async_remote_copy(
            src_ref=target,
            dst_ref=target,
            send_sem=send_sem.at[0],
            recv_sem=arrival,
            device_id=mate,
            device_id_type=pl.DeviceIdType.MESH,
        ).wait_recv()

    loads = [
        pltpu.make_async_copy(hidden_hbm, hidden, local_sem.at[0]),
        pltpu.make_async_copy(cotangent_hbm, cotangent, local_sem.at[1]),
        pltpu.make_async_copy(down_hbm, down, local_sem.at[2]),
        pltpu.make_async_copy(codes_hbm, codes, local_sem.at[5]),
        pltpu.make_async_copy(scale_hbm, scale_codes, local_sem.at[6]),
        pltpu.make_async_copy(gains_hbm, gains, local_sem.at[7]),
        pltpu.make_async_copy(raised_hbm, raised, local_sem.at[8]),
    ]
    for load in reversed(loads):
        load.start()

    barrier = pltpu.get_barrier_semaphore()

    def greet(to):
        pl.semaphore_signal(
            barrier, inc=1, device_id=to, device_id_type=pl.DeviceIdType.MESH
        )

    def greet_place(step, carry):
        greet(device(section, (place + step) % 32))
        return carry

    lax.fori_loop(1, 32, greet_place, 0)
    for step in range(1, layers):
        greet(device((section + step) % 8, place))
    greet(swap)

    for load in loads[2:]:
        load.wait()
    own_features = pl.ds(pl.multiple_of(place * 256, 256), 256)
    lane = lax.broadcasted_iota(jnp.int32, (8, 256), 1)
    outer = jnp.full((8, 256), second_scales[0, 0], F32)
    for group in range(1, 8):
        outer = jnp.where(lane >= group * SROWS, second_scales[0, group], outer)
    block_scale = outer * (scale_codes[...].astype(F32) + 1.0) / 256.0
    gain_lanes = jnp.broadcast_to(gains[:, own_features].astype(F32), (120, 256))
    columns_of = jnp.concatenate([block_scale, gain_lanes], axis=0).T
    side = lax.broadcasted_iota(jnp.int32, (256, HEAD), 1) < BLOCK
    low_rank = lax.dot_general(
        down[:, own_features], raised[...], (((0,), (0,)), ((), ())), preferred_element_type=F32
    )
    for tile in range(KV_HEADS):
        at = slice(tile * HEAD, (tile + 1) * HEAD)
        entries = codes[:, at]
        looked = jnp.full((256, HEAD), NF4_TABLE[0], F32)
        for entry in range(1, 16):
            looked = jnp.where(entries == entry, NF4_TABLE[entry], looked)
        left = columns_of[:, 2 * tile : 2 * tile + 1]
        right = columns_of[:, 2 * tile + 1 : 2 * tile + 2]
        base = (looked * jnp.where(side, left, right)).astype(BF16).astype(F32)
        rows_of = (base + adapter_scale * low_rank[:, at]) * columns_of[:, 8:9]
        shard[:, at] = rows_of.astype(BF16)
    pl.semaphore_wait(barrier, 31 + 7 + 1)

    quarter_at = (z % 2) * 2 + core
    fellows = (
        (quarter_at + 1 - 2 * core, mate),
        ((1 - z % 2) * 2 + core, device(section, xl * 16 + (z + 1 - 2 * (z % 2)) * 2 + core)),
        (
            (1 - z % 2) * 2 + 1 - core,
            device(section, xl * 16 + (z + 1 - 2 * (z % 2)) * 2 + 1 - core),
        ),
    )
    early_base = used[0]
    used[0] += 24
    y_up, y_down = (y + 1) % 4, (y + 3) % 4
    y_far = (y + 2) % 4

    def quad_copy(index):
        which, to = fellows[index]
        return (
            quad_send.at[which],
            quad_recv.at[quarter_at],
            quad_sem.at[quarter_at],
            to,
            send_sem.at[early_base + index],
        )

    def depth_copy(step):
        rows_at = mixes.at[section, z, core]
        to = device(section, xl * 16 + ((z + step) % 8) * 2 + core)
        return (rows_at, rows_at, depth_sem.at[z], to, send_sem.at[early_base + 2 + step])

    def mix_block(which_y, which, part=None):
        if part is None:
            return mixes.at[pl.ds(2 * which_y, 2), :, which]
        return mixes.at[pl.ds(2 * which_y, 2), pl.ds(part * 4, 4), which]

    mix_moves = (
        (mix_block(y, core), 0, (2 * y_up + xh, place)),
        (mix_block(y, core), 1, (2 * y_down + xh, place)),
        (mix_block(y_down, core, 0), 2, (2 * y_up + xh, place)),
        (mix_block(y_up, core, 1), 3, (2 * y_down + xh, place)),
        (mix_block(y_down, core), 4, mate),
        (mix_block(y_up, core), 5, mate),
        (mix_block(y_far, core, 0), 6, mate),
        (mix_block(y_far, core, 1), 7, mate),
        (mixes.at[section, :, core], 8, across),
        (mix_block(y, core), 9, mate),
        (mixes.at[section, :, core], 10, swap),
        (mixes.at[twin, :, core], 11, across),
    )

    def mix_copy(index):
        block, sem, to = mix_moves[index]
        return (block, block, mix_sem.at[sem], to, send_sem.at[early_base + 10 + index])

    def quad_start():
        own = shard[:128].astype(F32) + shard[128:].astype(F32)
        quad_send[...] = own.astype(BF16).reshape(4, 32, KVW)
        for index in range(3):
            transfer(*quad_copy(index))

    def depth_start():
        summed = quad_send[quarter_at].astype(F32)
        for which, _ in fellows:
            arrive(quad_recv.at[which], quad_sem.at[which])
            summed += quad_recv[which].astype(F32)
        mixes[section, z, core] = summed.astype(BF16)
        for step in range(1, 8):
            transfer(*depth_copy(step))

    def across_start():
        @pl.when(xl == 0)
        def _():
            for step in range(1, 8):
                at_z = (z + step) % 8
                arrive(mixes.at[section, at_z, core], depth_sem.at[at_z])
            transfer(*mix_copy(8))
            transfer(*mix_copy(10))

    def across_more():
        @pl.when(xl == 1)
        def _():
            arrive(mixes.at[twin, :, core], mix_sem.at[10])
            transfer(*mix_copy(11))
            arrive(mixes.at[section, :, core], mix_sem.at[8])

    def ring_start():
        @pl.when(xl == 0)
        def _():
            arrive(mixes.at[twin, :, core], mix_sem.at[11])

        for index in (0, 1, 9):
            transfer(*mix_copy(index))

    def ring_more():
        arrive(mix_block(y_down, core), mix_sem.at[0])
        transfer(*mix_copy(2))
        transfer(*mix_copy(4))
        arrive(mix_block(y_up, core), mix_sem.at[1])
        transfer(*mix_copy(3))
        transfer(*mix_copy(5))

    def ring_last():
        arrive(mix_block(y_far, core, 0), mix_sem.at[2])
        transfer(*mix_copy(6))
        arrive(mix_block(y_far, core, 1), mix_sem.at[3])
        transfer(*mix_copy(7))

    @pl.when(xl == 0)
    def _():
        quad_start()

    pending = []

    def slot(x, depth, which):
        return x * 16 + depth * 2 + which

    def half(block, h):
        return weight.at[block, pl.ds(h * 128, 128)]

    def pass_on(block, h, to):
        pending.append(transfer(half(block, h), half(block, h), weight_sem.at[block * 2 + h], to))

    def await_block(block, h):
        arrive(half(block, h), weight_sem.at[block * 2 + h])

    swapped_place = (place + 16) % 32

    @pl.when(xl != xh)
    def _():
        for h in range(2):
            transfer(
                shard.at[pl.ds(h * 128, 128)],
                half(swapped_place, h),
                weight_sem.at[swapped_place * 2 + h],
                swap,
                local_sem.at[3 + h],
            )

    @pl.when(xl == xh)
    def _():
        pltpu.make_async_copy(shard, weight.at[place], local_sem.at[3]).start()

    rows = pl.ds(y * 32, 32)
    chain_rows = pl.ds(section * 16, 16)

    def fold(ref):
        for head in range(KV_HEADS):
            part = jnp.zeros((16, HEAD), F32)
            for member in range(GROUP):
                at = (head * GROUP + member) * HEAD
                part += ref[chain_rows, pl.ds(at, HEAD)].astype(F32)
            yield head, part

    @pl.when(xl == xh)
    def _():
        pltpu.make_async_copy(shard, weight.at[place], local_sem.at[3]).wait()

    others = [place, slot(1 - xl, z, core)]

    for h in range(2):

        @pl.when(xl != xh)
        def _():
            await_block(place, h)

        for to in (across, above, below, mate):
            pass_on(place, h, to)

    @pl.when(xl == 0)
    def _():
        depth_start()

    loads[0].wait()
    loads[1].wait()
    for head, part in fold(hidden):
        folded[:, head * HEAD : (head + 1) * HEAD] = part
    for head, part in fold(cotangent):
        descent[:, head * HEAD : (head + 1) * HEAD] = part
    square = jnp.zeros((16, HEAD), F32)
    for at in range(0, width, HEAD):
        piece = hidden[chain_rows, pl.ds(at, HEAD)].astype(F32)
        square += piece * piece
    squares[...] = jnp.broadcast_to(jnp.sum(square, axis=1, keepdims=True), (16, HEAD))
    product[...] = jnp.zeros_like(product)

    await_block(others[1], 0)
    for to in (above, below, mate):
        pass_on(others[1], 0, to)


    def at_distance(distance):
        if distance == 0:
            return [z]
        if distance == 4:
            return [(z + 4) % 8]
        return [(z + 8 - distance) % 8, (z + distance) % 8]

    def multiply(distance, which):
        depths = len(at_distance(distance))

        def step(index, carry):
            x = index // depths
            depth = (z + 8 - distance + (index % depths) * 2 * distance) % 8
            block = slot(x, depth, which)
            columns = pl.ds(pl.multiple_of(column_base + (depth * 2 + which) * 256, 256), 256)
            product[x] += jnp.dot(hidden[:, columns], weight[block], preferred_element_type=F32)
            return carry

        lax.fori_loop(0, 2 * depths, step, 0)

    def relay_across(distance):
        for depth in at_distance(distance):
            block = slot(1 - xl, depth, core)
            await_block(block, 1)
            pass_on(block, 1, mate)

    def await_mate(distance):
        for depth in at_distance(distance):
            for x in range(2):
                for h in range(2):
                    await_block(slot(x, depth, 1 - core), h)

    hooks = {
        (1, 1): across_start,
        (1, 2): across_more,
        (2, 1): ring_start,
        (4, 0): ring_more,
    }
    for distance in range(1, 5):
        low, high = (z + 8 - distance) % 8, (z + distance) % 8
        for turn, (x, h, up_reach, down_reach) in enumerate(
            ((xl, 1, 3, 3), (xl, 0, 4, 3), (1 - xl, 0, 3, 4))
        ):
            for depth, reach, onward in ((low, up_reach, above), (high, down_reach, below)):
                if distance > reach:
                    continue
                block = slot(x, depth, core)
                await_block(block, h)
                if distance < reach:
                    pass_on(block, h, onward)
                if h == 1:
                    pass_on(block, h, across)
                pass_on(block, h, mate)
            if distance == 3 and h == 1:
                ends = slot(xl, low + (high - low) * core, core)
                pass_on(ends, 1, device(section, xl * 16 + ((z + 1 + 6 * core) % 8) * 2 + core))
            if distance == 4 and h == 1:
                await_block(slot(x, low, core), 1)
                pass_on(slot(x, low, core), 1, across)
                pass_on(slot(x, low, core), 1, mate)
            if (distance, turn) in hooks:
                hooks[distance, turn]()
        relay_across(distance - 1)
        multiply(distance - 1, core)
        if distance >= 2:
            await_mate(distance - 2)
            multiply(distance - 2, 1 - core)
    relay_across(4)
    ring_last()
    multiply(4, core)
    for distance in (3, 4):
        await_mate(distance)
        multiply(distance, 1 - core)

    product_send[...] = product[...].astype(BF16)
    for step in range(1, 8):
        to_section = (section + step) % 8
        pending.append(
            transfer(
                product_send.at[:, pl.ds(to_section * 16, 16)],
                product_recv.at[section],
                product_sem.at[section],
                (to_section, place),
            )
        )

    reply_base = used[0]
    used[0] += 24

    total_base = used[0]
    used[0] += 8

    def reply_copies(step):
        to_section = (section + step) % 8
        to = (to_section, place)
        at = reply_base + step * 3
        pair = pl.ds(to_section - to_section % 2, 2)
        return (
            (
                scaled_send.at[pair],
                scaled.at[:, chain_rows],
                reply_sem.at[section * 3],
                to,
                send_sem.at[at],
            ),
            (
                slope_send.at[to_section // 2],
                slopes.at[chain_rows],
                reply_sem.at[section * 3 + 1],
                to,
                send_sem.at[at + 1],
            ),
        )

    def total_copy(step, column):
        to_y = (y + step) % 4
        if column == 0:
            source, target = total_send.at[pl.ds(2 * to_y, 2)], total.at[:, chain_rows]
        else:
            source, target = total_send.at[2 * to_y + 1], total.at[1, chain_rows]
        return (
            source,
            target,
            reply_sem.at[section * 3 + 2],
            (2 * to_y + column, place),
            send_sem.at[total_base + step * 2 + column],
        )

    def each_total(column, act):
        for step in range(1, 4):
            act(total_copy(step, column))

        @pl.when(xh == 1 - column)
        def _():
            act(total_copy(0, column))

    product_recv[section] = product_send[:, chain_rows]
    for step in range(1, 8):
        sender = (section + step) % 8
        arrive(product_recv.at[sender], product_sem.at[sender])
    arrive(mix_block(y, 1 - core), mix_sem.at[9])
    arrive(mix_block(y_down, 1 - core), mix_sem.at[4])
    arrive(mix_block(y_up, 1 - core), mix_sem.at[5])
    arrive(mix_block(y_far, 1 - core, 0), mix_sem.at[6])
    arrive(mix_block(y_far, 1 - core, 1), mix_sem.at[7])

    square_sum = squares[:, :1]
    running = jnp.zeros((16, KVW), F32)
    for layer in range(layers):
        moved = 2.0 * folded[...] + GROUP * running
        energy = square_sum + jnp.sum(running * moved, axis=1, keepdims=True)
        inverse = 1.0 / jnp.sqrt(energy / width + epsilon)
        pair_at = layer - layer % 2
        mixed = product_recv[pair_at, layer % 2].astype(F32) + product_recv[
            pair_at + 1, layer % 2
        ].astype(F32)
        if layer:
            mixed += jnp.dot(
                running.astype(BF16), mixes[layer].reshape(KVW, KVW), preferred_element_type=F32
            )
        value = mixed * inverse
        totals[layer] = running
        values[layer] = value
        inverses[layer] = jnp.broadcast_to(inverse, (16, HEAD))
        total_send[layer] = running.astype(BF16)
        running = running + value
    each_total(0, lambda copy: transfer(*copy))
    direction = descent[...]
    for layer in reversed(range(layers)):
        inverse = inverses[layer][:, :1]
        slope = (
            jnp.sum(direction * values[layer], axis=1, keepdims=True)
            / width
            * inverse
            * inverse
        )
        step_scaled = (direction * inverse).astype(BF16)
        scaled_send[layer] = step_scaled
        at = (layer % 2) * 64
        slope_send[layer // 2, :, at : at + 64] = jnp.broadcast_to(slope, (16, 64)).astype(
            BF16
        )
        if layer:
            direction = (
                direction
                + lax.dot_general(
                    step_scaled,
                    mixes[layer].reshape(KVW, KVW),
                    (((1,), (1,)), ((), ())),
                    preferred_element_type=F32,
                )
                - (folded[...] + GROUP * totals[layer]) * slope
            )
    for item in range(2):
        for step in range(1, 8):
            transfer(*reply_copies(step)[item])
    each_total(1, lambda copy: transfer(*copy))
    own_pair = pl.ds(2 * y, 2)
    scaled[:, chain_rows] = scaled_send[own_pair]
    total[:, chain_rows] = total_send[own_pair]
    slopes[chain_rows] = slope_send[y]

    def await_totals(layers_at):
        for step in range(1, 8):
            sender = (section + step) % 8
            arrive(total.at[layers_at, pl.ds(sender * 16, 16)], reply_sem.at[sender * 3 + 2])

    for step in range(1, 8):
        sender = (section + step) % 8
        token_rows = pl.ds(sender * 16, 16)
        arrive(scaled.at[:, token_rows], reply_sem.at[sender * 3])
        arrive(slopes.at[token_rows], reply_sem.at[sender * 3 + 1])

    @pl.when(xh == 1)
    def _():
        shifts[...] = jnp.zeros_like(shifts)

    @pl.when(xh == 0)
    def _():
        await_totals(slice(None))
        shifts[...] = total[...]

    pair_base = used[0]
    used[0] += 28
    quarter = half_width // 4

    def pair_copy(q, step):
        to_y = (y + step) % 4
        columns = pl.ds(q * quarter, quarter)
        return (
            pair_send.at[pl.ds(to_y * 32, 32), columns],
            pair_recv.at[y, :, columns],
            pair_sem.at[y * 4 + q],
            (2 * to_y + xh, place),
            send_sem.at[pair_base + q * 3 + step - 1],
        )

    def later_copy(q, step):
        to_y = (y + step) % 4
        columns = pl.ds(q * quarter, quarter)
        return (
            later_send.at[to_y, :, columns],
            later.at[pl.ds(y * 32, 32), columns],
            later_sem.at[y * 4 + q],
            (2 * to_y + xh, place),
            send_sem.at[pair_base + 12 + q * 3 + step - 1],
        )

    def other_copy(q):
        return (
            other_send.at[:, pl.ds(q * quarter, quarter)],
            out.at[:, pl.ds(pl.multiple_of(column_base + q * quarter, quarter), quarter)],
            other_sem.at[q],
            (twin, place),
            send_sem.at[pair_base + 24 + q],
        )

    def hidden_gradients(q):
        def step(index, carry):
            block = q * 4 + index
            at = pl.multiple_of(block * 256, 256)
            columns = pl.ds(pl.multiple_of(column_base + at, 256), 256)
            part = hidden[:, columns].astype(F32)
            grads = []
            for pair in range(2):
                shift = shifts[pair, :, q * HEAD : (q + 1) * HEAD].astype(F32)
                current = part + jnp.concatenate([shift, shift], axis=1)
                slope = slopes[:, pair * 64 : pair * 64 + 1].astype(F32)
                grads.append(
                    lax.dot_general(
                        scaled[pair],
                        weight[pair * 16 + block],
                        (((1,), (1,)), ((), ())),
                        preferred_element_type=F32,
                    )
                    - current * slope
                )
            odd[:, pl.ds(at, 256)] = grads[1].astype(BF16)
            pair_send[:, pl.ds(at, 256)] = (grads[0] + grads[1]).astype(BF16)
            return carry

        lax.fori_loop(0, 4, step, 0)

    def send_pairs(q):
        @pl.when(y >= 1)
        def _():
            for step in range(1, 4):
                transfer(*pair_copy(q, step))

    def suffix(q):
        columns = pl.ds(q * quarter, quarter)
        for step in range(1, 4):
            from_y = (y + step) % 4

            @pl.when(from_y >= 1)
            def _():
                arrive(pair_recv.at[from_y, :, columns], pair_sem.at[from_y * 4 + q])

        @pl.when(y >= 1)
        def _():
            pair_recv[y, :, columns] = pair_send[rows, columns]

        running = pair_recv[3, :, columns].astype(F32)
        later_send[2, :, columns] = running.astype(BF16)
        running += pair_recv[2, :, columns].astype(F32)
        later_send[1, :, columns] = running.astype(BF16)
        running += pair_recv[1, :, columns].astype(F32)
        later_send[0, :, columns] = running.astype(BF16)
        for step in range(1, 4):
            to_y = (y + step) % 4

            @pl.when(to_y < 3)
            def _():
                transfer(*later_copy(q, step))

        @pl.when(y < 3)
        def _():
            later[rows, columns] = later_send[y, :, columns]

        @pl.when(y == 3)
        def _():
            later[:, columns] = jnp.zeros((128, quarter), BF16)

    def finish(q):
        @pl.when(y < 3)
        def _():
            for step in range(1, 4):
                from_y = (y + step) % 4
                target = later.at[pl.ds(from_y * 32, 32), pl.ds(q * quarter, quarter)]
                arrive(target, later_sem.at[from_y * 4 + q])

        def step(index, carry):
            at = pl.multiple_of(q * quarter + index * 256, 256)
            columns = pl.ds(at, 256)
            own_columns = pl.ds(pl.multiple_of(column_base + at, 256), 256)
            start = cotangent[:, own_columns].astype(F32) + later[:, columns].astype(F32)
            even_grad = (start + pair_send[:, columns].astype(F32)).astype(BF16)
            odd_grad = (start + odd[:, columns].astype(F32)).astype(BF16)
            out[:, own_columns] = jnp.where(xh == 0, even_grad, odd_grad)
            other_send[:, columns] = jnp.where(xh == 0, odd_grad, even_grad)
            return carry

        lax.fori_loop(0, 4, step, 0)
        pending.append(transfer(*other_copy(q)))

    def adapter_low():
        low = lax.dot_general(
            raised[...], scaled[xh], (((1,), (1,)), ((), ())), preferred_element_type=F32
        )
        return (adapter_scale * low).astype(BF16)

    def adapter_part(low, first, carry):
        def step(block, carry):
            columns = pl.ds(pl.multiple_of(block * 512, 512), 512)
            part = hidden[:, columns].astype(F32)
            if first < 8:
                at = pl.ds(pl.multiple_of((block // 2) * HEAD, HEAD), HEAD)
                shift = total[xh, :, at].astype(F32)
                part += jnp.concatenate([shift, shift, shift, shift], axis=1)
            grad = jnp.dot(low, part.astype(BF16), preferred_element_type=F32).astype(BF16)
            grad_send[block, 0, :64] = grad[:, :256]
            grad_send[block, 1, :64] = grad[:, 256:]
            gained = (part * gains[:, columns].astype(F32)).astype(BF16)
            return carry + lax.dot_general(
                gained, down[:, columns], (((1,), (1,)), ((), ())), preferred_element_type=F32
            )

        return lax.fori_loop(first, first + 8, step, carry)

    def adapter_up(carry):
        narrow[...] = carry.astype(BF16)
        up_grad = adapter_scale * lax.dot_general(
            scaled[xh], narrow[...], (((0,), (0,)), ((), ())), preferred_element_type=F32
        )
        padded = jnp.concatenate([up_grad, jnp.zeros((KVW, 192), F32)], axis=1)
        grad_send[:, :, 64:] = padded.astype(BF16).reshape(16, 2, 16, 256)

    def mate_copy():
        return (
            grad_send.at[:, 1 - core],
            grad_mate,
            grad_sem.at[16],
            mate,
            grad_send_sem.at[16],
        )

    def grad_copy(step):
        to = (z + step) % 8
        return (
            grad_sum.at[:, to],
            grad_recv.at[z],
            grad_sem.at[z],
            device(section, xl * 16 + to * 2 + core),
            grad_send_sem.at[step],
        )

    def send_grads(step, carry):
        transfer(*grad_copy(step))
        return carry

    def cross_copy():
        return (
            grad_cross.at[0],
            grad_cross.at[1],
            grad_sem.at[17],
            across,
            grad_send_sem.at[17],
        )

    def sum_mate(index, carry):
        both = grad_send[index, core].astype(F32) + grad_mate[index].astype(F32)
        grad_sum[index // 8, index % 8] = both.astype(BF16)
        return carry

    hidden_gradients(0)
    send_pairs(0)
    hidden_gradients(1)
    send_pairs(1)
    hidden_gradients(2)
    suffix(0)
    send_pairs(2)
    hidden_gradients(3)
    suffix(1)
    send_pairs(3)

    @pl.when(xh == 1)
    def _():
        await_totals(1)

    low = adapter_low()
    carry = adapter_part(low, 0, jnp.zeros((128, 64), F32))
    adapter_up(adapter_part(low, 8, carry))
    transfer(*mate_copy())
    finish(0)
    suffix(2)
    finish(1)
    arrive(grad_mate, grad_sem.at[16])
    lax.fori_loop(0, 16, sum_mate, 0)
    lax.fori_loop(1, 8, send_grads, 0)
    grad_recv[z] = grad_sum[:, z]
    suffix(3)
    finish(2)
    finish(3)

    def await_grads(step, carry):
        sender = (z + 8 - step) % 8
        arrive(grad_recv.at[sender], grad_sem.at[sender])
        return carry

    lax.fori_loop(1, 8, await_grads, 0)

    def sum_grads(index, carry):
        own, cross = carry
        return (
            own + grad_recv[index, xl].astype(F32),
            cross + grad_recv[index, 1 - xl].astype(F32),
        )

    nothing = jnp.zeros((80, 256), F32)
    summed, cross = lax.fori_loop(0, 8, sum_grads, (nothing, nothing))
    grad_cross[0] = cross.astype(BF16)
    transfer(*cross_copy())
    arrive(grad_cross.at[1], grad_sem.at[17])
    summed += grad_cross[1].astype(F32)
    down_out[...] = summed[:64] * gains[:, own_features].astype(F32)
    up_out[...] = summed[64:, :64]
    for q in range(4):
        columns = pl.ds(
            pl.multiple_of((1 - xh) * half_width + q * quarter, quarter), quarter
        )
        arrive(out.at[:, columns], other_sem.at[q])

    def gone(copy):
        source, target, arrival, to, sem = copy
        pltpu.make_async_remote_copy(
            src_ref=source,
            dst_ref=target,
            send_sem=sem,
            recv_sem=arrival,
            device_id=to,
            device_id_type=pl.DeviceIdType.MESH,
        ).wait_send()

    for copy in pending:
        copy.wait_send()

    @pl.when(xl != xh)
    def _():
        for h in range(2):
            gone(
                (
                    shard.at[pl.ds(h * 128, 128)],
                    half(swapped_place, h),
                    weight_sem.at[swapped_place * 2 + h],
                    swap,
                    local_sem.at[3 + h],
                )
            )

    @pl.when(xl == 0)
    def _():
        for index in range(3):
            gone(quad_copy(index))
        for step in range(1, 8):
            gone(depth_copy(step))
        gone(mix_copy(8))
        gone(mix_copy(10))

    @pl.when(xl == 1)
    def _():
        gone(mix_copy(11))

    for index in (0, 1, 2, 3, 4, 5, 6, 7, 9):
        gone(mix_copy(index))
    for step in range(1, 8):
        for copy in reply_copies(step):
            gone(copy)
    each_total(0, gone)
    each_total(1, gone)

    @pl.when(y >= 1)
    def _():
        for q in range(4):
            for step in range(1, 4):
                gone(pair_copy(q, step))

    for step in range(1, 4):

        @pl.when((y + step) % 4 < 3)
        def _():
            for q in range(4):
                gone(later_copy(q, step))

    def grads_gone(step, carry):
        gone(grad_copy(step))
        return carry

    lax.fori_loop(1, 8, grads_gone, 0)
    gone(mate_copy())
    gone(cross_copy())
    assert used[0] <= SENDS, used


SENDS = 256


def shards(
    codes,
    scale_codes,
    second_scales,
    gains,
    down_adapter,
    up_projection_weight,
    hidden_in,
    cotangent,
):
    tokens, width = hidden_in.shape
    vmem = pl.BlockSpec(memory_space=pltpu.VMEM)
    smem = pl.BlockSpec(memory_space=pltpu.SMEM)
    hbm = pl.BlockSpec(memory_space=pltpu.HBM)
    dma = pltpu.SemaphoreType.DMA
    input_grad, down_grad, up_grad = pl.pallas_call(
        functools.partial(chip_kernel, width),
        out_shape=(
            pltpu.VMEM((tokens, width), BF16),
            pltpu.VMEM((64, 256), F32),
            pltpu.VMEM((16, 64), F32),
        ),
        in_specs=[hbm, hbm, smem, hbm, hbm, hbm, hbm, hbm],
        out_specs=(vmem, vmem, vmem),
        scratch_shapes=[
            pltpu.VMEM((32, 256, KVW), BF16),
            pltpu.VMEM((8, 8, 2, 32, KVW), BF16),
            pltpu.VMEM((256, KVW), jnp.int32),
            pltpu.VMEM((8, 256), jnp.int32),
            pltpu.VMEM((1, width), BF16),
            pltpu.VMEM((64, KVW), BF16),
            pltpu.VMEM((256, KVW), BF16),
            pltpu.VMEM((4, 32, KVW), BF16),
            pltpu.VMEM((4, 32, KVW), BF16),
            pltpu.VMEM((tokens, width), BF16),
            pltpu.VMEM((tokens, width), BF16),
            pltpu.VMEM((64, width), BF16),
            pltpu.VMEM((2, tokens, KVW), F32),
            pltpu.VMEM((2, tokens, KVW), BF16),
            pltpu.VMEM((8, 2, 16, KVW), BF16),
            pltpu.VMEM((16, KVW), F32),
            pltpu.VMEM((16, KVW), F32),
            pltpu.VMEM((16, HEAD), F32),
            pltpu.VMEM((8, 16, KVW), F32),
            pltpu.VMEM((8, 16, KVW), F32),
            pltpu.VMEM((8, 16, HEAD), F32),
            pltpu.VMEM((8, 16, KVW), BF16),
            pltpu.VMEM((8, 16, KVW), BF16),
            pltpu.VMEM((4, 16, HEAD), BF16),
            pltpu.VMEM((2, tokens, KVW), BF16),
            pltpu.VMEM((2, tokens, KVW), BF16),
            pltpu.VMEM((2, tokens, KVW), BF16),
            pltpu.VMEM((tokens, HEAD), BF16),
            pltpu.VMEM((tokens, width // 2), BF16),
            pltpu.VMEM((tokens, width // 2), BF16),
            pltpu.VMEM((4, 32, width // 2), BF16),
            pltpu.VMEM((3, 32, width // 2), BF16),
            pltpu.VMEM((tokens, width // 2), BF16),
            pltpu.VMEM((tokens, width // 2), BF16),
            pltpu.VMEM((16, 2, 80, 256), BF16),
            pltpu.VMEM((16, 80, 256), BF16),
            pltpu.VMEM((2, 8, 80, 256), BF16),
            pltpu.VMEM((8, 2, 80, 256), BF16),
            pltpu.VMEM((2, 80, 256), BF16),
            pltpu.VMEM((tokens, 64), BF16),
            dma((9,)),
            dma((SENDS,)),
            dma((64,)),
            dma((4,)),
            dma((8,)),
            dma((12,)),
            dma((8,)),
            dma((24,)),
            dma((16,)),
            dma((16,)),
            dma((4,)),
            dma((18,)),
            dma((18,)),
        ],
        compiler_params=pltpu.CompilerParams(
            collective_id=0, has_side_effects=True, vmem_limit_bytes=56 * 2**20
        ),
        name="relay",
    )(
        codes[0],
        scale_codes[0].T,
        second_scales,
        gains,
        down_adapter[0].T,
        up_projection_weight[0].T,
        hidden_in,
        cotangent,
    )
    return (input_grad[None], down_grad.T[None], up_grad[None])


def solution(mesh):
    return jax.shard_map(
        shards,
        mesh=mesh,
        in_specs=(
            P("section", "fsdp", None),
            P("section", "fsdp", None),
            P("section", "fsdp"),
            P("section", None),
            P("section", None, None),
            P("section", None, None),
            P("fsdp", None),
            P("fsdp", None),
        ),
        out_specs=(
            P("section", "fsdp", None),
            P("section", "fsdp", None),
            P("section", "fsdp", None),
        ),
        check_vma=False,
    )
```
